32 devices in a mesh: section: 2 (over core), expert: 4 (over y, x), dp: 4 (over z).
Axes of the slice: x: 2, y: 2, z: 4, core: 2. Of those that a mesh axis runs over, the one named last changes fastest.
Arguments:
- inputs: bfloat16 [2, 4, 256, 1024], P(None, 'expert', 'dp'), may hold values from -36 to 36
- cotangent: bfloat16 [2, 4, 256, 1024], P(None, 'expert', 'dp'), may hold values from -6 to 6
- segment_ids: int32 [2, 4, 256], P(None, 'expert'), may hold values from 0 to 3, never falling along the last dimension, each value on 1 to 128 neighbouring positions
- routes: int32 [2, 2, 4, 256, 1], P('section', None, 'expert', 'dp'), may hold values from 0 to 7; in each aligned block of 64 rows (0 to 63, 64 to 127, ..., all dimensions but the last counted through in order) at most 10 rows name the same one
- norm_gains: bfloat16 [2, 2, 1024], P('section', None, ('expert', 'dp')), may hold values from 0.5 to 1.5
- norm_shifts: bfloat16 [2, 2, 1024], P('section', None, ('expert', 'dp')), may hold values from -3 to 3
- attn_qkv: bfloat16 [2, 1024, 3072], P('section', ('expert', 'dp')), may hold values from -0.1875 to 0.1875
- attn_proj: bfloat16 [2, 1024, 1024], P('section', ('expert', 'dp')), may hold values from -0.75 to 0.75
- dense_up: bfloat16 [2, 1024, 4096], P('section', ('expert', 'dp')), may hold values from -0.1875 to 0.1875
- dense_down: bfloat16 [2, 4096, 1024], P('section', ('expert', 'dp')), may hold values from -0.09375 to 0.09375
- router: bfloat16 [2, 1024, 8], P('section', ('expert', 'dp')), may hold values from -0.25 to 0.25
- mixer: bfloat16 [2, 1024, 2], P('section', ('expert', 'dp')), may hold values from -0.4375 to 0.4375
- expert_up: bfloat16 [2, 8, 1024, 4096], P('section', 'expert', None, 'dp'), may hold values from -0.1875 to 0.1875
- expert_down: bfloat16 [2, 8, 4096, 1024], P('section', 'expert', 'dp'), may hold values from -4 to 4
Outputs:
- activations: bfloat16 [2, 2, 4, 256, 1024], P('section', None, 'expert', 'dp')
- input_grads: float32 [2, 2, 4, 256, 1024], P('section', None, 'expert', 'dp')
- grad_norm_gains: float32 [2, 2, 1024], P('section', None, ('expert', 'dp'))
- grad_norm_shifts: float32 [2, 2, 1024], P('section', None, ('expert', 'dp'))
- grad_attn_qkv: float32 [2, 1024, 3072], P('section', ('expert', 'dp'))
- grad_attn_proj: float32 [2, 1024, 1024], P('section', ('expert', 'dp'))
- grad_dense_up: float32 [2, 1024, 4096], P('section', ('expert', 'dp'))
- grad_dense_down: float32 [2, 4096, 1024], P('section', ('expert', 'dp'))
- grad_router: float32 [2, 1024, 8], P('section', ('expert', 'dp'))
- grad_mixer: float32 [2, 1024, 2], P('section', ('expert', 'dp'))
- grad_expert_up: float32 [2, 8, 1024, 4096], P('section', 'expert', None, 'dp')
- grad_expert_down: float32 [2, 8, 4096, 1024], P('section', 'expert', 'dp')
- branch_rms: float32 [2, 3], P('section')
The draws below stay inside these ranges and needn't reach their ends.
Inputs may be any that keep to these rules, and one draw needn't show every extreme that they name: `routes`: in each layer and micro-batch, at most 10 of the 64 tokens of one device's aligned block go to one expert, and some expert receives exactly 10.
All inputs are finite; a program needn't handle non-finite values.
Results may differ from the reference program's by a relative error of at most 0.022.
Values may be sent and summed in bfloat16 or wider, within the bound.
No kernel may reach another device: no remote copies, remote signals or barrier semaphores. Data moves between devices by JAX's collectives and lax.ppermute only.
A program may use at most 256 MiB of HBM per device.

```python
import math
import jax
import jax.numpy as jnp
import numpy as np
from jax import lax

D = 1024
HEADS = 16
HEAD_DIM = 64
F = 4096
FFE = 4096
MB = 2
LEN_DEV = 64
EXPERTS = 8
LEN = 256
SEQS = 4
CAP = 10
N_DP = 4


def draw_inputs(key, part):
    dims_all = (MB, SEQS, LEN, D)
    ramp_pos = (jnp.arange(SEQS, dtype=jnp.float32)[:, None] / SEQS + jnp.arange(LEN, dtype=jnp.float32)[None, :] / LEN) * 0.5
    raw_noise = jnp.clip(jax.random.normal(key, dims_all, jnp.float32), -4.0, 4.0)
    factor = jnp.exp(ramp_pos * math.log(3.0))
    return (raw_noise * factor[None, :, :, None]).astype(jnp.bfloat16)


def steps_of(key, extent, shards, least, top_value):
    def one(axis_at, blocks):
        draws = jax.random.uniform(jax.random.fold_in(jax.random.fold_in(key, 6), axis_at), (blocks,), jnp.float32, least / len(shards), top_value / len(shards))
        return jnp.repeat(jnp.exp(draws), extent[axis_at] // blocks).reshape((-1,) + (1,) * (len(extent) - axis_at - 1))

    level = one(*shards[0])
    for cut in shards[1:]:
        level = level * one(*cut)
    return level


def length_profile(amount, total, reach, slope):
    loads = [(1 << 20) // math.isqrt(standing ** slope) + 1 for standing in range(2, amount + 1)]
    rest, counts = total - reach - (amount - 1), [1] * (amount - 1)
    while rest > 0:
        candidates = [i for i in range(amount - 1) if counts[i] < reach]
        mass, left = sum([loads[i] for i in candidates]), rest
        for i in candidates:
            addition = min(reach - counts[i], max(1, left * loads[i] // mass), rest)
            counts[i] = counts[i] + addition
            rest = rest - addition
    return np.array([reach] + counts)


def uneven_parts(own_key, number_of, total, bound, lean):
    if number_of == 2:
        one = jax.random.randint(own_key, (), max(1, total - bound), min(bound, total - 1) + 1)
        return jnp.stack([one, total - one])
    lengths = jnp.asarray(length_profile(number_of, total, bound, lean), jnp.int32)
    pairs = (number_of - 1) // 2
    source_of, taker = lengths[1:1 + 2 * pairs:2], lengths[2:2 + 2 * pairs:2]
    margin = jnp.minimum(source_of - 1, bound - taker)
    shifted = jax.random.randint(jax.random.fold_in(own_key, 1), (pairs,), 0, 1 << 20) % (margin + 1)
    lengths = lengths.at[1:1 + 2 * pairs:2].set(source_of - shifted).at[2:2 + 2 * pairs:2].set(taker + shifted)
    return lengths[jax.random.permutation(jax.random.fold_in(own_key, 2), number_of)]


def shared_out(rng, own, number, rows, count, top, limit, skew):
    ranking = jax.random.permutation(rng, count)
    heavy_load, ordinary = load_shares(count, rows * top, limit, skew, True), load_shares(count, rows * top, limit, skew, False)
    places = jnp.arange(count)

    def named(tallies, rotation):
        used = int((tallies > 0).sum())
        fixed = max(1, used // 4)
        passed = fixed + (places - fixed + rotation * (used - fixed)) % max(1, count - fixed)
        return jnp.zeros((count,), jnp.int32).at[ranking[jnp.where(places < fixed, places, passed)]].set(jnp.asarray(tallies, jnp.int32))

    tallies = jnp.where(number % 4 == 0, named(heavy_load, number // 4), named(ordinary, number - number // 4 - 1))
    mixed = jax.random.permutation(jax.random.fold_in(own, 3), count)
    donor, receiver = mixed[0:count // 2 * 2:2], mixed[1:count // 2 * 2:2]
    room = jnp.minimum(tallies[donor] - 1, limit - tallies[receiver]) // 2
    room = jnp.where((donor == ranking[0]) | (receiver == ranking[0]) | (tallies[receiver] == 0), 0, jnp.maximum(room, 0))
    passed = jax.random.randint(jax.random.fold_in(own, 4), (count // 2,), 0, 1 << 20) % (room + 1)
    tallies = tallies.at[donor].add(-passed).at[receiver].add(passed)
    members = jnp.searchsorted(jnp.cumsum(tallies), jnp.arange(rows * top), side="right").astype(jnp.int32)
    table = members.reshape(top, rows).T
    table = table[jax.random.permutation(jax.random.fold_in(own, 1), rows)]
    rotation = jax.random.randint(jax.random.fold_in(own, 2), (rows, 1), 0, top)
    return jnp.take_along_axis(table, (jnp.arange(top)[None, :] + rotation) % top, axis=1)


def load_shares(count, total, reach, skew, full):
    weights = [(1 << 20) // math.isqrt(standing ** skew) + 1 for standing in range(1, count + 1)]
    largest = reach if full else min(reach, max(-(-total // count), total * weights[0] // sum(weights)))
    least = 1 if total - largest >= count - 1 else 0
    given, spare = [largest] + [least] * (count - 1), total - largest - least * (count - 1)
    while spare > 0:
        candidates = [i for i in range(1, count) if given[i] < largest] or [i for i in range(1, count) if given[i] < reach]
        mass, left = sum([weights[i] for i in candidates]), spare
        for i in candidates:
            extra = min(reach - given[i], max(1, left * weights[i] // mass), spare)
            given[i] = given[i] + extra
            spare = spare - extra
    return np.array(given)


def normal_values(own_key, dims, width, bound, split=(), held_as=jnp.bfloat16):
    result = width * jax.random.normal(own_key, dims, jnp.float32)
    if split:
        result = result * steps_of(own_key, dims, split, -0.22, 0.18)
    return jnp.clip(result, -bound, bound).astype(held_as)


def setup_inputs(seed: int = 0) -> dict:
    key_of = jax.random.split(jax.random.key(seed), 15)
    inputs = draw_inputs(jax.random.fold_in(key_of[14], 71), 0)
    cotangent = normal_values(key_of[1], (MB, SEQS, LEN, D), 1.0, 6.0, ((1, 4), (2, 4)))
    segment_ids = jax.vmap(lambda own: jnp.searchsorted(jnp.cumsum(uneven_parts(own, 4, LEN, LEN // 2, 2)), jnp.arange(LEN), side="right"))(jax.random.split(key_of[2], MB * SEQS)).reshape((MB, SEQS, LEN)).astype(jnp.int32)
    routes_keys = jax.random.split(jax.random.fold_in(key_of[3], 1), 2 * MB * SEQS * LEN // LEN_DEV)
    routes_turns = jax.random.permutation(jax.random.fold_in(key_of[3], 3), 2 * MB * SEQS * LEN // LEN_DEV)
    routes = jax.vmap(lambda own, number: shared_out(jax.random.fold_in(key_of[3], 2), own, number, LEN_DEV, EXPERTS, 1, CAP, 2))(routes_keys, routes_turns).reshape((2, MB, SEQS, LEN, 1))
    norm_gains = jnp.clip(1.0 + 0.1 * jax.random.normal(key_of[4], (2, 2, D), jnp.float32), 0.5, 1.5).astype(jnp.bfloat16)
    norm_shifts = normal_values(key_of[5], (2, 2, D), 0.2, 3.0, ((0, 2), (2, 16)))
    attn_qkv = normal_values(key_of[6], (2, D, 3 * D), D ** -0.5, 0.1875, ((0, 2), (1, 16)))
    attn_proj = normal_values(key_of[7], (2, D, D), (D // 16) ** -0.5, 0.75, ((0, 2), (1, 16)))
    dense_up = normal_values(key_of[8], (2, D, F), D ** -0.5, 0.1875, ((0, 2), (1, 16)))
    dense_down = normal_values(key_of[9], (2, F, D), F ** -0.5, 0.09375, ((0, 2), (1, 16)))
    router = normal_values(key_of[10], (2, D, EXPERTS), 0.016, 0.25, ((0, 2), (1, 16)))
    mixer = normal_values(key_of[11], (2, D, 2), 0.03, 0.4375, ((0, 2), (1, 16)))
    expert_up = normal_values(key_of[12], (2, EXPERTS, D, FFE), D ** -0.5, 0.1875, ((0, 2), (1, 4), (3, 4)))
    expert_down = normal_values(key_of[13], (2, EXPERTS, FFE, D), (2.25 * EXPERTS / FFE ** 0.5), 4.0, ((0, 2), (1, 4), (2, 4)))
    return {"inputs": inputs, "cotangent": cotangent, "segment_ids": segment_ids, "routes": routes, "norm_gains": norm_gains, "norm_shifts": norm_shifts, "attn_qkv": attn_qkv, "attn_proj": attn_proj, "dense_up": dense_up, "dense_down": dense_down, "router": router, "mixer": mixer, "expert_up": expert_up, "expert_down": expert_down}


exact_precision_mode = lax.Precision.HIGHEST

@jax.custom_vjp
def low(v):
    return lax.optimization_barrier(v.astype(jnp.bfloat16)).astype(jnp.float32)

@jax.custom_vjp
def low_back(v):
    return v

def low_keep(v):
    return (low(v), None)

def low_pass(kept, grad):
    return (grad,)

def back_keep(v):
    return (v, None)

def back_low(kept, grad):
    return (low(grad),)
low.defvjp(low_keep, low_pass)
low_back.defvjp(back_keep, back_low)

def matmul(left_mat, right_mat):
    return jnp.dot(left_mat, right_mat, precision=exact_precision_mode)

def layer_norm(value_rows, gain_vec, shift_vec):
    centre = lax.optimization_barrier(jnp.mean(value_rows, axis=-1, keepdims=True))
    centred = value_rows - centre
    variance = lax.optimization_barrier(jnp.mean(centred * centred, axis=-1, keepdims=True))
    return centred * lax.rsqrt(variance + 1e-05) * gain_vec + shift_vec

def gelu_tanh(value_rows):
    return jax.nn.gelu(value_rows, approximate=True)

def attend(packed):
    queries, keys_part, values_part, segments = packed
    seq_len = segments.shape[0]
    scores = low_back(jnp.einsum('ihd,jhd->hij', queries, keys_part, precision=exact_precision_mode) * 0.125)
    places = jnp.arange(seq_len, dtype=jnp.int32)
    allowed = (segments[:, None] == segments[None, :]) & (places[None, :] <= places[:, None])
    weights_soft = jax.nn.softmax(jnp.where(allowed[None], scores, -jnp.inf), axis=-1)
    heads_mixed = jnp.einsum('hij,jhd->ihd', low(weights_soft), values_part, precision=exact_precision_mode)
    return heads_mixed.reshape(seq_len, -1)

def expert_block(packed):
    token_row_block, up_mat, down_mat = packed
    hidden = low_back(matmul(token_row_block, up_mat))
    return low_back(low(matmul(low(gelu_tanh(hidden)), down_mat)))

def layer(value_rows, params, segment_ids, route_ids):
    norm_gain, norm_shift, w_qkv, w_proj, w_up, w_down, w_router, w_mix, exp_up, exp_down = params
    mb_count, seq_count, seq_len, model_width = value_rows.shape
    normed = low(layer_norm(value_rows, norm_gain[0], norm_shift[0]))
    qkv_low = low_back(low(matmul(normed, w_qkv)))
    qkv_heads = qkv_low.reshape(mb_count * seq_count, seq_len, 3, HEADS, HEAD_DIM)
    attended = lax.map(jax.checkpoint(attend), (qkv_heads[:, :, 0], qkv_heads[:, :, 1], qkv_heads[:, :, 2], segment_ids.reshape(mb_count * seq_count, seq_len)))
    attended = low_back(low(attended.reshape(value_rows.shape)))
    attn_branch = low_back(matmul(attended, w_proj))
    residual = value_rows + attn_branch
    mid_low = low(layer_norm(residual, norm_gain[1], norm_shift[1]))
    up_act = low_back(matmul(mid_low, w_up))
    dense_branch = low_back(matmul(low(gelu_tanh(up_act)), w_down))
    logits = low_back(matmul(mid_low, w_router))
    probs = jax.nn.softmax(logits, axis=-1)
    route_flat = route_ids[..., 0]
    one_hot = (route_flat[..., None] == jnp.arange(EXPERTS, dtype=jnp.int32)).astype(jnp.float32)
    gate = lax.optimization_barrier(jnp.sum(probs * one_hot, axis=-1, keepdims=True))
    coef = jax.nn.softmax(low_back(matmul(mid_low, w_mix)), axis=-1)
    blocks = mb_count * seq_count * N_DP
    token_row_block = low_back(mid_low).reshape(blocks, LEN_DEV, model_width)
    block_route = route_flat.reshape(blocks, LEN_DEV).astype(jnp.int32)
    hot_int = (block_route[..., None] == jnp.arange(EXPERTS, dtype=jnp.int32)).astype(jnp.int32)
    slot_rank = lax.optimization_barrier(jnp.sum((jnp.cumsum(hot_int, axis=1) - hot_int) * hot_int, axis=-1)).astype(jnp.int32)
    target = block_route * CAP + slot_rank
    slot_lookup_table = (jnp.arange(EXPERTS * CAP, dtype=jnp.int32)[None, :, None] == target[:, None, :]).astype(jnp.float32)
    holding_arrays = jnp.einsum('sir,srp->sip', slot_lookup_table, token_row_block, precision=exact_precision_mode)
    holding_arrays = holding_arrays.reshape(blocks, EXPERTS, CAP, model_width).transpose(1, 0, 2, 3).reshape(EXPERTS, blocks * CAP, model_width)
    expert_results = lax.map(jax.checkpoint(expert_block), (holding_arrays, exp_up, exp_down))
    expert_results = expert_results.reshape(EXPERTS, blocks, CAP, model_width).transpose(1, 0, 2, 3).reshape(blocks, EXPERTS * CAP, model_width)
    expert_path_output = jnp.einsum('vyn,vyg->vng', slot_lookup_table, expert_results, precision=exact_precision_mode).reshape(value_rows.shape)
    mlp_branch = coef[..., 0:1] * dense_branch + coef[..., 1:2] * gate * expert_path_output
    output = residual + mlp_branch
    branch_stats = jnp.sqrt(jnp.stack([jnp.mean(attn_branch * attn_branch), jnp.mean(mlp_branch * mlp_branch), jnp.mean(output * output)]))
    return (output, branch_stats)

def reference(inputs, cotangent, segment_ids, routes, norm_gains, norm_shifts, attn_qkv, attn_proj, dense_up, dense_down, router, mixer, expert_up, expert_down):
    weight_list = (norm_gains, norm_shifts, attn_qkv, attn_proj, dense_up, dense_down, router, mixer, expert_up, expert_down)

    def section_params(index):
        return tuple((weight_arr[index].astype(jnp.float32) for weight_arr in weight_list))
    first_out, first_back, first_stats = jax.vjp(lambda value_rows, *params: layer(value_rows, params, segment_ids, routes[0]), inputs.astype(jnp.float32), *section_params(0), has_aux=True)
    second_in = low(first_out)
    second_out, second_back, second_stats = jax.vjp(lambda value_rows, *params: layer(value_rows, params, segment_ids, routes[1]), second_in, *section_params(1), has_aux=True)
    second_grads = second_back(cotangent.astype(jnp.float32))
    first_grads = first_back(low(second_grads[0]))
    grads = [jnp.stack([first_grad, second_grad]) for first_grad, second_grad in zip(first_grads[1:], second_grads[1:])]
    activations = jnp.stack([first_out, second_out]).astype(jnp.bfloat16)
    input_grads = jnp.stack([first_grads[0], second_grads[0]])
    branch_rms = jnp.stack([first_stats, second_stats])
    return (activations, input_grads, grads[0], grads[1], grads[2], grads[3], grads[4], grads[5], grads[6], grads[7], grads[8], grads[9], branch_rms)
```

```python
import jax
import jax.numpy as jnp
from jax import lax
from jax.sharding import PartitionSpec as P

HEADS = 16
HEAD_DIM = 64
EVERY = ("section", "expert", "dp")
HOMES = ("section", "expert")


def layer_norm(value_rows, gain_vec, shift_vec):
    centre = jnp.mean(value_rows, axis=-1, keepdims=True)
    centred = value_rows - centre
    variance = jnp.mean(centred * centred, axis=-1, keepdims=True)
    return centred * lax.rsqrt(variance + 1e-05) * gain_vec + shift_vec


def gelu_tanh(value_rows):
    return jax.nn.gelu(value_rows, approximate=True)


def gelu_grad(value_rows, grad_in):
    return jax.vjp(gelu_tanh, value_rows)[1](grad_in)[0]


def product(left_mat, right_mat):
    return jnp.dot(left_mat, right_mat, preferred_element_type=jnp.float32)


def product_tn(left_mat, right_mat):
    return lax.dot_general(
        left_mat, right_mat, (((0,), (0,)), ((), ())), preferred_element_type=jnp.float32
    )


def product_nt(left_mat, right_mat):
    return lax.dot_general(
        left_mat, right_mat, (((1,), (1,)), ((), ())), preferred_element_type=jnp.float32
    )


def low(values):
    return values.astype(jnp.bfloat16)


def exchange(blocks, axes):
    return lax.all_to_all(blocks, axes, split_axis=0, concat_axis=0, tiled=True)


def spread(block, axes):
    count = lax.axis_size(axes)
    return exchange(jnp.broadcast_to(block[None], (count,) + block.shape), axes)


def gather_rows(block):
    return lax.all_gather(block, "dp", axis=0, tiled=True)


def sum_blocks(blocks):
    return jnp.sum(blocks.astype(jnp.float32), axis=0)


def scatter_rows(partial_rows):
    count = lax.axis_size("dp")
    blocks = low(partial_rows).reshape(count, -1, partial_rows.shape[-1])
    return sum_blocks(exchange(blocks, "dp"))


def other_core(block):
    return lax.ppermute(block, "section", [(0, 1), (1, 0)])


def both_cores(block):
    return jnp.concatenate([block, other_core(block)], axis=0)


def halves_for_cores(block, section_id):
    half = block.shape[1] // 2
    kept = lax.dynamic_slice_in_dim(block, section_id * half, half, axis=1)
    sent = lax.dynamic_slice_in_dim(block, (1 - section_id) * half, half, axis=1)
    return jnp.concatenate([kept, other_core(sent)], axis=0)


def shards(
    inputs,
    cotangent,
    segment_ids,
    routes,
    norm_gains,
    norm_shifts,
    attn_qkv,
    attn_proj,
    dense_up,
    dense_down,
    router,
    mixer,
    expert_up,
    expert_down,
):
    sections = lax.axis_size("section")
    groups = lax.axis_size("expert")
    dp_size = lax.axis_size("dp")
    section_id = lax.axis_index("section")
    expert_id = lax.axis_index("expert")
    micro_count = inputs.shape[0]
    seq_rows = inputs.shape[2]
    width = inputs.shape[3]
    full_len = segment_ids.shape[2]
    experts_total = router.shape[2]
    hidden_rows = dense_down.shape[1]
    weight_rows = attn_qkv.shape[1]
    heads_here = HEADS // dp_size
    head_width = heads_here * HEAD_DIM
    capacity = max(2, 5 * seq_rows // (4 * experts_total))
    slots = dp_size * capacity
    devices = sections * groups * dp_size

    small_parts = jnp.concatenate([norm_gains[0], norm_shifts[0], router[0].T, mixer[0].T], axis=0)
    small_count = small_parts.shape[0]
    route_row = low(routes[0, :, 0, :, 0])
    message = jnp.concatenate([small_parts.reshape(-1), route_row.reshape(-1)])
    filled = message.shape[0]
    padded = -(-filled // 1024) * 1024
    message = jnp.pad(message, (0, padded - filled)).reshape(padded // 128, 128)
    small_all = spread(message, EVERY).reshape(sections, groups, dp_size, padded)
    params_all = small_all[..., : small_count * weight_rows].reshape(
        sections, groups * dp_size, small_count, weight_rows
    )
    params_all = params_all.transpose(0, 2, 1, 3).reshape(sections, small_count, width)
    routes_all = lax.dynamic_index_in_dim(
        small_all[..., small_count * weight_rows : filled], expert_id, 1, keepdims=False
    ).reshape(sections, dp_size, micro_count, seq_rows)
    routes_all = lax.dynamic_index_in_dim(routes_all, section_id, 2, keepdims=False)
    routes_all = routes_all.astype(jnp.int32)

    qkv_cols = attn_qkv[0].reshape(weight_rows, 3, dp_size, head_width).transpose(2, 0, 1, 3)
    qkv_cols = exchange(qkv_cols.reshape(dp_size, weight_rows, 3 * head_width), "dp")
    qkv_both = spread(spread(qkv_cols, "expert").reshape(width, 3 * head_width), "section")
    proj_rows = exchange(
        jnp.broadcast_to(attn_proj, (dp_size,) + attn_proj.shape[1:]), "dp"
    ).reshape(dp_size * weight_rows, width)
    proj_both = spread(spread(proj_rows, "expert").reshape(width, width), "section")
    up_cols = dense_up[0].reshape(weight_rows, groups, dp_size, hidden_rows).transpose(2, 0, 1, 3)
    hidden_here = groups * hidden_rows
    up_cols = exchange(up_cols.reshape(dp_size, weight_rows, hidden_here), "dp")
    up_both = spread(spread(up_cols, "expert").reshape(width, hidden_here), "section")
    down_both = spread(spread(dense_down[0], "expert").reshape(hidden_here, width), "section")
    exp_up_both = exchange(expert_up[0], "section")
    exp_down_both = exchange(expert_down[0], "section")

    segments = lax.dynamic_index_in_dim(segment_ids[:, 0], section_id, 0, keepdims=False)
    places = jnp.arange(full_len, dtype=jnp.int32)
    allowed = (segments[:, None] == segments[None, :]) & (places[None, :] <= places[:, None])
    earlier = (places[None, :] < places[:, None]) & (
        places[None, :] // seq_rows == places[:, None] // seq_rows
    )

    def slot_table(route_now):
        rank = jnp.sum(
            ((route_now[:, None] == route_now[None, :]) & earlier).astype(jnp.int32), axis=1
        )
        home = route_now % sections * groups + route_now // sections
        target = home * slots + places // seq_rows * capacity + rank
        slot_ids = jnp.arange(sections * groups * slots, dtype=jnp.int32)
        table = low(slot_ids[:, None] == target[None, :])
        hot = route_now[:, None] == jnp.arange(experts_total, dtype=jnp.int32)[None, :]
        return table, hot.astype(jnp.float32)

    def to_experts(token_rows, table):
        packed = low(product(table, token_rows)).reshape(sections * groups, slots, width)
        return exchange(packed, HOMES).reshape(-1, width)

    def from_experts(expert_rows, table):
        returned = exchange(low(expert_rows).reshape(sections * groups, slots, width), HOMES)
        return product_tn(table, returned.reshape(-1, width))

    def heads_of(columns):
        return columns.reshape(-1, heads_here, HEAD_DIM)

    def split_heads(packed):
        return [heads_of(packed[:, i * head_width : (i + 1) * head_width]) for i in range(3)]

    def forward_layer(layer, layer_in):
        params = params_all[layer].astype(jnp.float32)
        table, hot = slot_table(routes_all[layer].reshape(full_len))
        normed = low(layer_norm(layer_in, params[0:1], params[2:3]))
        normed_seq = gather_rows(normed)
        qkv = low(product(normed_seq, qkv_both[layer]))
        queries, keys, values = split_heads(qkv)
        scores = jnp.einsum("ihd,jhd->hij", queries, keys, preferred_element_type=jnp.float32)
        scores = jnp.where(allowed[None], scores * 0.125, -jnp.inf)
        exp_scores = jnp.exp(scores - jnp.max(scores, axis=-1, keepdims=True))
        probs = exp_scores / jnp.sum(exp_scores, axis=-1, keepdims=True)
        probs_low = low(probs)
        mixed = jnp.einsum("hij,jhd->ihd", probs_low, values, preferred_element_type=jnp.float32)
        mixed = exchange(low(mixed).reshape(dp_size, seq_rows, head_width), "dp")
        mixed = mixed.transpose(1, 0, 2).reshape(seq_rows, width)
        attn_branch = product(mixed, proj_both[layer])
        residual = layer_in + attn_branch
        mid_seq = gather_rows(low(layer_norm(residual, params[1:2], params[3:4])))
        expert_rows = to_experts(mid_seq, table)
        small_weights = params_all[layer, 4:]
        small_logits = product_nt(mid_seq, small_weights)
        gate_probs = jax.nn.softmax(small_logits[:, :experts_total], axis=-1)
        gate = jnp.sum(gate_probs * hot, axis=-1, keepdims=True)
        coef = jax.nn.softmax(small_logits[:, experts_total:], axis=-1)
        hidden = product(mid_seq, up_both[layer])
        hidden_low = low(gelu_tanh(hidden))
        dense_part = product(hidden_low, down_both[layer])
        exp_hidden = product(expert_rows, exp_up_both[layer])
        exp_hidden_low = low(gelu_tanh(exp_hidden))
        expert_part = from_experts(product(exp_hidden_low, exp_down_both[layer]), table)
        branch = scatter_rows(coef[:, 0:1] * dense_part + coef[:, 1:2] * gate * expert_part)
        layer_out = residual + branch
        squares = jnp.stack(
            [
                jnp.sum(attn_branch * attn_branch),
                jnp.sum(branch * branch),
                jnp.sum(layer_out * layer_out),
            ]
        )
        record = {
            "params": params,
            "small_weights": small_weights,
            "table": table,
            "hot": hot,
            "layer_in": layer_in,
            "normed_seq": normed_seq,
            "qkv": qkv,
            "probs": probs,
            "probs_low": probs_low,
            "mixed": mixed,
            "residual": residual,
            "mid_seq": mid_seq,
            "expert_rows": expert_rows,
            "gate_probs": gate_probs,
            "gate": gate,
            "coef": coef,
            "hidden": hidden,
            "hidden_low": hidden_low,
            "dense_part": dense_part,
            "exp_hidden": exp_hidden,
            "exp_hidden_low": exp_hidden_low,
            "expert_part": expert_part,
        }
        return layer_out, squares, record

    def backward_layer(layer, grad_low, record):
        grad_out = grad_low.astype(jnp.float32)
        params = record["params"]
        coef, gate, table = record["coef"], record["gate"], record["table"]
        grad_seq = gather_rows(grad_low).astype(jnp.float32)
        d_dense = low(coef[:, 0:1] * grad_seq)
        d_expert = low(coef[:, 1:2] * gate * grad_seq)
        expert_grad_rows = to_experts(d_expert, table)
        dense_dot = jnp.sum(grad_seq * record["dense_part"], axis=-1, keepdims=True)
        expert_dot = jnp.sum(grad_seq * record["expert_part"], axis=-1, keepdims=True)
        d_coef = jnp.concatenate([dense_dot, gate * expert_dot], axis=1)
        d_mix = coef * (d_coef - jnp.sum(coef * d_coef, axis=-1, keepdims=True))
        d_logits = record["gate_probs"] * (record["hot"] - gate) * (coef[:, 1:2] * expert_dot)
        d_small = low(jnp.concatenate([d_logits, d_mix], axis=1))
        d_up = low(gelu_grad(record["hidden"], product_nt(d_dense, down_both[layer])))
        d_mid_part = product_nt(d_up, up_both[layer]) + product(d_small, record["small_weights"])
        d_exp_hidden = gelu_grad(
            record["exp_hidden"], product_nt(expert_grad_rows, exp_down_both[layer])
        )
        d_exp_hidden = low(d_exp_hidden)
        d_mid_part = d_mid_part + from_experts(
            product_nt(d_exp_hidden, exp_up_both[layer]), table
        )
        d_mid = scatter_rows(d_mid_part)
        g_exp_up = product_tn(record["expert_rows"], d_exp_hidden)
        g_exp_down = product_tn(record["exp_hidden_low"], expert_grad_rows)
        mid_both = both_cores(record["mid_seq"])
        g_up = product_tn(mid_both, halves_for_cores(d_up, section_id))
        g_down = product_tn(
            both_cores(record["hidden_low"]), halves_for_cores(d_dense, section_id)
        )
        g_small = product_tn(d_small, record["mid_seq"])
        norm_back = jax.vjp(layer_norm, record["residual"], params[1:2], params[3:4])[1]
        d_resid_norm, d_gain_one, d_shift_one = norm_back(d_mid)
        d_resid = grad_out + d_resid_norm
        d_attn = low(d_resid)
        g_proj = product_tn(both_cores(record["mixed"]), halves_for_cores(d_attn, section_id))
        d_mixed = low(product_nt(d_attn, proj_both[layer]))
        d_mixed = d_mixed.reshape(seq_rows, dp_size, head_width).transpose(1, 0, 2)
        d_mixed = heads_of(exchange(d_mixed, "dp").reshape(full_len, head_width))
        queries, keys, values = split_heads(record["qkv"])
        probs = record["probs"]
        d_values = jnp.einsum(
            "hij,ihd->jhd", record["probs_low"], d_mixed, preferred_element_type=jnp.float32
        )
        d_probs = jnp.einsum("ihd,jhd->hij", d_mixed, values, preferred_element_type=jnp.float32)
        d_scores = low(probs * (d_probs - jnp.sum(probs * d_probs, axis=-1, keepdims=True)))
        d_queries = jnp.einsum(
            "hij,jhd->ihd", d_scores, keys, preferred_element_type=jnp.float32
        )
        d_keys = jnp.einsum(
            "hij,ihd->jhd", d_scores, queries, preferred_element_type=jnp.float32
        )
        d_qkv = low(
            jnp.concatenate(
                [
                    (d_queries * 0.125).reshape(full_len, head_width),
                    (d_keys * 0.125).reshape(full_len, head_width),
                    d_values.reshape(full_len, head_width),
                ],
                axis=1,
            )
        )
        d_normed = scatter_rows(product_nt(d_qkv, qkv_both[layer]))
        g_qkv = product_tn(
            both_cores(record["normed_seq"]), halves_for_cores(d_qkv, section_id)
        )
        first_back = jax.vjp(layer_norm, record["layer_in"], params[0:1], params[2:3])[1]
        d_input_norm, d_gain_zero, d_shift_zero = first_back(d_normed)
        small_grads = jnp.concatenate(
            [d_gain_zero, d_gain_one, d_shift_zero, d_shift_one, g_small], axis=0
        )

        def over_expert(grad_mat):
            blocks = low(grad_mat).reshape(groups, -1, grad_mat.shape[-1])
            return sum_blocks(exchange(blocks, "expert"))

        def over_dp(grad_mat):
            blocks = low(grad_mat).reshape(dp_size, weight_rows, grad_mat.shape[-1])
            return exchange(blocks, "dp")

        reduced = {
            "qkv": over_dp(over_expert(g_qkv)),
            "proj": sum_blocks(over_dp(over_expert(g_proj))),
            "up": over_dp(over_expert(g_up)),
            "down": over_expert(g_down),
        }
        return d_resid + d_input_norm, reduced, small_grads, g_exp_up, g_exp_down

    own_input = lax.dynamic_index_in_dim(inputs[:, 0], section_id, 0, keepdims=False)
    own_grad = lax.dynamic_index_in_dim(cotangent[:, 0], section_id, 0, keepdims=False)
    out_zero, squares_zero, record_zero = forward_layer(0, own_input.astype(jnp.float32))
    out_zero = low(out_zero)
    out_one, squares_one, record_one = forward_layer(1, out_zero.astype(jnp.float32))
    grad_one, reduced_one, small_one, exp_up_one, exp_down_one = backward_layer(
        1, own_grad, record_one
    )
    grad_zero, reduced_zero, small_zero, exp_up_zero, exp_down_zero = backward_layer(
        0, low(grad_one), record_zero
    )

    def to_owner(layer_zero, layer_one):
        return exchange(jnp.stack([layer_zero, layer_one]), "section")

    activations = to_owner(out_zero, low(out_one))
    input_grads = to_owner(grad_zero, grad_one)
    grad_exp_up = to_owner(exp_up_zero, exp_up_one)
    grad_exp_down = to_owner(exp_down_zero, exp_down_one)
    joined = {
        name: to_owner(reduced_zero[name].astype(jnp.float32), reduced_one[name].astype(jnp.float32))
        for name in reduced_zero
    }
    grad_qkv = joined["qkv"].transpose(2, 1, 0, 3).reshape(weight_rows, dp_size, 3, head_width)
    grad_qkv = grad_qkv.transpose(0, 2, 1, 3).reshape(weight_rows, 3 * width)
    grad_up = joined["up"].reshape(sections, dp_size, weight_rows, groups // sections, hidden_rows)
    grad_up = grad_up.transpose(2, 0, 3, 1, 4).reshape(weight_rows, -1)
    grad_proj = joined["proj"].transpose(1, 0, 2).reshape(weight_rows, width)
    grad_down = joined["down"].transpose(1, 0, 2).reshape(hidden_rows, width)

    small_grads = jnp.stack([small_zero, small_one]).reshape(
        sections, small_count, groups * dp_size, weight_rows
    )
    small_grads = small_grads.transpose(0, 2, 1, 3).reshape(
        sections, groups * dp_size, small_count * weight_rows
    )
    squares = jnp.stack([squares_zero, squares_one])
    squares = jnp.broadcast_to(squares[:, None], (sections, groups * dp_size, 3))
    small_message = jnp.concatenate([small_grads, squares], axis=-1)
    filled_back = small_message.shape[-1]
    padded_back = -(-filled_back // 1024) * 1024
    small_message = jnp.pad(small_message, ((0, 0), (0, 0), (0, padded_back - filled_back)))
    small_sum = sum_blocks(
        exchange(small_message.reshape(devices, padded_back // 128, 128), EVERY)
    ).reshape(-1)
    sums = small_sum[: small_count * weight_rows].reshape(small_count, weight_rows)
    totals = small_sum[small_count * weight_rows : filled_back]
    element_count = micro_count * seq_rows * width * groups * dp_size
    branch_rms = jnp.sqrt(totals / element_count)[None]
    return (
        activations[None, :, None],
        input_grads[None, :, None],
        sums[None, 0:2],
        sums[None, 2:4],
        grad_qkv[None],
        grad_proj[None],
        grad_up[None],
        grad_down[None],
        sums[4 : 4 + experts_total].T[None],
        sums[4 + experts_total :].T[None],
        grad_exp_up[None],
        grad_exp_down[None],
        branch_rms,
    )


def solution(mesh):
    placed = (
        P(None, "expert", "dp", None),
        P(None, "expert", "dp", None),
        P(None, "expert", None),
        P("section", None, "expert", "dp", None),
        P("section", None, ("expert", "dp")),
        P("section", None, ("expert", "dp")),
        P("section", ("expert", "dp"), None),
        P("section", ("expert", "dp"), None),
        P("section", ("expert", "dp"), None),
        P("section", ("expert", "dp"), None),
        P("section", ("expert", "dp"), None),
        P("section", ("expert", "dp"), None),
        P("section", "expert", None, "dp"),
        P("section", "expert", "dp", None),
    )
    return jax.shard_map(
        shards,
        mesh=mesh,
        in_specs=placed,
        out_specs=(
            P("section", None, "expert", "dp", None),
            P("section", None, "expert", "dp", None),
            P("section", None, ("expert", "dp")),
            P("section", None, ("expert", "dp")),
            P("section", ("expert", "dp"), None),
            P("section", ("expert", "dp"), None),
            P("section", ("expert", "dp"), None),
            P("section", ("expert", "dp"), None),
            P("section", ("expert", "dp"), None),
            P("section", ("expert", "dp"), None),
            P("section", "expert", None, "dp"),
            P("section", "expert", "dp", None),
            P("section", None),
        ),
        check_vma=False,
    )
```

```python
import jax
import jax.numpy as jnp
from jax import lax
from jax.sharding import PartitionSpec as P

HEADS = 16
HEAD_DIM = 64
EVERY = ("section", "expert", "dp")
HOMES = ("section", "expert")


def layer_norm(value_rows, gain_vec, shift_vec):
    centre = jnp.mean(value_rows, axis=-1, keepdims=True)
    centred = value_rows - centre
    variance = jnp.mean(centred * centred, axis=-1, keepdims=True)
    return centred * lax.rsqrt(variance + 1e-05) * gain_vec + shift_vec


def gelu_tanh(value_rows):
    return jax.nn.gelu(value_rows, approximate=True)


def gelu_grad(value_rows, grad_in):
    return jax.vjp(gelu_tanh, value_rows)[1](grad_in)[0]


def product(left_mat, right_mat):
    return jnp.dot(left_mat, right_mat, preferred_element_type=jnp.float32)


def product_tn(left_mat, right_mat):
    return lax.dot_general(
        left_mat, right_mat, (((0,), (0,)), ((), ())), preferred_element_type=jnp.float32
    )


def product_nt(left_mat, right_mat):
    return lax.dot_general(
        left_mat, right_mat, (((1,), (1,)), ((), ())), preferred_element_type=jnp.float32
    )


def low(values):
    return values.astype(jnp.bfloat16)


def exchange(blocks, axes):
    return lax.all_to_all(blocks, axes, split_axis=0, concat_axis=0, tiled=True)


def spread(block, axes):
    count = lax.axis_size(axes)
    return exchange(jnp.broadcast_to(block[None], (count,) + block.shape), axes)


def gather_rows(block):
    return lax.all_gather(block, "dp", axis=0, tiled=True)


def sum_blocks(blocks):
    return jnp.sum(blocks.astype(jnp.float32), axis=0)


def scatter_rows(partial_rows):
    count = lax.axis_size("dp")
    blocks = low(partial_rows).reshape(count, -1, partial_rows.shape[-1])
    return sum_blocks(exchange(blocks, "dp"))


def other_core(block):
    return lax.ppermute(block, "section", [(0, 1), (1, 0)])


def place_blocks(blocks, index_of):
    placed = jnp.zeros((len(blocks),) + blocks[0].shape, blocks[0].dtype)
    for step, block in enumerate(blocks):
        placed = lax.dynamic_update_index_in_dim(placed, block, index_of(step), 0)
    return placed


def permute_spread(block, axis):
    count = lax.axis_size(axis)
    place = lax.axis_index(axis)
    blocks = [block]
    for step in range(1, count):
        route = [((i - step) % count, i) for i in range(count)]
        blocks.append(lax.ppermute(block, axis, route))
    return place_blocks(blocks, lambda step: (place - step) % count)


def permute_parts(blocks, axis):
    count = lax.axis_size(axis)
    place = lax.axis_index(axis)
    parts = [lax.dynamic_index_in_dim(blocks, place, 0, keepdims=False)]
    for step in range(1, count):
        route = [((i - step) % count, i) for i in range(count)]
        part = lax.dynamic_index_in_dim(blocks, (place + step) % count, 0, keepdims=False)
        parts.append(lax.ppermute(part, axis, route))
    return parts


def permute_exchange(blocks, axis):
    count = lax.axis_size(axis)
    place = lax.axis_index(axis)
    return place_blocks(permute_parts(blocks, axis), lambda step: (place - step) % count)


def permute_sum(blocks, axis):
    return sum(part.astype(jnp.float32) for part in permute_parts(blocks, axis))


def both_cores(block):
    return jnp.concatenate([block, other_core(block)], axis=0)


def halves_for_cores(block, section_id):
    half = block.shape[1] // 2
    kept = lax.dynamic_slice_in_dim(block, section_id * half, half, axis=1)
    sent = lax.dynamic_slice_in_dim(block, (1 - section_id) * half, half, axis=1)
    return jnp.concatenate([kept, other_core(sent)], axis=0)


def shards(
    inputs,
    cotangent,
    segment_ids,
    routes,
    norm_gains,
    norm_shifts,
    attn_qkv,
    attn_proj,
    dense_up,
    dense_down,
    router,
    mixer,
    expert_up,
    expert_down,
):
    sections = lax.axis_size("section")
    groups = lax.axis_size("expert")
    dp_size = lax.axis_size("dp")
    section_id = lax.axis_index("section")
    expert_id = lax.axis_index("expert")
    micro_count = inputs.shape[0]
    seq_rows = inputs.shape[2]
    width = inputs.shape[3]
    full_len = segment_ids.shape[2]
    experts_total = router.shape[2]
    hidden_rows = dense_down.shape[1]
    weight_rows = attn_qkv.shape[1]
    heads_here = HEADS // dp_size
    head_width = heads_here * HEAD_DIM
    capacity = max(2, 5 * seq_rows // (4 * experts_total))
    slots = dp_size * capacity
    devices = sections * groups * dp_size

    small_parts = jnp.concatenate([norm_gains[0], norm_shifts[0], router[0].T, mixer[0].T], axis=0)
    small_count = small_parts.shape[0]
    route_row = low(routes[0, :, 0, :, 0])
    message = jnp.concatenate([small_parts.reshape(-1), route_row.reshape(-1)])
    filled = message.shape[0]
    padded = -(-filled // 1024) * 1024
    message = jnp.pad(message, (0, padded - filled)).reshape(padded // 128, 128)
    small_all = spread(message, EVERY).reshape(sections, groups, dp_size, padded)
    params_all = small_all[..., : small_count * weight_rows].reshape(
        sections, groups * dp_size, small_count, weight_rows
    )
    params_all = params_all.transpose(0, 2, 1, 3).reshape(sections, small_count, width)
    routes_all = lax.dynamic_index_in_dim(
        small_all[..., small_count * weight_rows : filled], expert_id, 1, keepdims=False
    ).reshape(sections, dp_size, micro_count, seq_rows)
    routes_all = lax.dynamic_index_in_dim(routes_all, section_id, 2, keepdims=False)
    routes_all = routes_all.astype(jnp.int32)

    on_first = section_id == 0

    def by_layer(of_own_layer, of_other_layer):
        return (
            jnp.where(on_first, of_own_layer, of_other_layer),
            jnp.where(on_first, of_other_layer, of_own_layer),
        )

    qkv_cols = attn_qkv[0].reshape(weight_rows, 3, dp_size, head_width).transpose(2, 0, 1, 3)
    qkv_cols = exchange(qkv_cols.reshape(dp_size, weight_rows, 3 * head_width), "dp")
    qkv_own = spread(qkv_cols, "expert").reshape(width, 3 * head_width)
    qkv_both = by_layer(qkv_own, other_core(qkv_own))
    proj_own = spread(permute_spread(attn_proj[0], "dp"), "expert").reshape(width, width)
    proj_both = by_layer(proj_own, other_core(proj_own))
    hidden_here = groups * hidden_rows
    down_both = lax.all_gather(dense_down[0], HOMES, axis=0, tiled=True)
    down_both = down_both.reshape(sections, hidden_here, width)
    up_cols = dense_up[0].reshape(weight_rows, groups, dp_size, hidden_rows).transpose(2, 0, 1, 3)
    up_cols = permute_exchange(up_cols.reshape(dp_size, weight_rows, hidden_here), "dp")
    up_cols = up_cols.reshape(dp_size * weight_rows, hidden_here)
    up_both = lax.all_gather(up_cols, HOMES, axis=0, tiled=True)
    up_both = up_both.reshape(sections, width, hidden_here)

    def expert_of_layers(own_layer):
        kept = lax.dynamic_index_in_dim(own_layer, section_id, 0, keepdims=False)
        sent = lax.dynamic_index_in_dim(own_layer, 1 - section_id, 0, keepdims=False)
        return by_layer(kept, other_core(sent))

    exp_up_both = expert_of_layers(expert_up[0])
    exp_down_both = expert_of_layers(expert_down[0])

    segments = lax.dynamic_index_in_dim(segment_ids[:, 0], section_id, 0, keepdims=False)
    places = jnp.arange(full_len, dtype=jnp.int32)
    allowed = (segments[:, None] == segments[None, :]) & (places[None, :] <= places[:, None])
    earlier = (places[None, :] < places[:, None]) & (
        places[None, :] // seq_rows == places[:, None] // seq_rows
    )

    def slot_table(route_now):
        rank = jnp.sum(
            ((route_now[:, None] == route_now[None, :]) & earlier).astype(jnp.int32), axis=1
        )
        home = route_now % sections * groups + route_now // sections
        target = home * slots + places // seq_rows * capacity + rank
        slot_ids = jnp.arange(sections * groups * slots, dtype=jnp.int32)
        table = low(slot_ids[:, None] == target[None, :])
        hot = route_now[:, None] == jnp.arange(experts_total, dtype=jnp.int32)[None, :]
        return table, hot.astype(jnp.float32)

    def to_experts(token_rows, table):
        packed = low(product(table, token_rows)).reshape(sections * groups, slots, width)
        return exchange(packed, HOMES).reshape(-1, width)

    def from_experts(expert_rows, table):
        returned = exchange(low(expert_rows).reshape(sections * groups, slots, width), HOMES)
        return product_tn(table, returned.reshape(-1, width))

    def heads_of(columns):
        return columns.reshape(-1, heads_here, HEAD_DIM)

    def split_heads(packed):
        return [heads_of(packed[:, i * head_width : (i + 1) * head_width]) for i in range(3)]

    def forward_layer(layer, layer_in):
        params = params_all[layer].astype(jnp.float32)
        table, hot = slot_table(routes_all[layer].reshape(full_len))
        normed = low(layer_norm(layer_in, params[0:1], params[2:3]))
        normed_seq = gather_rows(normed)
        qkv = low(product(normed_seq, qkv_both[layer]))
        queries, keys, values = split_heads(qkv)
        scores = jnp.einsum("ihd,jhd->hij", queries, keys, preferred_element_type=jnp.float32)
        scores = jnp.where(allowed[None], scores * 0.125, -jnp.inf)
        exp_scores = jnp.exp(scores - jnp.max(scores, axis=-1, keepdims=True))
        probs = exp_scores / jnp.sum(exp_scores, axis=-1, keepdims=True)
        probs_low = low(probs)
        mixed = jnp.einsum("hij,jhd->ihd", probs_low, values, preferred_element_type=jnp.float32)
        mixed = exchange(low(mixed).reshape(dp_size, seq_rows, head_width), "dp")
        mixed = mixed.transpose(1, 0, 2).reshape(seq_rows, width)
        attn_branch = product(mixed, proj_both[layer])
        residual = layer_in + attn_branch
        mid_seq = gather_rows(low(layer_norm(residual, params[1:2], params[3:4])))
        expert_rows = to_experts(mid_seq, table)
        small_weights = params_all[layer, 4:]
        small_logits = product_nt(mid_seq, small_weights)
        gate_probs = jax.nn.softmax(small_logits[:, :experts_total], axis=-1)
        gate = jnp.sum(gate_probs * hot, axis=-1, keepdims=True)
        coef = jax.nn.softmax(small_logits[:, experts_total:], axis=-1)
        hidden = product(mid_seq, up_both[layer])
        hidden_low = low(gelu_tanh(hidden))
        dense_part = product(hidden_low, down_both[layer])
        exp_hidden = product(expert_rows, exp_up_both[layer])
        exp_hidden_low = low(gelu_tanh(exp_hidden))
        expert_part = from_experts(product(exp_hidden_low, exp_down_both[layer]), table)
        branch = scatter_rows(coef[:, 0:1] * dense_part + coef[:, 1:2] * gate * expert_part)
        layer_out = residual + branch
        squares = jnp.stack(
            [
                jnp.sum(attn_branch * attn_branch),
                jnp.sum(branch * branch),
                jnp.sum(layer_out * layer_out),
            ]
        )
        record = {
            "params": params,
            "small_weights": small_weights,
            "table": table,
            "hot": hot,
            "layer_in": layer_in,
            "normed_seq": normed_seq,
            "qkv": qkv,
            "probs": probs,
            "probs_low": probs_low,
            "mixed": mixed,
            "residual": residual,
            "mid_seq": mid_seq,
            "expert_rows": expert_rows,
            "gate_probs": gate_probs,
            "gate": gate,
            "coef": coef,
            "hidden": hidden,
            "hidden_low": hidden_low,
            "dense_part": dense_part,
            "exp_hidden": exp_hidden,
            "exp_hidden_low": exp_hidden_low,
            "expert_part": expert_part,
        }
        return layer_out, squares, record

    def backward_layer(layer, grad_low, grad_seq, record):
        grad_out = grad_low.astype(jnp.float32)
        params = record["params"]
        coef, gate, table = record["coef"], record["gate"], record["table"]
        grad_seq = grad_seq.astype(jnp.float32)
        d_dense = low(coef[:, 0:1] * grad_seq)
        d_expert = low(coef[:, 1:2] * gate * grad_seq)
        expert_grad_rows = to_experts(d_expert, table)
        dense_dot = jnp.sum(grad_seq * record["dense_part"], axis=-1, keepdims=True)
        expert_dot = jnp.sum(grad_seq * record["expert_part"], axis=-1, keepdims=True)
        d_coef = jnp.concatenate([dense_dot, gate * expert_dot], axis=1)
        d_mix = coef * (d_coef - jnp.sum(coef * d_coef, axis=-1, keepdims=True))
        d_logits = record["gate_probs"] * (record["hot"] - gate) * (coef[:, 1:2] * expert_dot)
        d_small = low(jnp.concatenate([d_logits, d_mix], axis=1))
        d_up = low(gelu_grad(record["hidden"], product_nt(d_dense, down_both[layer])))
        d_mid_part = product_nt(d_up, up_both[layer]) + product(d_small, record["small_weights"])
        d_exp_hidden = gelu_grad(
            record["exp_hidden"], product_nt(expert_grad_rows, exp_down_both[layer])
        )
        d_exp_hidden = low(d_exp_hidden)
        d_mid_part = d_mid_part + from_experts(
            product_nt(d_exp_hidden, exp_up_both[layer]), table
        )
        d_mid = scatter_rows(d_mid_part)
        expert_operands = (
            record["expert_rows"],
            d_exp_hidden,
            record["exp_hidden_low"],
            expert_grad_rows,
        )
        mid_both = both_cores(record["mid_seq"])
        g_up = product_tn(mid_both, halves_for_cores(d_up, section_id))
        g_down = product_tn(
            both_cores(record["hidden_low"]), halves_for_cores(d_dense, section_id)
        )
        g_small = product_tn(d_small, record["mid_seq"])
        norm_back = jax.vjp(layer_norm, record["residual"], params[1:2], params[3:4])[1]
        d_resid_norm, d_gain_one, d_shift_one = norm_back(d_mid)
        d_resid = grad_out + d_resid_norm
        d_attn = low(d_resid)
        g_proj = product_tn(both_cores(record["mixed"]), halves_for_cores(d_attn, section_id))
        d_mixed = low(product_nt(d_attn, proj_both[layer]))
        d_mixed = d_mixed.reshape(seq_rows, dp_size, head_width).transpose(1, 0, 2)
        d_mixed = heads_of(exchange(d_mixed, "dp").reshape(full_len, head_width))
        queries, keys, values = split_heads(record["qkv"])
        probs = record["probs"]
        d_values = jnp.einsum(
            "hij,ihd->jhd", record["probs_low"], d_mixed, preferred_element_type=jnp.float32
        )
        d_probs = jnp.einsum("ihd,jhd->hij", d_mixed, values, preferred_element_type=jnp.float32)
        d_scores = low(probs * (d_probs - jnp.sum(probs * d_probs, axis=-1, keepdims=True)))
        d_queries = jnp.einsum(
            "hij,jhd->ihd", d_scores, keys, preferred_element_type=jnp.float32
        )
        d_keys = jnp.einsum(
            "hij,ihd->jhd", d_scores, queries, preferred_element_type=jnp.float32
        )
        d_qkv = low(
            jnp.concatenate(
                [
                    (d_queries * 0.125).reshape(full_len, head_width),
                    (d_keys * 0.125).reshape(full_len, head_width),
                    d_values.reshape(full_len, head_width),
                ],
                axis=1,
            )
        )
        d_normed = scatter_rows(product_nt(d_qkv, qkv_both[layer]))
        g_qkv = product_tn(
            both_cores(record["normed_seq"]), halves_for_cores(d_qkv, section_id)
        )
        first_back = jax.vjp(layer_norm, record["layer_in"], params[0:1], params[2:3])[1]
        d_input_norm, d_gain_zero, d_shift_zero = first_back(d_normed)
        small_grads = jnp.concatenate(
            [d_gain_zero, d_gain_one, d_shift_zero, d_shift_one, g_small], axis=0
        )

        def over_expert(grad_mat):
            return lax.psum_scatter(low(grad_mat), "expert", scatter_dimension=0, tiled=True)

        def by_rows(grad_mat, count):
            return low(grad_mat).reshape(count, -1, grad_mat.shape[-1])

        if layer == 0:
            qkv_sum = exchange(by_rows(sum_blocks(exchange(by_rows(g_qkv, groups), "expert")), dp_size), "dp")
        else:
            qkv_sum = permute_exchange(by_rows(over_expert(g_qkv), dp_size), "dp")
        proj_sum = permute_sum(by_rows(g_proj, groups), "expert")
        reduced = {
            "qkv": qkv_sum,
            "proj": permute_sum(by_rows(proj_sum, dp_size), "dp"),
            "up": permute_exchange(by_rows(over_expert(g_up), dp_size), "dp"),
            "down": over_expert(g_down),
        }
        return d_resid + d_input_norm, reduced, small_grads, expert_operands

    own_input = lax.dynamic_index_in_dim(inputs[:, 0], section_id, 0, keepdims=False)
    own_grad = lax.dynamic_index_in_dim(cotangent[:, 0], section_id, 0, keepdims=False)
    grad_seqs = lax.all_gather(cotangent[:, 0], "dp", axis=1, tiled=True)
    own_grad_seq = lax.dynamic_index_in_dim(grad_seqs, section_id, 0, keepdims=False)
    out_zero, squares_zero, record_zero = forward_layer(0, own_input.astype(jnp.float32))
    out_zero = low(out_zero)
    out_one, squares_one, record_one = forward_layer(1, out_zero.astype(jnp.float32))
    out_one = low(out_one)
    grad_one, reduced_one, small_one, operands_one = backward_layer(
        1, own_grad, own_grad_seq, record_one
    )
    grad_one_low = low(grad_one)
    grad_zero, reduced_zero, small_zero, operands_zero = backward_layer(
        0, grad_one_low, gather_rows(grad_one_low), record_zero
    )

    def to_owner(layer_zero, layer_one):
        from_other_zero, from_other_one = other_core(layer_zero), other_core(layer_one)
        return jnp.stack(
            [
                jnp.where(on_first, layer_zero, from_other_one),
                jnp.where(on_first, from_other_zero, layer_one),
            ]
        )

    activations = to_owner(out_zero, out_one)
    input_grads = to_owner(grad_zero, grad_one)
    rows_in, d_hidden_in, hidden_in, d_rows_in = [
        to_owner(of_zero, of_one) for of_zero, of_one in zip(operands_zero, operands_one)
    ]
    grad_exp_up = jnp.einsum(
        "erd,erh->edh", rows_in, d_hidden_in, preferred_element_type=jnp.float32
    )
    grad_exp_down = jnp.einsum(
        "erh,erd->ehd", hidden_in, d_rows_in, preferred_element_type=jnp.float32
    )
    joined = {
        name: to_owner(reduced_zero[name], reduced_one[name]).astype(jnp.float32)
        for name in reduced_zero
    }
    grad_qkv = joined["qkv"].transpose(2, 1, 0, 3).reshape(weight_rows, dp_size, 3, head_width)
    grad_qkv = grad_qkv.transpose(0, 2, 1, 3).reshape(weight_rows, 3 * width)
    grad_up = joined["up"].reshape(sections, dp_size, weight_rows, groups // sections, hidden_rows)
    grad_up = grad_up.transpose(2, 0, 3, 1, 4).reshape(weight_rows, -1)
    grad_proj = joined["proj"].transpose(1, 0, 2).reshape(weight_rows, width)
    grad_down = joined["down"].transpose(1, 0, 2).reshape(hidden_rows, width)

    small_grads = jnp.stack([small_zero, small_one]).reshape(
        sections, small_count, groups * dp_size, weight_rows
    )
    small_grads = small_grads.transpose(0, 2, 1, 3).reshape(
        sections, groups * dp_size, small_count * weight_rows
    )
    squares = jnp.stack([squares_zero, squares_one])
    squares = jnp.broadcast_to(squares[:, None], (sections, groups * dp_size, 3))
    small_message = jnp.concatenate([small_grads, squares], axis=-1)
    filled_back = small_message.shape[-1]
    padded_back = -(-filled_back // 1024) * 1024
    small_message = jnp.pad(small_message, ((0, 0), (0, 0), (0, padded_back - filled_back)))
    small_sum = sum_blocks(
        exchange(small_message.reshape(devices, padded_back // 128, 128), EVERY)
    ).reshape(-1)
    sums = small_sum[: small_count * weight_rows].reshape(small_count, weight_rows)
    totals = small_sum[small_count * weight_rows : filled_back]
    element_count = micro_count * seq_rows * width * groups * dp_size
    branch_rms = jnp.sqrt(totals / element_count)[None]
    return (
        activations[None, :, None],
        input_grads[None, :, None],
        sums[None, 0:2],
        sums[None, 2:4],
        grad_qkv[None],
        grad_proj[None],
        grad_up[None],
        grad_down[None],
        sums[4 : 4 + experts_total].T[None],
        sums[4 + experts_total :].T[None],
        grad_exp_up[None],
        grad_exp_down[None],
        branch_rms,
    )


def solution(mesh):
    placed = (
        P(None, "expert", "dp", None),
        P(None, "expert", "dp", None),
        P(None, "expert", None),
        P("section", None, "expert", "dp", None),
        P("section", None, ("expert", "dp")),
        P("section", None, ("expert", "dp")),
        P("section", ("expert", "dp"), None),
        P("section", ("expert", "dp"), None),
        P("section", ("expert", "dp"), None),
        P("section", ("expert", "dp"), None),
        P("section", ("expert", "dp"), None),
        P("section", ("expert", "dp"), None),
        P("section", "expert", None, "dp"),
        P("section", "expert", "dp", None),
    )
    return jax.shard_map(
        shards,
        mesh=mesh,
        in_specs=placed,
        out_specs=(
            P("section", None, "expert", "dp", None),
            P("section", None, "expert", "dp", None),
            P("section", None, ("expert", "dp")),
            P("section", None, ("expert", "dp")),
            P("section", ("expert", "dp"), None),
            P("section", ("expert", "dp"), None),
            P("section", ("expert", "dp"), None),
            P("section", ("expert", "dp"), None),
            P("section", ("expert", "dp"), None),
            P("section", ("expert", "dp"), None),
            P("section", "expert", None, "dp"),
            P("section", "expert", "dp", None),
            P("section", None),
        ),
        check_vma=False,
    )
```

```python
from types import SimpleNamespace

import jax
import jax.numpy as jnp
from jax import lax
from jax.experimental import pallas as pl
from jax.experimental.pallas import tpu as pltpu
from jax.sharding import PartitionSpec as P

HEADS = 16
HEAD_DIM = 64
SEC, EX, DP = "section", "expert", "dp"
EVERY = (SEC, EX, DP)
HOMES = (SEC, EX)


def layer_norm(value_rows, gain_vec, shift_vec):
    centre = jnp.mean(value_rows, axis=-1, keepdims=True)
    centred = value_rows - centre
    variance = jnp.mean(centred * centred, axis=-1, keepdims=True)
    return centred * lax.rsqrt(variance + 1e-05) * gain_vec + shift_vec


def gelu_tanh(value_rows):
    return jax.nn.gelu(value_rows, approximate=True)


def gelu_grad(value_rows, grad_in):
    return jax.vjp(gelu_tanh, value_rows)[1](grad_in)[0]


def product(left_mat, right_mat):
    return jnp.dot(left_mat, right_mat, preferred_element_type=jnp.float32)


def product_tn(left_mat, right_mat):
    return lax.dot_general(
        left_mat, right_mat, (((0,), (0,)), ((), ())), preferred_element_type=jnp.float32
    )


def product_nt(left_mat, right_mat):
    return lax.dot_general(
        left_mat, right_mat, (((1,), (1,)), ((), ())), preferred_element_type=jnp.float32
    )


def low(values):
    return values.astype(jnp.bfloat16)


def exchange(blocks, axes):
    return lax.all_to_all(blocks, axes, split_axis=0, concat_axis=0, tiled=True)


def spread(block, axes):
    count = lax.axis_size(axes)
    return exchange(jnp.broadcast_to(block[None], (count,) + block.shape), axes)


def gather_rows(block):
    return lax.all_gather(block, DP, axis=0, tiled=True)


def sum_blocks(blocks):
    return jnp.sum(blocks.astype(jnp.float32), axis=0)


def row_blocks(partial_rows):
    return low(partial_rows).reshape(lax.axis_size(DP), -1, partial_rows.shape[-1])


def beside(move, blocks, work, operands, late=()):
    blocks, operands = lax.optimization_barrier((blocks, operands))
    return lax.optimization_barrier((move(blocks), work(*operands, *late)))


def over_dp(blocks):
    return exchange(blocks, DP)


def over_homes(blocks):
    return exchange(blocks, HOMES)


def after(values, event):
    return lax.optimization_barrier((values, event))[0]


def permute_copies(block, axis):
    count = lax.axis_size(axis)
    blocks = [block]
    for step in range(1, count):
        route = [((i - step) % count, i) for i in range(count)]
        blocks.append(lax.ppermute(block, axis, route))
    return blocks


def own_parts(blocks, axis):
    count = lax.axis_size(axis)
    place = lax.axis_index(axis)
    return [
        lax.dynamic_index_in_dim(blocks, (place + step) % count, 0, keepdims=False)
        for step in range(count)
    ]


def sent_parts(parts, axis):
    count = len(parts)
    return [parts[0]] + [
        lax.ppermute(parts[step], axis, [((i - step) % count, i) for i in range(count)])
        for step in range(1, count)
    ]


def permute_parts(blocks, axis):
    return sent_parts(own_parts(blocks, axis), axis)


SCALAR = pl.BlockSpec(memory_space=pltpu.SMEM)
WHOLE = pl.BlockSpec(memory_space=pltpu.VMEM)


def in_order(blocks, axis):
    count = lax.axis_size(axis)

    def kernel(place, *refs):
        for step in range(count):
            refs[-1][(place[0] + count - step) % count] = refs[step][...]

    return pl.pallas_call(
        kernel,
        out_shape=jax.ShapeDtypeStruct((count,) + blocks[0].shape, blocks[0].dtype),
        in_specs=[SCALAR] + [WHOLE] * count,
        compiler_params=pltpu.CompilerParams(vmem_limit_bytes=32 << 20),
        name="in_order",
    )(lax.axis_index(axis).reshape(1), *blocks)


def finish_weights(section_id, ups, attns, down_sums, hidden_rows):
    dp_size, rows, half_hidden = ups[0].shape
    down_rows, half_width = down_sums[0].shape
    width = 2 * half_width
    head_width = width // dp_size
    qkv_half = 3 * head_width // 2

    def kernel(place, *refs):
        qkv_ref, proj_ref, up_ref, down_ref = refs[12:]

        def write(up_halves, attn_halves, down_halves):
            for half in range(2):
                up, attn = up_halves[half], attn_halves[half]
                here = slice(half * half_width, (half + 1) * half_width)
                proj_sum = attn[0, :, :half_width].astype(jnp.float32)
                for z in range(1, dp_size):
                    proj_sum = proj_sum + attn[z, :, :half_width].astype(jnp.float32)
                proj_ref[:, here] = proj_sum
                down_ref[:, here] = down_halves[half][...].astype(jnp.float32)
                for z in range(dp_size):
                    for piece in range(half_hidden // hidden_rows):
                        group = half * (half_hidden // hidden_rows) + piece
                        start = (group * dp_size + z) * hidden_rows
                        up_ref[:, start : start + hidden_rows] = up[
                            z, :, piece * hidden_rows : (piece + 1) * hidden_rows
                        ].astype(jnp.float32)
                    at = 0
                    while at < qkv_half:
                        column = half * qkv_half + at
                        part, inner = column // head_width, column % head_width
                        size = min(head_width - inner, qkv_half - at)
                        first = half_width + at
                        start = part * width + z * head_width + inner
                        qkv_ref[:, start : start + size] = attn[
                            z, :, first : first + size
                        ].astype(jnp.float32)
                        at = at + size

        @pl.when(place[0] == 0)
        def _():
            write(refs[0:2], refs[4:6], refs[8:10])

        @pl.when(place[0] != 0)
        def _():
            write(refs[3:1:-1], refs[7:5:-1], refs[11:9:-1])

    shapes = ((rows, 3 * width), (rows, width), (rows, 2 * half_hidden * dp_size), (down_rows, width))
    return pl.pallas_call(
        kernel,
        out_shape=[jax.ShapeDtypeStruct(shape, jnp.float32) for shape in shapes],
        in_specs=[SCALAR] + [WHOLE] * 12,
        compiler_params=pltpu.CompilerParams(vmem_limit_bytes=32 << 20),
        name="finish_weights",
    )(section_id.reshape(1), *ups, *attns, *down_sums)


def finish_rows(section_id, *arrays):
    count = len(arrays)

    def kernel(place, *refs):
        outs = refs[4 * count :]
        for index in range(count):
            own_zero, other_zero, own_one, other_one = refs[4 * index : 4 * index + 4]

            @pl.when(place[0] == 0)
            def _():
                outs[index][0] = own_zero[...]
                outs[index][1] = other_zero[...]

            @pl.when(place[0] != 0)
            def _():
                outs[index][0] = other_one[...]
                outs[index][1] = own_one[...]

    return pl.pallas_call(
        kernel,
        out_shape=[
            jax.ShapeDtypeStruct((2,) + array[0].shape, array[0].dtype) for array in arrays
        ],
        in_specs=[SCALAR] + [WHOLE] * (4 * count),
        compiler_params=pltpu.CompilerParams(vmem_limit_bytes=32 << 20),
        name="finish_rows",
    )(section_id.reshape(1), *[rows for array in arrays for rows in array])


def sum_parts(parts):
    return sum(part.astype(jnp.float32) for part in parts)


def softmax_rows(queries, keys, allowed):
    scores = product_nt(queries, keys) * 0.125
    scores = jnp.where(allowed, scores, -jnp.inf)
    exp_scores = jnp.exp(scores - jnp.max(scores, axis=-1, keepdims=True))
    return exp_scores / jnp.sum(exp_scores, axis=-1, keepdims=True)


def allowed_keys(seg_column, seg_row):
    rows, columns = seg_column.shape[0], seg_row.shape[1]
    query_at = lax.broadcasted_iota(jnp.int32, (rows, columns), 0)
    key_at = lax.broadcasted_iota(jnp.int32, (rows, columns), 1)
    return (seg_column == seg_row) & (key_at <= query_at)


def head_slices(packed, head, head_width):
    start = head * HEAD_DIM
    return [
        packed[:, part * head_width + start : part * head_width + start + HEAD_DIM]
        for part in range(3)
    ]


def attention_kernel(seg_column, seg_row, qkv_ref, mixed_ref):
    head_width = mixed_ref.shape[1]
    allowed = allowed_keys(seg_column[...], seg_row[...])
    packed = qkv_ref[...]
    mixed = []
    for head in range(head_width // HEAD_DIM):
        queries, keys, values = head_slices(packed, head, head_width)
        probs = softmax_rows(queries, keys, allowed)
        mixed.append(low(product(low(probs), values)))
    mixed_ref[...] = jnp.concatenate(mixed, axis=1)


def attention_back_kernel(seg_column, seg_row, qkv_ref, d_mixed_ref, d_qkv_ref):
    head_width = d_mixed_ref.shape[1]
    allowed = allowed_keys(seg_column[...], seg_row[...])
    packed = qkv_ref[...]
    d_mixed_all = d_mixed_ref[...]
    grads = [[], [], []]
    for head in range(head_width // HEAD_DIM):
        queries, keys, values = head_slices(packed, head, head_width)
        d_mixed = d_mixed_all[:, head * HEAD_DIM : (head + 1) * HEAD_DIM]
        probs = softmax_rows(queries, keys, allowed)
        d_probs = product_nt(d_mixed, values)
        d_scores = low(probs * (d_probs - jnp.sum(probs * d_probs, axis=-1, keepdims=True)))
        grads[0].append(low(product(d_scores, keys) * 0.125))
        grads[1].append(low(product_tn(d_scores, queries) * 0.125))
        grads[2].append(low(product_tn(low(probs), d_mixed)))
    d_qkv_ref[...] = jnp.concatenate(grads[0] + grads[1] + grads[2], axis=1)


def attention(segments, qkv):
    head_width = qkv.shape[1] // 3
    return pl.pallas_call(
        attention_kernel,
        out_shape=jax.ShapeDtypeStruct((qkv.shape[0], head_width), jnp.bfloat16),
        compiler_params=pltpu.CompilerParams(vmem_limit_bytes=32 << 20),
        name="attention",
    )(segments[:, None], segments[None, :], qkv)


def attention_back(segments, qkv, d_mixed):
    return pl.pallas_call(
        attention_back_kernel,
        out_shape=jax.ShapeDtypeStruct(qkv.shape, jnp.bfloat16),
        compiler_params=pltpu.CompilerParams(vmem_limit_bytes=32 << 20),
        name="attention_back",
    )(segments[:, None], segments[None, :], qkv, d_mixed)


OWNER_TILE = 256


def owner_grads(section_id, left_mats, right_mats):
    rows, left_width = left_mats[0].shape
    right_width = right_mats[0].shape[1]
    tiles = left_width // OWNER_TILE

    def kernel(place, *refs):
        out_ref = refs[8]
        expert, tile = pl.program_id(0), pl.program_id(1)
        first = place[0] == 0
        for source, here in enumerate(
            (
                first & (expert == 0),
                first & (expert == 1),
                ~first & (expert == 1),
                ~first & (expert == 0),
            )
        ):

            @pl.when(here)
            def _():
                left = refs[source][:, pl.ds(tile * OWNER_TILE, OWNER_TILE)]
                out_ref[0] = product_tn(left, refs[4 + source][...])

    whole = [
        pl.BlockSpec(mat.shape, lambda expert, tile: (0, 0))
        for mat in (*left_mats, *right_mats)
    ]
    return pl.pallas_call(
        kernel,
        out_shape=jax.ShapeDtypeStruct((2, left_width, right_width), jnp.float32),
        grid=(2, tiles),
        in_specs=[pl.BlockSpec(memory_space=pltpu.SMEM)] + whole,
        out_specs=pl.BlockSpec((1, OWNER_TILE, right_width), lambda expert, tile: (expert, tile, 0)),
        compiler_params=pltpu.CompilerParams(vmem_limit_bytes=40 << 20),
        name="owner_grads",
    )(section_id.reshape(1), *left_mats, *right_mats)


def statistics(value_rows):
    centre = jnp.mean(value_rows, axis=-1, keepdims=True)
    centred = value_rows - centre
    variance = jnp.mean(centred * centred, axis=-1, keepdims=True)
    spread_inverse = lax.rsqrt(variance + 1e-05)
    return centred * spread_inverse, spread_inverse


def column_sums(value_rows):
    return jnp.sum(value_rows, axis=0, keepdims=True)


def block_sum(blocks_ref):
    total = blocks_ref[0].astype(jnp.float32)
    for place in range(1, blocks_ref.shape[0]):
        total = total + blocks_ref[place].astype(jnp.float32)
    return total


def call(kernel, name, outs, *operands):
    return pl.pallas_call(
        kernel,
        out_shape=[jax.ShapeDtypeStruct(shape, dtype) for shape, dtype in outs],
        compiler_params=pltpu.CompilerParams(vmem_limit_bytes=32 << 20),
        name=name,
    )(*operands)


def project(mixed_blocks, proj_mat, layer_in, gain, shift):
    def kernel(mixed_ref, proj_ref, in_ref, gain_ref, shift_ref, rows_ref, res_ref, mid_ref, sq_ref):
        places = mixed_ref.shape[0]
        mixed = jnp.concatenate([mixed_ref[place] for place in range(places)], axis=1)
        rows_ref[...] = mixed
        branch = product(mixed, proj_ref[...])
        residual = in_ref[...].astype(jnp.float32) + branch
        res_ref[...] = residual
        mid_ref[...] = low(statistics(residual)[0] * gain_ref[...] + shift_ref[...])
        sq_ref[...] = column_sums(branch * branch)

    rows, width = layer_in.shape
    outs = [((rows, width), jnp.bfloat16), ((rows, width), jnp.float32)]
    outs += [((rows, width), jnp.bfloat16), ((1, width), jnp.float32)]
    return call(kernel, "project", outs, mixed_blocks, proj_mat, layer_in, gain, shift)


def layer_end(branch_blocks, residual, gain, shift):
    def kernel(blocks_ref, res_ref, gain_ref, shift_ref, out_ref, normed_ref, sq_ref):
        branch = block_sum(blocks_ref)
        layer_out = res_ref[...] + branch
        rounded = low(layer_out)
        out_ref[...] = rounded
        normed = statistics(rounded.astype(jnp.float32))[0]
        normed_ref[...] = low(normed * gain_ref[...] + shift_ref[...])
        sq_ref[0:1] = column_sums(branch * branch)
        sq_ref[1:2] = column_sums(layer_out * layer_out)

    shape = residual.shape
    outs = [(shape, jnp.bfloat16), (shape, jnp.bfloat16), ((2, shape[1]), jnp.float32)]
    return call(kernel, "layer_end", outs, branch_blocks, residual, gain, shift)


def norm_back(blocks_ref, value_ref, gain_ref, grad_ref, gain_grad_ref, shift_grad_ref):
    d_normed = block_sum(blocks_ref)
    normed, spread_inverse = statistics(value_ref[...].astype(jnp.float32))
    gain_grad_ref[...] = column_sums(d_normed * normed)
    shift_grad_ref[...] = column_sums(d_normed)
    d_centred = d_normed * gain_ref[...]
    along = jnp.mean(d_centred * normed, axis=-1, keepdims=True)
    d_value = d_centred - jnp.mean(d_centred, axis=-1, keepdims=True) - normed * along
    return grad_ref[...].astype(jnp.float32) + d_value * spread_inverse


def mid_back(mid_blocks, residual, gain, grad_out, proj_mat, dp_size):
    def kernel(blocks_ref, res_ref, gain_ref, grad_ref, proj_ref, *outs):
        sum_ref, low_ref, mixed_ref, gain_grad_ref, shift_grad_ref = outs
        grad = norm_back(blocks_ref, res_ref, gain_ref, grad_ref, gain_grad_ref, shift_grad_ref)
        sum_ref[...] = grad
        low_ref[...] = low(grad)
        d_mixed = low(product_nt(low(grad), proj_ref[...]))
        part = d_mixed.shape[1] // dp_size
        for place in range(dp_size):
            mixed_ref[place] = d_mixed[:, place * part : (place + 1) * part]

    rows, width = residual.shape
    row = ((1, width), jnp.float32)
    outs = [((rows, width), jnp.float32), ((rows, width), jnp.bfloat16)]
    outs += [((dp_size, rows, width // dp_size), jnp.bfloat16), row, row]
    return call(kernel, "mid_back", outs, mid_blocks, residual, gain, grad_out, proj_mat)


def input_back(in_blocks, layer_in, gain, grad_resid):
    def kernel(blocks_ref, in_ref, gain_ref, grad_ref, sum_ref, low_ref, gain_grad_ref, shift_grad_ref):
        grad = norm_back(blocks_ref, in_ref, gain_ref, grad_ref, gain_grad_ref, shift_grad_ref)
        sum_ref[...] = grad
        low_ref[...] = low(grad)

    shape = layer_in.shape
    row = ((1, shape[1]), jnp.float32)
    outs = [(shape, jnp.float32), (shape, jnp.bfloat16), row, row]
    return call(kernel, "input_back", outs, in_blocks, layer_in, gain, grad_resid)


LANES = 128


def pack_small(parts_of_layers, squares_of_layers, weight_rows):
    layers = len(parts_of_layers)
    flat = [part for parts in parts_of_layers for part in parts] + list(squares_of_layers)
    width = flat[0].shape[1]
    used = sum(part.shape[0] for part in parts_of_layers[0])
    height = -(-(used + 1) // 8) * 8
    places = width // weight_rows

    def kernel(*refs):
        out_ref, rows_ref = refs[-2], refs[-1]
        per_layer = len(parts_of_layers[0])
        for layer in range(layers):
            rows_ref[...] = jnp.zeros(rows_ref.shape, jnp.float32)
            start = 0
            for part in refs[layer * per_layer : (layer + 1) * per_layer]:
                rows_ref[start : start + part.shape[0]] = part[...]
                start = start + part.shape[0]
            lane = lax.broadcasted_iota(jnp.int32, (1, width), 1) % LANES
            marked = jnp.zeros((1, width), jnp.float32)
            sums = jnp.sum(refs[layers * per_layer + layer][...], axis=1, keepdims=True)
            for kind in range(3):
                marked = jnp.where(lane == kind, sums[kind : kind + 1], marked)
            rows_ref[start : start + 1] = marked
            for place in range(places):
                column = place * weight_rows // LANES * LANES
                out_ref[layer * places + place] = rows_ref[:, column : column + LANES]

    return pl.pallas_call(
        kernel,
        out_shape=jax.ShapeDtypeStruct((layers * places, height, LANES), jnp.float32),
        scratch_shapes=[pltpu.VMEM((height, width), jnp.float32)],
        name="pack_small",
    )(*flat)


def other_core(block):
    return lax.ppermute(block, SEC, [(0, 1), (1, 0)])


def both_cores(block):
    return jnp.concatenate([block, other_core(block)], axis=0)


def halves_for_cores(block, section_id):
    half = block.shape[1] // 2
    kept = lax.dynamic_slice_in_dim(block, section_id * half, half, axis=1)
    sent = lax.dynamic_slice_in_dim(block, (1 - section_id) * half, half, axis=1)
    return jnp.concatenate([kept, other_core(sent)], axis=0)


def shards(
    inputs,
    cotangent,
    segment_ids,
    routes,
    norm_gains,
    norm_shifts,
    attn_qkv,
    attn_proj,
    dense_up,
    dense_down,
    router,
    mixer,
    expert_up,
    expert_down,
):
    sections = lax.axis_size(SEC)
    groups = lax.axis_size(EX)
    dp_size = lax.axis_size(DP)
    section_id = lax.axis_index(SEC)
    expert_id = lax.axis_index(EX)
    micro_count = inputs.shape[0]
    seq_rows = inputs.shape[2]
    width = inputs.shape[3]
    full_len = segment_ids.shape[2]
    experts_total = router.shape[2]
    hidden_rows = dense_down.shape[1]
    weight_rows = attn_qkv.shape[1]
    heads_here = HEADS // dp_size
    head_width = heads_here * HEAD_DIM
    capacity = max(2, 5 * seq_rows // (4 * experts_total))
    slots = dp_size * capacity
    devices = sections * groups * dp_size

    small_parts = jnp.concatenate([norm_gains[0], norm_shifts[0], router[0].T, mixer[0].T], axis=0)
    small_count = small_parts.shape[0]
    route_row = low(routes[0, :, 0, :, 0])
    message = jnp.concatenate([small_parts.reshape(-1), route_row.reshape(-1)])
    filled = message.shape[0]
    padded = -(-filled // 1024) * 1024
    message = jnp.pad(message, (0, padded - filled)).reshape(padded // 128, 128)

    def expert_parts(*own_layers):
        return [
            (
                lax.dynamic_index_in_dim(own_layer, section_id, 0, keepdims=False),
                lax.dynamic_index_in_dim(own_layer, 1 - section_id, 0, keepdims=False),
            )
            for own_layer in own_layers
        ]

    hidden_here = groups * hidden_rows
    small_all, (proj_rows, up_parts) = beside(
        lambda blocks: exchange(blocks, EVERY),
        jnp.broadcast_to(message[None], (devices,) + message.shape),
        lambda proj_shard, up_cols: (
            in_order(permute_copies(proj_shard, DP), DP),
            own_parts(
                up_cols.reshape(weight_rows, groups, dp_size, hidden_rows)
                .transpose(2, 0, 1, 3)
                .reshape(dp_size, weight_rows, hidden_here),
                DP,
            ),
        ),
        (attn_proj[0], dense_up[0]),
    )
    small_all = small_all.reshape(sections, groups, dp_size, padded)

    def params_of(small_all):
        params_all = small_all[..., : small_count * weight_rows].reshape(
            sections, groups * dp_size, small_count, weight_rows
        )
        return params_all.transpose(0, 2, 1, 3).reshape(sections, small_count, width)

    def routes_of(small_all):
        routes_all = lax.dynamic_index_in_dim(
            small_all[..., small_count * weight_rows : filled], expert_id, 1, keepdims=False
        ).reshape(sections, dp_size, micro_count, seq_rows)
        routes_all = lax.dynamic_index_in_dim(routes_all, section_id, 2, keepdims=False)
        return routes_all.astype(jnp.int32)

    on_first = section_id == 0

    def by_layer(pair):
        of_own_layer, of_other_layer = pair
        return (
            jnp.where(on_first, of_own_layer, of_other_layer),
            jnp.where(on_first, of_other_layer, of_own_layer),
        )

    proj_both = lax.all_gather(proj_rows.reshape(-1, width), HOMES, axis=0, tiled=True)
    proj_both = proj_both.reshape(sections, width, width)
    qkv_cols = attn_qkv[0].reshape(weight_rows, 3, dp_size, head_width).transpose(2, 0, 1, 3)
    qkv_cols, small_all = lax.optimization_barrier(
        (qkv_cols.reshape(dp_size, weight_rows, 3 * head_width), small_all)
    )
    qkv_cols, expert_weights = beside(
        over_dp, qkv_cols, expert_parts, (expert_up[0], expert_down[0])
    )
    params_all = params_of(small_all)
    routes_all = routes_of(small_all)
    own_input = lax.dynamic_index_in_dim(inputs[:, 0], section_id, 0, keepdims=False)
    first_params = params_all[0].astype(jnp.float32)
    first_normed = low(
        layer_norm(own_input.astype(jnp.float32), first_params[0:1], first_params[2:3])
    )
    qkv_own, (first_seq, up_rows) = beside(
        lambda blocks: exchange(blocks, EX),
        jnp.broadcast_to(qkv_cols[None], (groups,) + qkv_cols.shape),
        lambda rows, *parts: (
            in_order(permute_copies(rows, DP), DP),
            in_order(sent_parts(parts, DP), DP),
        ),
        (first_normed, *up_parts),
    )
    first_seq = first_seq.reshape(full_len, width)
    qkv_own = qkv_own.reshape(width, 3 * head_width)
    qkv_pair = (qkv_own, other_core(qkv_own))
    exp_up_pair, exp_down_pair = [(kept, other_core(sent)) for kept, sent in expert_weights]
    first_qkv = low(product(first_seq, by_layer(qkv_pair)[0]))
    up_both = lax.all_gather(up_rows.reshape(-1, hidden_here), HOMES, axis=0, tiled=True)
    up_both = up_both.reshape(sections, width, hidden_here)
    down_both = lax.all_gather(dense_down[0], HOMES, axis=0, tiled=True)
    down_both = down_both.reshape(sections, hidden_here, width)

    segments = lax.dynamic_index_in_dim(segment_ids[:, 0], section_id, 0, keepdims=False)
    places = jnp.arange(full_len, dtype=jnp.int32)
    earlier = (places[None, :] < places[:, None]) & (
        places[None, :] // seq_rows == places[:, None] // seq_rows
    )

    def slot_table(route_now):
        rank = jnp.sum(
            ((route_now[:, None] == route_now[None, :]) & earlier).astype(jnp.int32), axis=1
        )
        home = route_now % sections * groups + route_now // sections
        target = home * slots + places // seq_rows * capacity + rank
        slot_ids = jnp.arange(sections * groups * slots, dtype=jnp.int32)
        table = low(slot_ids[:, None] == target[None, :])
        hot = route_now[:, None] == jnp.arange(experts_total, dtype=jnp.int32)[None, :]
        return table, hot.astype(jnp.float32)

    def packed_rows(token_rows, table):
        return low(product(table, token_rows)).reshape(sections * groups, slots, width)

    def coefficients(mid_seq, small_weights, hot):
        small_logits = product_nt(mid_seq, small_weights)
        gate_probs = jax.nn.softmax(small_logits[:, :experts_total], axis=-1)
        gate = jnp.sum(gate_probs * hot, axis=-1, keepdims=True)
        coef = jax.nn.softmax(small_logits[:, experts_total:], axis=-1)
        return gate_probs, gate, coef

    def dense_in(mid_seq, up_mat):
        hidden = product(mid_seq, up_mat)
        return hidden, low(gelu_tanh(hidden))

    def attended(qkv):
        return attention(segments, qkv).reshape(dp_size, seq_rows, head_width)

    def forward_zero():
        params = first_params
        table, hot = slot_table(routes_all[0].reshape(full_len))
        mixed, residual, mid, attn_squares = project(
            over_dp(attended(first_qkv)), proj_both[0], own_input, params[1:2], params[3:4]
        )
        mid_seq = gather_rows(mid)
        small_weights = params_all[0, 4:]
        exp_up_mat, exp_down_mat = by_layer(exp_up_pair)[0], by_layer(exp_down_pair)[0]

        expert_rows, (gate_probs, gate, coef) = beside(
            over_homes,
            packed_rows(mid_seq, table),
            lambda mid_seq, small_weights: coefficients(mid_seq, small_weights, hot),
            (mid_seq, small_weights),
        )
        expert_rows = expert_rows.reshape(-1, width)
        exp_hidden = product(expert_rows, exp_up_mat)
        exp_hidden_low = low(gelu_tanh(exp_hidden))

        def return_work(mid_seq, up_mat, down_mat):
            hidden, hidden_low = dense_in(mid_seq, up_mat)
            return hidden, hidden_low, product(hidden_low, down_mat)

        returned, (hidden, hidden_low, dense_part) = beside(
            over_homes,
            low(product(exp_hidden_low, exp_down_mat)).reshape(-1, slots, width),
            return_work,
            (mid_seq,),
            (up_both[0], down_both[0]),
        )
        expert_part = product_tn(table, returned.reshape(-1, width))
        branch_part = coef[:, 0:1] * dense_part + coef[:, 1:2] * gate * expert_part
        branch, settled = beside(
            over_dp,
            row_blocks(branch_part),
            lambda *pairs: [by_layer(pair) for pair in pairs],
            (qkv_pair, exp_up_pair, exp_down_pair),
        )
        next_params = params_all[1].astype(jnp.float32)
        out_low, next_normed, squares = layer_end(
            branch, residual, next_params[0:1], next_params[2:3]
        )
        record = SimpleNamespace(
            params=params,
            small_weights=small_weights,
            table=table,
            hot=hot,
            layer_in=own_input,
            normed_seq=first_seq,
            qkv=first_qkv,
            mixed=mixed,
            residual=residual,
            mid_seq=mid_seq,
            expert_rows=expert_rows,
            gate_probs=gate_probs,
            gate=gate,
            coef=coef,
            hidden=hidden,
            hidden_low=hidden_low,
            dense_part=dense_part,
            exp_hidden=exp_hidden,
            exp_hidden_low=exp_hidden_low,
            expert_part=expert_part,
        )
        squares = jnp.concatenate([attn_squares, squares], axis=0)
        return out_low, next_normed, squares, record, settled

    def forward_one(layer_in, normed):
        params = params_all[1].astype(jnp.float32)
        table, hot = slot_table(routes_all[1].reshape(full_len))
        normed_seq = gather_rows(normed)
        qkv = low(product(normed_seq, qkv_both[1]))
        mixed, residual, mid, attn_squares = project(
            over_dp(attended(qkv)), proj_both[1], layer_in, params[1:2], params[3:4]
        )
        mid_seq = gather_rows(mid)
        grad_seqs = lax.all_gather(after(cotangent[:, 0], mid_seq), DP, axis=1, tiled=True)
        own_grad_seq = lax.dynamic_index_in_dim(grad_seqs, section_id, 0, keepdims=False)
        small_weights = params_all[1, 4:]

        def dispatch_work(mid_seq, small_weights, up_mat):
            return coefficients(mid_seq, small_weights, hot), dense_in(mid_seq, up_mat)

        expert_rows, ((gate_probs, gate, coef), (hidden, hidden_low)) = beside(
            over_homes,
            packed_rows(mid_seq, table),
            dispatch_work,
            (mid_seq, small_weights, up_both[1]),
        )
        expert_rows = expert_rows.reshape(-1, width)
        exp_hidden = product(expert_rows, exp_up_both[1])
        exp_hidden_low = low(gelu_tanh(exp_hidden))
        returned, dense_part = beside(
            over_homes,
            low(product(exp_hidden_low, exp_down_both[1])).reshape(-1, slots, width),
            product,
            (hidden_low, down_both[1]),
        )
        expert_part = product_tn(table, returned.reshape(-1, width))
        branch_part = coef[:, 0:1] * dense_part + coef[:, 1:2] * gate * expert_part
        branch = lax.psum_scatter(low(branch_part), DP, scatter_dimension=0, tiled=True)
        record = SimpleNamespace(
            params=params,
            small_weights=small_weights,
            table=table,
            hot=hot,
            layer_in=layer_in,
            normed_seq=normed_seq,
            qkv=qkv,
            mixed=mixed,
            residual=residual,
            mid_seq=mid_seq,
            expert_rows=expert_rows,
            gate_probs=gate_probs,
            gate=gate,
            coef=coef,
            hidden=hidden,
            hidden_low=hidden_low,
            dense_part=dense_part,
            exp_hidden=exp_hidden,
            exp_hidden_low=exp_hidden_low,
            expert_part=expert_part,
        )
        return branch, attn_squares, record, own_grad_seq

    def over_expert(grad_mat):
        return lax.psum_scatter(grad_mat, EX, scatter_dimension=0, tiled=True)

    def by_rows(grad_mat, count):
        return low(grad_mat).reshape(count, -1, grad_mat.shape[-1])

    def shared_product(left_mat, right_mat):
        return low(
            product_tn(both_cores(left_mat), halves_for_cores(right_mat, section_id))
        )

    def dp_blocks(*grad_mats):
        blocks = [by_rows(grad_mat, dp_size) for grad_mat in grad_mats]
        return own_parts(jnp.concatenate(blocks, axis=2), DP)

    half_hidden, half_width = hidden_here // 2, width // 2

    def backward_layer(layer, grad_low, grad_seq, record, sums_one=(), operands_one=None, settle=()):
        params = record.params
        coef, gate, table = record.coef, record.gate, record.table
        grad_seq = grad_seq.astype(jnp.float32)
        d_expert = low(coef[:, 1:2] * gate * grad_seq)

        def dense_back(grad_seq, coef, down_mat, up_mat, *sums_one):
            early = dp_blocks(*sums_one) if sums_one else ()
            d_dense = low(coef[:, 0:1] * grad_seq)
            dense_dot = jnp.sum(grad_seq * record.dense_part, axis=-1, keepdims=True)
            expert_dot = jnp.sum(grad_seq * record.expert_part, axis=-1, keepdims=True)
            d_coef = jnp.concatenate([dense_dot, gate * expert_dot], axis=1)
            d_mix = coef * (d_coef - jnp.sum(coef * d_coef, axis=-1, keepdims=True))
            d_logits = record.gate_probs * (record.hot - gate) * (coef[:, 1:2] * expert_dot)
            d_small = low(jnp.concatenate([d_logits, d_mix], axis=1))
            d_up = low(gelu_grad(record.hidden, product_nt(d_dense, down_mat)))
            d_mid_part = product_nt(d_up, up_mat) + product(d_small, record.small_weights)
            return d_dense, d_small, d_up, d_mid_part, early

        expert_grad_rows, (d_dense, d_small, d_up, d_mid_part, early) = beside(
            over_homes,
            packed_rows(d_expert, table),
            dense_back,
            (grad_seq, coef, down_both[layer], up_both[layer]),
            tuple(sums_one),
        )
        expert_grad_rows = expert_grad_rows.reshape(-1, width)
        d_exp_hidden = low(
            gelu_grad(record.exp_hidden, product_nt(expert_grad_rows, exp_down_both[layer]))
        )
        expert_operands = (
            record.expert_rows,
            d_exp_hidden,
            record.exp_hidden_low,
            expert_grad_rows,
        )

        swapped = tuple(other_core(operand) for operand in expert_operands)

        def owner_mats(index):
            return (
                expert_operands[index],
                swapped[index],
                operands_one[0][index],
                operands_one[1][index],
            )

        def dense_grads(hidden_low, d_dense, mid_seq, d_up, d_small):
            g_dense = [shared_product(mid_seq, d_up), shared_product(hidden_low, d_dense)]
            g_small = product_tn(d_small, mid_seq)
            return jnp.concatenate(g_dense, axis=1), g_small

        expert_back = low(product_nt(d_exp_hidden, exp_up_both[layer])).reshape(-1, slots, width)
        if layer == 0:
            returned, (parts_one, g_exp_down) = beside(
                over_homes,
                expert_back,
                lambda early, *mats: (sent_parts(early, DP), owner_grads(section_id, *mats)),
                (early, owner_mats(2), owner_mats(3)),
            )
        else:
            returned = over_homes(expert_back)
        d_mid_part = d_mid_part + product_tn(table, returned.reshape(-1, width))
        mid_blocks, operands = lax.optimization_barrier(
            (
                row_blocks(d_mid_part),
                (record.hidden_low, d_dense, record.mid_seq, d_up, d_small),
            )
        )
        g_dense, g_small = dense_grads(*operands)
        dense_sum = over_expert(g_dense)
        d_mid, g_dense, g_small = lax.optimization_barrier(
            (over_dp(mid_blocks), g_dense, g_small)
        )
        d_resid, d_attn, d_mixed, d_gain_one, d_shift_one = mid_back(
            d_mid, record.residual, params[1:2], grad_low, proj_both[layer], dp_size
        )
        d_mixed, g_proj = beside(over_dp, d_mixed, shared_product, (record.mixed, d_attn))
        d_qkv = attention_back(segments, record.qkv, d_mixed.reshape(full_len, head_width))

        in_blocks, normed_seq, d_qkv = lax.optimization_barrier(
            (row_blocks(product_nt(d_qkv, qkv_both[layer])), record.normed_seq, d_qkv)
        )
        g_attn = jnp.concatenate([g_proj, shared_product(normed_seq, d_qkv)], axis=1)
        attn_sum = over_expert(g_attn)
        beside_it = (g_attn, settle)
        d_normed, beside_it = lax.optimization_barrier((over_dp(in_blocks), beside_it))
        def finish(in_blocks):
            return input_back(in_blocks, record.layer_in, params[0:1], d_resid)

        up_moved = None
        if layer == 0:
            up_moved, finished = beside(
                over_dp, by_rows(dense_sum[:, :half_hidden], dp_size), finish, (), (d_normed,)
            )
        else:
            finished = finish(d_normed)
        d_input, d_input_low, d_gain_zero, d_shift_zero = finished
        small_grads = (d_gain_zero, d_gain_one, d_shift_zero, d_shift_one, g_small)
        if layer == 0:
            extra = (parts_one, owner_mats, g_exp_down, up_moved)
        else:
            extra = (expert_operands, swapped, beside_it[1])
        return d_input, d_input_low, (dense_sum, attn_sum), small_grads, extra

    own_grad = lax.dynamic_index_in_dim(cotangent[:, 0], section_id, 0, keepdims=False)
    out_zero, next_normed, squares_zero, record_zero, settled = forward_zero()
    qkv_both, exp_up_both, exp_down_both = settled
    branch_one, attn_squares_one, record_one, own_grad_seq = forward_one(out_zero, next_normed)
    grad_one, grad_one_low, sums_one, small_one, operands_one = backward_layer(
        1, own_grad, own_grad_seq, record_one, settle=branch_one
    )
    dense_one, attn_one = sums_one
    branch_one = operands_one[2].astype(jnp.float32)
    out_one = record_one.residual + branch_one
    squares_one = jnp.concatenate(
        [attn_squares_one, column_sums(branch_one * branch_one), column_sums(out_one * out_one)]
    )
    out_one = low(out_one)
    grad_zero, _, (dense_zero, attn_zero), small_zero, extra = backward_layer(
        0,
        grad_one_low,
        gather_rows(grad_one_low),
        record_zero,
        (dense_one[:, :half_hidden], attn_one),
        operands_one,
    )
    parts_one, owner_mats, grad_exp_down, up_zero = extra

    moved_one = in_order(after(parts_one, grad_zero), DP)
    small_message = pack_small(
        (small_zero, small_one), (squares_zero, squares_one), weight_rows
    )
    small_moved, grad_exp_up = beside(
        lambda blocks: exchange(blocks, EVERY),
        small_message,
        lambda *mats: owner_grads(section_id, *mats),
        (owner_mats(0), owner_mats(1)),
    )
    attn_zero = over_dp(by_rows(attn_zero, dp_size))
    up_one, attn_one = moved_one[..., :half_hidden], moved_one[..., half_hidden:]
    down_zero, down_one = dense_zero[:, half_hidden:], dense_one[:, half_hidden:]

    def of_both(of_zero, of_one):
        return of_zero, other_core(of_zero), of_one, other_core(of_one)

    grad_qkv, grad_proj, grad_up, grad_down = finish_weights(
        section_id,
        of_both(up_zero, up_one),
        of_both(attn_zero, attn_one),
        of_both(down_zero, down_one),
        hidden_rows,
    )
    activations, input_grads = finish_rows(
        section_id, of_both(out_zero, out_one), of_both(grad_zero, grad_one)
    )
    small_sum = jnp.sum(small_moved, axis=0)
    place = expert_id * dp_size + lax.axis_index(DP)
    sums = lax.dynamic_slice_in_dim(
        small_sum[:small_count], place * weight_rows % LANES, weight_rows, axis=1
    )
    totals = small_sum[small_count, :3]
    element_count = micro_count * seq_rows * width * groups * dp_size
    branch_rms = jnp.sqrt(totals / element_count)[None]
    return (
        activations[None, :, None],
        input_grads[None, :, None],
        sums[None, 0:2],
        sums[None, 2:4],
        grad_qkv[None],
        grad_proj[None],
        grad_up[None],
        grad_down[None],
        sums[4 : 4 + experts_total].T[None],
        sums[4 + experts_total :].T[None],
        grad_exp_up[None],
        grad_exp_down[None],
        branch_rms,
    )


def solution(mesh):
    placed = (
        P(None, EX, DP, None),
        P(None, EX, DP, None),
        P(None, EX, None),
        P(SEC, None, EX, DP, None),
        P(SEC, None, (EX, DP)),
        P(SEC, None, (EX, DP)),
        P(SEC, (EX, DP), None),
        P(SEC, (EX, DP), None),
        P(SEC, (EX, DP), None),
        P(SEC, (EX, DP), None),
        P(SEC, (EX, DP), None),
        P(SEC, (EX, DP), None),
        P(SEC, EX, None, DP),
        P(SEC, EX, DP, None),
    )
    return jax.shard_map(
        shards,
        mesh=mesh,
        in_specs=placed,
        out_specs=(
            P(SEC, None, EX, DP, None),
            P(SEC, None, EX, DP, None),
            P(SEC, None, (EX, DP)),
            P(SEC, None, (EX, DP)),
            P(SEC, (EX, DP), None),
            P(SEC, (EX, DP), None),
            P(SEC, (EX, DP), None),
            P(SEC, (EX, DP), None),
            P(SEC, (EX, DP), None),
            P(SEC, (EX, DP), None),
            P(SEC, EX, None, DP),
            P(SEC, EX, DP, None),
            P(SEC, None),
        ),
        check_vma=False,
    )
```

```python
from types import SimpleNamespace

import jax
import jax.numpy as jnp
from jax import lax
from jax.experimental import pallas as pl
from jax.experimental.pallas import tpu as pltpu
from jax.sharding import PartitionSpec as P

HEADS = 16
HEAD_DIM = 64
SEC, EX, DP = "section", "expert", "dp"
EVERY = (SEC, EX, DP)
HOMES = (SEC, EX)
LANES = 128


def layer_norm(value_rows, gain_vec, shift_vec):
    centre = jnp.mean(value_rows, axis=-1, keepdims=True)
    centred = value_rows - centre
    variance = jnp.mean(centred * centred, axis=-1, keepdims=True)
    return centred * lax.rsqrt(variance + 1e-05) * gain_vec + shift_vec


def gelu_tanh(value_rows):
    return jax.nn.gelu(value_rows, approximate=True)


def gelu_grad(value_rows, grad_in):
    return jax.vjp(gelu_tanh, value_rows)[1](grad_in)[0]


def product(left_mat, right_mat):
    return jnp.dot(left_mat, right_mat, preferred_element_type=jnp.float32)


def product_tn(left_mat, right_mat):
    return lax.dot_general(
        left_mat, right_mat, (((0,), (0,)), ((), ())), preferred_element_type=jnp.float32
    )


def product_nt(left_mat, right_mat):
    return lax.dot_general(
        left_mat, right_mat, (((1,), (1,)), ((), ())), preferred_element_type=jnp.float32
    )


def low(values):
    return values.astype(jnp.bfloat16)


def exchange(blocks, axes):
    return lax.all_to_all(blocks, axes, split_axis=0, concat_axis=0, tiled=True)


def spread(block, axes):
    count = lax.axis_size(axes)
    return exchange(jnp.broadcast_to(block[None], (count,) + block.shape), axes)


def gather_rows(block):
    return lax.all_gather(block, DP, axis=0, tiled=True)


def sum_blocks(blocks):
    return jnp.sum(blocks.astype(jnp.float32), axis=0)


def row_blocks(partial_rows):
    return low(partial_rows).reshape(lax.axis_size(DP), -1, partial_rows.shape[-1])


def beside(move, blocks, work, operands, late=()):
    blocks, operands = lax.optimization_barrier((blocks, operands))
    return lax.optimization_barrier((move(blocks), work(*operands, *late)))


def started(operands, blocks):
    tile = blocks[0, :16, :128]
    return after(operands, other_core(tile))


def over_dp(blocks):
    return exchange(blocks, DP)


def over_homes(blocks):
    return exchange(blocks, HOMES)


def after(values, event):
    return lax.optimization_barrier((values, event))[0]


def permute_copies(block, axis):
    count = lax.axis_size(axis)
    blocks = [block]
    for step in range(1, count):
        route = [((i - step) % count, i) for i in range(count)]
        blocks.append(lax.ppermute(block, axis, route))
    return blocks


def own_parts(blocks, axis):
    count = lax.axis_size(axis)
    place = lax.axis_index(axis)
    return [
        lax.dynamic_index_in_dim(blocks, (place + step) % count, 0, keepdims=False)
        for step in range(count)
    ]


def sent_parts(parts, axis):
    count = len(parts)
    return [parts[0]] + [
        lax.ppermute(parts[step], axis, [((i - step) % count, i) for i in range(count)])
        for step in range(1, count)
    ]


def permute_parts(blocks, axis):
    return sent_parts(own_parts(blocks, axis), axis)


SCALAR = pl.BlockSpec(memory_space=pltpu.SMEM)
WHOLE = pl.BlockSpec(memory_space=pltpu.VMEM)


def in_order(blocks, axis):
    count = lax.axis_size(axis)

    def kernel(place, *refs):
        for step in range(count):
            refs[-1][(place[0] + count - step) % count] = refs[step][...]

    return pl.pallas_call(
        kernel,
        out_shape=jax.ShapeDtypeStruct((count,) + blocks[0].shape, blocks[0].dtype),
        in_specs=[SCALAR] + [WHOLE] * count,
        compiler_params=pltpu.CompilerParams(vmem_limit_bytes=32 << 20),
        name="in_order",
    )(lax.axis_index(axis).reshape(1), *blocks)


def finish_weights(section_id, ups, attns, down_sums, hidden_rows):
    dp_size, rows, half_hidden = ups[0].shape
    down_rows, half_width = down_sums[0].shape
    width = 2 * half_width
    head_width = width // dp_size
    qkv_half = 3 * head_width // 2

    def kernel(place, *refs):
        qkv_ref, proj_ref, up_ref, down_ref = refs[12:]

        def write(up_halves, attn_halves, down_halves):
            for half in range(2):
                up, attn = up_halves[half], attn_halves[half]
                here = slice(half * half_width, (half + 1) * half_width)
                proj_sum = attn[0, :, :half_width].astype(jnp.float32)
                for z in range(1, dp_size):
                    proj_sum = proj_sum + attn[z, :, :half_width].astype(jnp.float32)
                proj_ref[:, here] = proj_sum
                down_ref[:, here] = down_halves[half][...].astype(jnp.float32)
                for z in range(dp_size):
                    for piece in range(half_hidden // hidden_rows):
                        group = half * (half_hidden // hidden_rows) + piece
                        start = (group * dp_size + z) * hidden_rows
                        up_ref[:, start : start + hidden_rows] = up[
                            z, :, piece * hidden_rows : (piece + 1) * hidden_rows
                        ].astype(jnp.float32)
                    at = 0
                    while at < qkv_half:
                        column = half * qkv_half + at
                        part, inner = column // head_width, column % head_width
                        size = min(head_width - inner, qkv_half - at)
                        first = half_width + at
                        start = part * width + z * head_width + inner
                        qkv_ref[:, start : start + size] = attn[
                            z, :, first : first + size
                        ].astype(jnp.float32)
                        at = at + size

        @pl.when(place[0] == 0)
        def _():
            write(refs[0:2], refs[4:6], refs[8:10])

        @pl.when(place[0] != 0)
        def _():
            write(refs[3:1:-1], refs[7:5:-1], refs[11:9:-1])

    shapes = ((rows, 3 * width), (rows, width), (rows, 2 * half_hidden * dp_size), (down_rows, width))
    return pl.pallas_call(
        kernel,
        out_shape=[jax.ShapeDtypeStruct(shape, jnp.float32) for shape in shapes],
        in_specs=[SCALAR] + [WHOLE] * 12,
        compiler_params=pltpu.CompilerParams(vmem_limit_bytes=32 << 20),
        name="finish_weights",
    )(section_id.reshape(1), *ups, *attns, *down_sums)


def finish_rows(section_id, *arrays):
    count = len(arrays)

    def kernel(place, *refs):
        outs = refs[4 * count :]
        for index in range(count):
            own_zero, other_zero, own_one, other_one = refs[4 * index : 4 * index + 4]

            @pl.when(place[0] == 0)
            def _():
                outs[index][0] = own_zero[...]
                outs[index][1] = other_zero[...]

            @pl.when(place[0] != 0)
            def _():
                outs[index][0] = other_one[...]
                outs[index][1] = own_one[...]

    return pl.pallas_call(
        kernel,
        out_shape=[
            jax.ShapeDtypeStruct((2,) + array[0].shape, array[0].dtype) for array in arrays
        ],
        in_specs=[SCALAR] + [WHOLE] * (4 * count),
        compiler_params=pltpu.CompilerParams(vmem_limit_bytes=32 << 20),
        name="finish_rows",
    )(section_id.reshape(1), *[rows for array in arrays for rows in array])


def sum_parts(parts):
    return sum(part.astype(jnp.float32) for part in parts)


def softmax_rows(queries, keys, allowed):
    scores = product_nt(queries, keys) * 0.125
    scores = jnp.where(allowed, scores, -jnp.inf)
    exp_scores = jnp.exp(scores - jnp.max(scores, axis=-1, keepdims=True))
    return exp_scores / jnp.sum(exp_scores, axis=-1, keepdims=True)


def allowed_keys(seg_column, seg_row):
    rows, columns = seg_column.shape[0], seg_row.shape[1]
    query_at = lax.broadcasted_iota(jnp.int32, (rows, columns), 0)
    key_at = lax.broadcasted_iota(jnp.int32, (rows, columns), 1)
    return (seg_column == seg_row) & (key_at <= query_at)


def head_slices(packed, head, head_width):
    start = head * HEAD_DIM
    return [
        packed[:, part * head_width + start : part * head_width + start + HEAD_DIM]
        for part in range(3)
    ]


def attention_kernel(seg_column, seg_row, qkv_ref, mixed_ref):
    head_width = mixed_ref.shape[1]
    allowed = allowed_keys(seg_column[...], seg_row[...])
    packed = qkv_ref[...]
    mixed = []
    for head in range(head_width // HEAD_DIM):
        queries, keys, values = head_slices(packed, head, head_width)
        probs = softmax_rows(queries, keys, allowed)
        mixed.append(low(product(low(probs), values)))
    mixed_ref[...] = jnp.concatenate(mixed, axis=1)


def attention_back_kernel(seg_column, seg_row, qkv_ref, d_mixed_ref, d_qkv_ref):
    head_width = d_mixed_ref.shape[1]
    allowed = allowed_keys(seg_column[...], seg_row[...])
    packed = qkv_ref[...]
    d_mixed_all = d_mixed_ref[...]
    grads = [[], [], []]
    for head in range(head_width // HEAD_DIM):
        queries, keys, values = head_slices(packed, head, head_width)
        d_mixed = d_mixed_all[:, head * HEAD_DIM : (head + 1) * HEAD_DIM]
        probs = softmax_rows(queries, keys, allowed)
        d_probs = product_nt(d_mixed, values)
        d_scores = low(probs * (d_probs - jnp.sum(probs * d_probs, axis=-1, keepdims=True)))
        grads[0].append(low(product(d_scores, keys) * 0.125))
        grads[1].append(low(product_tn(d_scores, queries) * 0.125))
        grads[2].append(low(product_tn(low(probs), d_mixed)))
    d_qkv_ref[...] = jnp.concatenate(grads[0] + grads[1] + grads[2], axis=1)


def attention(segments, qkv):
    head_width = qkv.shape[1] // 3
    return pl.pallas_call(
        attention_kernel,
        out_shape=jax.ShapeDtypeStruct((qkv.shape[0], head_width), jnp.bfloat16),
        compiler_params=pltpu.CompilerParams(vmem_limit_bytes=32 << 20),
        name="attention",
    )(segments[:, None], segments[None, :], qkv)


def attention_back(segments, qkv, d_mixed):
    return pl.pallas_call(
        attention_back_kernel,
        out_shape=jax.ShapeDtypeStruct(qkv.shape, jnp.bfloat16),
        compiler_params=pltpu.CompilerParams(vmem_limit_bytes=32 << 20),
        name="attention_back",
    )(segments[:, None], segments[None, :], qkv, d_mixed)


def pair_grads(section_id, *pairs):
    mats = [side for left, right in pairs for side in (left, other_core(left), right, other_core(right))]
    left_width = pairs[0][0].shape[1]
    halves = [right.shape[1] // 2 for _, right in pairs]

    def kernel(place, *refs):
        start = 0
        for index, half in enumerate(halves):
            left_own, left_other, right_own, right_other = refs[4 * index : 4 * index + 4]
            here = pl.ds(pl.multiple_of(place[0] * half, LANES), half)
            total = product_tn(left_own[...], right_own[:, here])
            total = total + product_tn(left_other[...], right_other[:, here])
            refs[-1][:, start : start + half] = low(total)
            start = start + half

    return pl.pallas_call(
        kernel,
        out_shape=jax.ShapeDtypeStruct((left_width, sum(halves)), jnp.bfloat16),
        in_specs=[SCALAR] + [WHOLE] * len(mats),
        compiler_params=pltpu.CompilerParams(vmem_limit_bytes=40 << 20),
        name="pair_grads",
    )(section_id.reshape(1), *mats)


OWNER_TILE = 256


def owner_grads(section_id, left_mats, right_mats):
    rows, left_width = left_mats[0].shape
    right_width = right_mats[0].shape[1]
    tiles = left_width // OWNER_TILE

    def kernel(place, *refs):
        out_ref = refs[8]
        expert, tile = pl.program_id(0), pl.program_id(1)
        first = place[0] == 0
        for source, here in enumerate(
            (
                first & (expert == 0),
                first & (expert == 1),
                ~first & (expert == 1),
                ~first & (expert == 0),
            )
        ):

            @pl.when(here)
            def _():
                left = refs[source][:, pl.ds(tile * OWNER_TILE, OWNER_TILE)]
                out_ref[0] = product_tn(left, refs[4 + source][...])

    whole = [
        pl.BlockSpec(mat.shape, lambda expert, tile: (0, 0))
        for mat in (*left_mats, *right_mats)
    ]
    return pl.pallas_call(
        kernel,
        out_shape=jax.ShapeDtypeStruct((2, left_width, right_width), jnp.float32),
        grid=(2, tiles),
        in_specs=[pl.BlockSpec(memory_space=pltpu.SMEM)] + whole,
        out_specs=pl.BlockSpec((1, OWNER_TILE, right_width), lambda expert, tile: (expert, tile, 0)),
        compiler_params=pltpu.CompilerParams(vmem_limit_bytes=40 << 20),
        name="owner_grads",
    )(section_id.reshape(1), *left_mats, *right_mats)


def statistics(value_rows):
    centre = jnp.mean(value_rows, axis=-1, keepdims=True)
    centred = value_rows - centre
    variance = jnp.mean(centred * centred, axis=-1, keepdims=True)
    spread_inverse = lax.rsqrt(variance + 1e-05)
    return centred * spread_inverse, spread_inverse


def column_sums(value_rows):
    return jnp.sum(value_rows, axis=0, keepdims=True)


def block_sum(blocks_ref):
    total = blocks_ref[0].astype(jnp.float32)
    for place in range(1, blocks_ref.shape[0]):
        total = total + blocks_ref[place].astype(jnp.float32)
    return total


def call(kernel, name, outs, *operands):
    specs = [
        pl.BlockSpec(memory_space=pl.ANY) if operand.shape[1:] == (operand.shape[-1],) * 2 else WHOLE
        for operand in operands
    ]
    mats = [operand.shape[1:] for operand, spec in zip(operands, specs) if spec is not WHOLE]
    scratch = [pltpu.VMEM(shape, jnp.bfloat16) for shape in mats]
    scratch += [pltpu.SemaphoreType.DMA for _ in mats]
    return pl.pallas_call(
        kernel,
        in_specs=specs,
        out_shape=[jax.ShapeDtypeStruct(shape, dtype) for shape, dtype in outs],
        scratch_shapes=scratch,
        compiler_params=pltpu.CompilerParams(vmem_limit_bytes=32 << 20),
        name=name,
    )(*operands)


def project(layer, mixed_blocks, proj_mat, layer_in, gain, shift):
    def kernel(mixed_ref, proj_ref, in_ref, gain_ref, shift_ref, *outs):
        rows_ref, res_ref, mid_ref, sq_ref, proj_here, arrived = outs
        fetch = pltpu.make_async_copy(proj_ref.at[layer], proj_here, arrived)
        fetch.start()
        places = mixed_ref.shape[0]
        mixed = jnp.concatenate([mixed_ref[place] for place in range(places)], axis=1)
        rows_ref[...] = mixed
        fetch.wait()
        branch = product(mixed, proj_here[...])
        residual = in_ref[...].astype(jnp.float32) + branch
        res_ref[...] = residual
        mid_ref[...] = low(statistics(residual)[0] * gain_ref[...] + shift_ref[...])
        sq_ref[...] = column_sums(branch * branch)

    rows, width = layer_in.shape
    outs = [((rows, width), jnp.bfloat16), ((rows, width), jnp.float32)]
    outs += [((rows, width), jnp.bfloat16), ((1, width), jnp.float32)]
    return call(kernel, "project", outs, mixed_blocks, proj_mat, layer_in, gain, shift)


def layer_end(branch_blocks, residual, gain, shift):
    def kernel(blocks_ref, res_ref, gain_ref, shift_ref, out_ref, normed_ref, sq_ref):
        branch = block_sum(blocks_ref)
        layer_out = res_ref[...] + branch
        rounded = low(layer_out)
        out_ref[...] = rounded
        normed = statistics(rounded.astype(jnp.float32))[0]
        normed_ref[...] = low(normed * gain_ref[...] + shift_ref[...])
        sq_ref[0:1] = column_sums(branch * branch)
        sq_ref[1:2] = column_sums(layer_out * layer_out)

    shape = residual.shape
    outs = [(shape, jnp.bfloat16), (shape, jnp.bfloat16), ((2, shape[1]), jnp.float32)]
    return call(kernel, "layer_end", outs, branch_blocks, residual, gain, shift)


def norm_back(blocks_ref, value_ref, gain_ref, grad_ref, gain_grad_ref, shift_grad_ref):
    d_normed = block_sum(blocks_ref)
    normed, spread_inverse = statistics(value_ref[...].astype(jnp.float32))
    gain_grad_ref[...] = column_sums(d_normed * normed)
    shift_grad_ref[...] = column_sums(d_normed)
    d_centred = d_normed * gain_ref[...]
    along = jnp.mean(d_centred * normed, axis=-1, keepdims=True)
    d_value = d_centred - jnp.mean(d_centred, axis=-1, keepdims=True) - normed * along
    return grad_ref[...].astype(jnp.float32) + d_value * spread_inverse


def mid_back(layer, mid_blocks, residual, gain, grad_out, proj_mat, dp_size):
    def kernel(blocks_ref, res_ref, gain_ref, grad_ref, proj_ref, *outs):
        sum_ref, low_ref, mixed_ref, gain_grad_ref, shift_grad_ref, proj_here, arrived = outs
        fetch = pltpu.make_async_copy(proj_ref.at[layer], proj_here, arrived)
        fetch.start()
        grad = norm_back(blocks_ref, res_ref, gain_ref, grad_ref, gain_grad_ref, shift_grad_ref)
        sum_ref[...] = grad
        low_ref[...] = low(grad)
        fetch.wait()
        d_mixed = low(product_nt(low(grad), proj_here[...]))
        part = d_mixed.shape[1] // dp_size
        for place in range(dp_size):
            mixed_ref[place] = d_mixed[:, place * part : (place + 1) * part]

    rows, width = residual.shape
    row = ((1, width), jnp.float32)
    outs = [((rows, width), jnp.float32), ((rows, width), jnp.bfloat16)]
    outs += [((dp_size, rows, width // dp_size), jnp.bfloat16), row, row]
    return call(kernel, "mid_back", outs, mid_blocks, residual, gain, grad_out, proj_mat)


def input_back(in_blocks, layer_in, gain, grad_resid):
    def kernel(blocks_ref, in_ref, gain_ref, grad_ref, sum_ref, low_ref, gain_grad_ref, shift_grad_ref):
        grad = norm_back(blocks_ref, in_ref, gain_ref, grad_ref, gain_grad_ref, shift_grad_ref)
        sum_ref[...] = grad
        low_ref[...] = low(grad)

    shape = layer_in.shape
    row = ((1, shape[1]), jnp.float32)
    outs = [(shape, jnp.float32), (shape, jnp.bfloat16), row, row]
    return call(kernel, "input_back", outs, in_blocks, layer_in, gain, grad_resid)


def pack_small(parts_of_layers, squares_of_layers, weight_rows):
    layers = len(parts_of_layers)
    flat = [part for parts in parts_of_layers for part in parts] + list(squares_of_layers)
    width = flat[0].shape[1]
    used = sum(part.shape[0] for part in parts_of_layers[0])
    height = -(-(used + 1) // 8) * 8
    places = width // weight_rows

    def kernel(*refs):
        out_ref, rows_ref = refs[-2], refs[-1]
        per_layer = len(parts_of_layers[0])
        for layer in range(layers):
            rows_ref[...] = jnp.zeros(rows_ref.shape, jnp.float32)
            start = 0
            for part in refs[layer * per_layer : (layer + 1) * per_layer]:
                rows_ref[start : start + part.shape[0]] = part[...]
                start = start + part.shape[0]
            lane = lax.broadcasted_iota(jnp.int32, (1, width), 1) % LANES
            marked = jnp.zeros((1, width), jnp.float32)
            sums = jnp.sum(refs[layers * per_layer + layer][...], axis=1, keepdims=True)
            for kind in range(3):
                marked = jnp.where(lane == kind, sums[kind : kind + 1], marked)
            rows_ref[start : start + 1] = marked
            for place in range(places):
                column = place * weight_rows // LANES * LANES
                out_ref[layer * places + place] = rows_ref[:, column : column + LANES]

    return pl.pallas_call(
        kernel,
        out_shape=jax.ShapeDtypeStruct((layers * places, height, LANES), jnp.float32),
        scratch_shapes=[pltpu.VMEM((height, width), jnp.float32)],
        name="pack_small",
    )(*flat)


def other_core(block):
    return lax.ppermute(block, SEC, [(0, 1), (1, 0)])


def shards(
    inputs,
    cotangent,
    segment_ids,
    routes,
    norm_gains,
    norm_shifts,
    attn_qkv,
    attn_proj,
    dense_up,
    dense_down,
    router,
    mixer,
    expert_up,
    expert_down,
):
    sections = lax.axis_size(SEC)
    groups = lax.axis_size(EX)
    dp_size = lax.axis_size(DP)
    section_id = lax.axis_index(SEC)
    expert_id = lax.axis_index(EX)
    micro_count = inputs.shape[0]
    seq_rows = inputs.shape[2]
    width = inputs.shape[3]
    full_len = segment_ids.shape[2]
    experts_total = router.shape[2]
    hidden_rows = dense_down.shape[1]
    weight_rows = attn_qkv.shape[1]
    heads_here = HEADS // dp_size
    head_width = heads_here * HEAD_DIM
    capacity = max(2, 5 * seq_rows // (4 * experts_total))
    slots = dp_size * capacity
    devices = sections * groups * dp_size

    small_parts = jnp.concatenate([norm_gains[0], norm_shifts[0], router[0].T, mixer[0].T], axis=0)
    small_count = small_parts.shape[0]
    route_row = low(routes[0, :, 0, :, 0])
    message = jnp.concatenate([small_parts.reshape(-1), route_row.reshape(-1)])
    filled = message.shape[0]
    padded = -(-filled // 1024) * 1024
    message = jnp.pad(message, (0, padded - filled)).reshape(padded // 128, 128)

    def expert_parts(*own_layers):
        return [
            (
                lax.dynamic_index_in_dim(own_layer, section_id, 0, keepdims=False),
                lax.dynamic_index_in_dim(own_layer, 1 - section_id, 0, keepdims=False),
            )
            for own_layer in own_layers
        ]

    hidden_here = groups * hidden_rows
    small_all, (proj_rows, up_parts) = beside(
        lambda blocks: exchange(blocks, EVERY),
        jnp.broadcast_to(message[None], (devices,) + message.shape),
        lambda proj_shard, up_cols: (
            in_order(permute_copies(proj_shard, DP), DP),
            own_parts(
                up_cols.reshape(weight_rows, groups, dp_size, hidden_rows)
                .transpose(2, 0, 1, 3)
                .reshape(dp_size, weight_rows, hidden_here),
                DP,
            ),
        ),
        (attn_proj[0], dense_up[0]),
    )
    small_all = small_all.reshape(sections, groups, dp_size, padded)

    def params_of(small_all):
        params_all = small_all[..., : small_count * weight_rows].reshape(
            sections, groups * dp_size, small_count, weight_rows
        )
        return params_all.transpose(0, 2, 1, 3).reshape(sections, small_count, width)

    def routes_of(small_all):
        routes_all = lax.dynamic_index_in_dim(
            small_all[..., small_count * weight_rows : filled], expert_id, 1, keepdims=False
        ).reshape(sections, dp_size, micro_count, seq_rows)
        routes_all = lax.dynamic_index_in_dim(routes_all, section_id, 2, keepdims=False)
        return routes_all.astype(jnp.int32)

    on_first = section_id == 0

    def by_layer(pair):
        of_own_layer, of_other_layer = pair
        return (
            jnp.where(on_first, of_own_layer, of_other_layer),
            jnp.where(on_first, of_other_layer, of_own_layer),
        )

    proj_both = lax.all_gather(proj_rows.reshape(-1, width), HOMES, axis=0, tiled=True)
    proj_both = proj_both.reshape(sections, width, width)
    qkv_cols = attn_qkv[0].reshape(weight_rows, 3, dp_size, head_width).transpose(2, 0, 1, 3)
    qkv_cols, small_all = lax.optimization_barrier(
        (qkv_cols.reshape(dp_size, weight_rows, 3 * head_width), small_all)
    )
    qkv_cols, expert_weights = beside(
        over_dp, qkv_cols, expert_parts, (expert_up[0], expert_down[0])
    )
    params_all = params_of(small_all)
    routes_all = routes_of(small_all)
    own_input = lax.dynamic_index_in_dim(inputs[:, 0], section_id, 0, keepdims=False)
    first_params = params_all[0].astype(jnp.float32)
    first_normed = low(
        layer_norm(own_input.astype(jnp.float32), first_params[0:1], first_params[2:3])
    )
    down_both = lax.all_gather(dense_down[0], HOMES, axis=0, tiled=True)
    qkv_own, (first_seq, up_rows, down_both) = beside(
        lambda blocks: exchange(blocks, EX),
        jnp.broadcast_to(qkv_cols[None], (groups,) + qkv_cols.shape),
        lambda rows, parts, down_both: (
            in_order(permute_copies(rows, DP), DP),
            in_order(sent_parts(parts, DP), DP),
            down_both,
        ),
        (first_normed, up_parts),
        (down_both,),
    )
    first_seq = first_seq.reshape(full_len, width)
    qkv_own = qkv_own.reshape(width, 3 * head_width)
    qkv_pair = (qkv_own, other_core(qkv_own))
    exp_up_pair, exp_down_pair = [(kept, other_core(sent)) for kept, sent in expert_weights]
    first_qkv = low(product(first_seq, by_layer(qkv_pair)[0]))
    up_both = lax.all_gather(up_rows.reshape(-1, hidden_here), HOMES, axis=0, tiled=True)
    up_both = up_both.reshape(sections, width, hidden_here)
    down_both = down_both.reshape(sections, hidden_here, width)

    segments = lax.dynamic_index_in_dim(segment_ids[:, 0], section_id, 0, keepdims=False)
    places = jnp.arange(full_len, dtype=jnp.int32)
    earlier = (places[None, :] < places[:, None]) & (
        places[None, :] // seq_rows == places[:, None] // seq_rows
    )

    def slot_table(route_now):
        rank = jnp.sum(
            ((route_now[:, None] == route_now[None, :]) & earlier).astype(jnp.int32), axis=1
        )
        home = route_now % sections * groups + route_now // sections
        target = home * slots + places // seq_rows * capacity + rank
        slot_ids = jnp.arange(sections * groups * slots, dtype=jnp.int32)
        table = low(slot_ids[:, None] == target[None, :])
        hot = route_now[:, None] == jnp.arange(experts_total, dtype=jnp.int32)[None, :]
        return table, hot.astype(jnp.float32)

    def packed_rows(token_rows, table):
        return low(product(table, token_rows)).reshape(sections * groups, slots, width)

    def coefficients(mid_seq, small_weights, hot):
        small_logits = product_nt(mid_seq, small_weights)
        gate_probs = jax.nn.softmax(small_logits[:, :experts_total], axis=-1)
        gate = jnp.sum(gate_probs * hot, axis=-1, keepdims=True)
        coef = jax.nn.softmax(small_logits[:, experts_total:], axis=-1)
        return gate_probs, gate, coef

    own_expert = (
        jnp.arange(experts_total, dtype=jnp.int32)[None, :] == expert_id * sections + section_id
    ).astype(jnp.float32)

    def row_scale(expert_rows, small_weights):
        _, gate, coef = coefficients(expert_rows, small_weights, own_expert)
        return coef[:, 1:2] * gate

    def dense_in(mid_seq, up_mat):
        hidden = product(mid_seq, up_mat)
        return hidden, low(gelu_tanh(hidden))

    def attended(qkv):
        return attention(segments, qkv).reshape(dp_size, seq_rows, head_width)

    def forward_zero():
        params = first_params
        table, hot = slot_table(routes_all[0].reshape(full_len))
        mixed, residual, mid, attn_squares = project(
            0, over_dp(attended(first_qkv)), proj_both, own_input, params[1:2], params[3:4]
        )
        mid_seq = gather_rows(mid)
        small_weights = params_all[0, 4:]
        exp_up_mat, exp_down_mat = by_layer(exp_up_pair)[0], by_layer(exp_down_pair)[0]

        expert_rows, ((gate_probs, gate, coef), own_grad_seq) = beside(
            over_homes,
            packed_rows(mid_seq, table),
            lambda mid_seq, small_weights, grad: (
                coefficients(mid_seq, small_weights, hot),
                in_order(permute_copies(grad, DP), DP).reshape(full_len, width),
            ),
            (mid_seq, small_weights, own_grad),
        )
        expert_rows = expert_rows.reshape(-1, width)
        exp_hidden = product(expert_rows, exp_up_mat)
        exp_hidden_low = low(gelu_tanh(exp_hidden))

        def return_work(mid_seq, expert_rows, up_mat, down_mat):
            hidden, hidden_low = dense_in(mid_seq, up_mat)
            scale = row_scale(expert_rows, small_weights)
            return scale, hidden, hidden_low, product(hidden_low, down_mat)

        returned, (scale, hidden, hidden_low, dense_part) = beside(
            over_homes,
            low(product(exp_hidden_low, exp_down_mat)).reshape(-1, slots, width),
            return_work,
            (mid_seq, expert_rows),
            (up_both[0], down_both[0]),
        )
        expert_part = product_tn(table, returned.reshape(-1, width))
        branch_part = coef[:, 0:1] * dense_part + coef[:, 1:2] * gate * expert_part
        branch, settled = beside(
            over_dp,
            row_blocks(branch_part),
            lambda *pairs: [by_layer(pair) for pair in pairs],
            (qkv_pair, exp_up_pair, exp_down_pair),
        )
        next_params = params_all[1].astype(jnp.float32)
        out_low, next_normed, squares = layer_end(
            branch, residual, next_params[0:1], next_params[2:3]
        )
        record = SimpleNamespace(
            params=params,
            small_weights=small_weights,
            table=table,
            hot=hot,
            layer_in=own_input,
            normed_seq=first_seq,
            qkv=first_qkv,
            mixed=mixed,
            residual=residual,
            mid_seq=mid_seq,
            expert_rows=expert_rows,
            scale=scale,
            gate_probs=gate_probs,
            gate=gate,
            coef=coef,
            hidden=hidden,
            hidden_low=hidden_low,
            dense_part=dense_part,
            exp_hidden=exp_hidden,
            exp_hidden_low=exp_hidden_low,
            expert_part=expert_part,
        )
        squares = jnp.concatenate([attn_squares, squares], axis=0)
        return out_low, next_normed, squares, record, (*settled, own_grad_seq)

    def forward_one(layer_in, normed, own_grad_seq):
        params = params_all[1].astype(jnp.float32)
        table, hot = slot_table(routes_all[1].reshape(full_len))
        normed_seq = gather_rows(normed)
        qkv = low(product(normed_seq, qkv_both[1]))
        mixed, up_apart = beside(
            over_dp, attended(qkv), lambda mats: (mats[0], mats[1]), (up_both,)
        )
        mixed, residual, mid, attn_squares = project(
            1, mixed, proj_both, layer_in, params[1:2], params[3:4]
        )
        grad_rows, mid_seq = beside(
            over_homes, packed_rows(own_grad_seq, table), gather_rows, (mid,)
        )
        small_weights = params_all[1, 4:]

        def dispatch_work(mid_seq, small_weights, up_mat, down_both):
            return (
                coefficients(mid_seq, small_weights, hot),
                dense_in(mid_seq, up_mat),
                (down_both[0], down_both[1]),
            )

        expert_rows, ((gate_probs, gate, coef), (hidden, hidden_low), down_apart) = beside(
            over_homes,
            packed_rows(mid_seq, table),
            dispatch_work,
            (mid_seq, small_weights, up_apart[1], down_both),
        )
        expert_rows = expert_rows.reshape(-1, width)
        exp_hidden = product(expert_rows, exp_up_both[1])
        exp_hidden_low = low(gelu_tanh(exp_hidden))
        returned, (dense_part, scale) = beside(
            over_homes,
            low(product(exp_hidden_low, exp_down_both[1])).reshape(-1, slots, width),
            lambda hidden_low, down_mat, expert_rows: (
                product(hidden_low, down_mat),
                row_scale(expert_rows, small_weights),
            ),
            (hidden_low, down_apart[1], expert_rows),
        )
        expert_part = product_tn(table, returned.reshape(-1, width))
        branch_part = coef[:, 0:1] * dense_part + coef[:, 1:2] * gate * expert_part
        branch = lax.psum_scatter(low(branch_part), DP, scatter_dimension=0, tiled=True)
        record = SimpleNamespace(
            params=params,
            small_weights=small_weights,
            table=table,
            hot=hot,
            layer_in=layer_in,
            normed_seq=normed_seq,
            qkv=qkv,
            mixed=mixed,
            residual=residual,
            mid_seq=mid_seq,
            expert_rows=expert_rows,
            scale=scale,
            gate_probs=gate_probs,
            gate=gate,
            coef=coef,
            hidden=hidden,
            hidden_low=hidden_low,
            dense_part=dense_part,
            exp_hidden=exp_hidden,
            exp_hidden_low=exp_hidden_low,
            expert_part=expert_part,
        )
        return branch, attn_squares, record, grad_rows, up_apart, down_apart

    def over_expert(grad_mat):
        return lax.psum_scatter(grad_mat, EX, scatter_dimension=0, tiled=True)

    def by_rows(grad_mat, count):
        return low(grad_mat).reshape(count, -1, grad_mat.shape[-1])

    def dp_blocks(*grad_mats):
        blocks = [by_rows(grad_mat, dp_size) for grad_mat in grad_mats]
        return own_parts(jnp.concatenate(blocks, axis=2), DP)

    half_hidden, half_width = hidden_here // 2, width // 2

    def backward_layer(layer, grad_low, grad_seq, record, sums_one=(), operands_one=None, settle=(), grad_rows=None):
        params = record.params
        coef, gate, table = record.coef, record.gate, record.table
        def dense_back(grad_seq, coef, down_mat, up_mat, *sums_one):
            grad_seq = grad_seq.astype(jnp.float32)
            early = dp_blocks(*sums_one) if sums_one else ()
            d_dense = low(coef[:, 0:1] * grad_seq)
            dense_dot = jnp.sum(grad_seq * record.dense_part, axis=-1, keepdims=True)
            expert_dot = jnp.sum(grad_seq * record.expert_part, axis=-1, keepdims=True)
            d_coef = jnp.concatenate([dense_dot, gate * expert_dot], axis=1)
            d_mix = coef * (d_coef - jnp.sum(coef * d_coef, axis=-1, keepdims=True))
            d_logits = record.gate_probs * (record.hot - gate) * (coef[:, 1:2] * expert_dot)
            d_small = low(jnp.concatenate([d_logits, d_mix], axis=1))
            d_up = low(gelu_grad(record.hidden, product_nt(d_dense, down_mat)))
            d_mid_part = product_nt(d_up, up_mat) + product(d_small, record.small_weights)
            return d_dense, d_small, d_up, d_mid_part, early

        dense_operands = (grad_seq, coef, down_apart[layer], up_apart[layer])
        if layer == 0:
            grad_rows, dense_grad = beside(
                over_homes,
                packed_rows(grad_seq, table),
                dense_back,
                dense_operands,
                tuple(sums_one),
            )
        expert_grad_rows = low(
            record.scale * grad_rows.reshape(-1, width).astype(jnp.float32)
        )
        d_exp_hidden = low(
            gelu_grad(record.exp_hidden, product_nt(expert_grad_rows, exp_down_both[layer]))
        )
        expert_operands = (
            record.expert_rows,
            d_exp_hidden,
            record.exp_hidden_low,
            expert_grad_rows,
        )

        swapped = tuple(other_core(operand) for operand in expert_operands)

        def owner_mats(index):
            return (
                expert_operands[index],
                swapped[index],
                operands_one[0][index],
                operands_one[1][index],
            )

        def dense_grads(hidden_low, d_dense, mid_seq, d_up, d_small):
            g_dense = pair_grads(section_id, (mid_seq, d_up), (hidden_low, d_dense))
            return g_dense, product_tn(d_small, mid_seq)

        expert_back = low(product_nt(d_exp_hidden, exp_up_both[layer])).reshape(-1, slots, width)
        if layer == 0:
            returned, (parts_one, g_exp_down) = beside(
                over_homes,
                expert_back,
                lambda early, *mats: (sent_parts(early, DP), owner_grads(section_id, *mats)),
                (dense_grad[4], owner_mats(2), owner_mats(3)),
            )
        else:
            returned, dense_grad = beside(
                over_homes,
                expert_back,
                lambda blocks, *operands: dense_back(*started(operands, blocks)),
                (expert_back, *dense_operands),
            )
        d_dense, d_small, d_up, d_mid_part, _ = dense_grad
        d_mid_part = d_mid_part + product_tn(table, returned.reshape(-1, width))
        mid_blocks, operands = lax.optimization_barrier(
            (
                row_blocks(d_mid_part),
                (record.hidden_low, d_dense, record.mid_seq, d_up, d_small),
            )
        )
        g_dense, g_small = dense_grads(*operands)
        d_mid, g_dense, g_small = lax.optimization_barrier(
            (over_dp(mid_blocks), g_dense, g_small)
        )
        dense_sum = over_expert(g_dense)
        d_resid, d_attn, d_mixed, d_gain_one, d_shift_one = mid_back(
            layer, d_mid, record.residual, params[1:2], grad_low, proj_both, dp_size
        )
        d_mixed = over_dp(d_mixed)

        def attention_grads(d_mixed):
            d_qkv = attention_back(segments, record.qkv, d_mixed.reshape(full_len, head_width))
            return d_qkv, row_blocks(product_nt(d_qkv, qkv_both[layer]))

        d_qkv, in_blocks = attention_grads(d_mixed)
        in_blocks, normed_seq, d_qkv = lax.optimization_barrier(
            (in_blocks, record.normed_seq, d_qkv)
        )
        g_attn = pair_grads(section_id, (record.mixed, d_attn), (normed_seq, d_qkv))
        attn_sum = over_expert(g_attn)
        beside_it = (g_attn, settle)
        d_normed, beside_it = lax.optimization_barrier((over_dp(in_blocks), beside_it))
        d_input, d_input_low, d_gain_zero, d_shift_zero = input_back(
            d_normed, record.layer_in, params[0:1], d_resid
        )
        small_grads = (d_gain_zero, d_gain_one, d_shift_zero, d_shift_one, g_small)
        if layer == 0:
            extra = (parts_one, owner_mats, g_exp_down)
        else:
            extra = (expert_operands, swapped, beside_it[1])
        return d_input, d_input_low, (dense_sum, attn_sum), small_grads, extra

    own_grad = lax.dynamic_index_in_dim(cotangent[:, 0], section_id, 0, keepdims=False)
    out_zero, next_normed, squares_zero, record_zero, settled = forward_zero()
    qkv_both, exp_up_both, exp_down_both, own_grad_seq = settled
    branch_one, attn_squares_one, record_one, grad_rows, up_apart, down_apart = forward_one(
        out_zero, next_normed, own_grad_seq
    )
    grad_one, grad_one_low, sums_one, small_one, operands_one = backward_layer(
        1, own_grad, own_grad_seq, record_one, settle=branch_one, grad_rows=grad_rows
    )
    dense_one, attn_one = sums_one
    branch_one = operands_one[2].astype(jnp.float32)
    out_one = record_one.residual + branch_one
    squares_one = jnp.concatenate(
        [attn_squares_one, column_sums(branch_one * branch_one), column_sums(out_one * out_one)]
    )
    out_one = low(out_one)
    grad_zero, _, (dense_zero, attn_zero), small_zero, extra = backward_layer(
        0,
        grad_one_low,
        gather_rows(grad_one_low),
        record_zero,
        (dense_one[:, :half_hidden], attn_one),
        operands_one,
    )
    parts_one, owner_mats, grad_exp_down = extra

    moved_one = in_order(after(parts_one, grad_zero), DP)
    small_message = pack_small(
        (small_zero, small_one), (squares_zero, squares_one), weight_rows
    )
    small_moved, grad_exp_up = beside(
        lambda blocks: exchange(blocks, EVERY),
        small_message,
        lambda *mats: owner_grads(section_id, *mats),
        (owner_mats(0), owner_mats(1)),
    )
    up_zero = over_dp(by_rows(after(dense_zero[:, :half_hidden], small_moved), dp_size))
    attn_zero = over_dp(by_rows(after(attn_zero, up_zero), dp_size))
    up_one, attn_one = moved_one[..., :half_hidden], moved_one[..., half_hidden:]
    down_zero, down_one = dense_zero[:, half_hidden:], dense_one[:, half_hidden:]

    def of_both(of_zero, of_one):
        return of_zero, other_core(of_zero), of_one, other_core(of_one)

    grad_qkv, grad_proj, grad_up, grad_down = finish_weights(
        section_id,
        of_both(up_zero, up_one),
        of_both(attn_zero, attn_one),
        of_both(down_zero, down_one),
        hidden_rows,
    )
    activations, input_grads = finish_rows(
        section_id, of_both(out_zero, out_one), of_both(grad_zero, grad_one)
    )
    small_sum = jnp.sum(small_moved, axis=0)
    place = expert_id * dp_size + lax.axis_index(DP)
    sums = lax.dynamic_slice_in_dim(
        small_sum[:small_count], place * weight_rows % LANES, weight_rows, axis=1
    )
    totals = small_sum[small_count, :3]
    element_count = micro_count * seq_rows * width * groups * dp_size
    branch_rms = jnp.sqrt(totals / element_count)[None]
    return (
        activations[None, :, None],
        input_grads[None, :, None],
        sums[None, 0:2],
        sums[None, 2:4],
        grad_qkv[None],
        grad_proj[None],
        grad_up[None],
        grad_down[None],
        sums[4 : 4 + experts_total].T[None],
        sums[4 + experts_total :].T[None],
        grad_exp_up[None],
        grad_exp_down[None],
        branch_rms,
    )


def solution(mesh):
    placed = (
        P(None, EX, DP, None),
        P(None, EX, DP, None),
        P(None, EX, None),
        P(SEC, None, EX, DP, None),
        P(SEC, None, (EX, DP)),
        P(SEC, None, (EX, DP)),
        P(SEC, (EX, DP), None),
        P(SEC, (EX, DP), None),
        P(SEC, (EX, DP), None),
        P(SEC, (EX, DP), None),
        P(SEC, (EX, DP), None),
        P(SEC, (EX, DP), None),
        P(SEC, EX, None, DP),
        P(SEC, EX, DP, None),
    )
    return jax.shard_map(
        shards,
        mesh=mesh,
        in_specs=placed,
        out_specs=(
            P(SEC, None, EX, DP, None),
            P(SEC, None, EX, DP, None),
            P(SEC, None, (EX, DP)),
            P(SEC, None, (EX, DP)),
            P(SEC, (EX, DP), None),
            P(SEC, (EX, DP), None),
            P(SEC, (EX, DP), None),
            P(SEC, (EX, DP), None),
            P(SEC, (EX, DP), None),
            P(SEC, (EX, DP), None),
            P(SEC, EX, None, DP),
            P(SEC, EX, DP, None),
            P(SEC, None),
        ),
        check_vma=False,
    )
```

```python
from types import SimpleNamespace

import jax
import jax.numpy as jnp
from jax import lax
from jax.experimental import pallas as pl
from jax.experimental.pallas import tpu as pltpu
from jax.sharding import PartitionSpec as P

HEADS = 16
HEAD_DIM = 64
SEC, EX, DP = "section", "expert", "dp"
EVERY = (SEC, EX, DP)
HOMES = (SEC, EX)
LANES = 128


def layer_norm(value_rows, gain_vec, shift_vec):
    centre = jnp.mean(value_rows, axis=-1, keepdims=True)
    centred = value_rows - centre
    variance = jnp.mean(centred * centred, axis=-1, keepdims=True)
    return centred * lax.rsqrt(variance + 1e-05) * gain_vec + shift_vec


def gelu_tanh(value_rows):
    return jax.nn.gelu(value_rows, approximate=True)


def gelu_grad(value_rows, grad_in):
    return jax.vjp(gelu_tanh, value_rows)[1](grad_in)[0]


def product(left_mat, right_mat):
    return jnp.dot(left_mat, right_mat, preferred_element_type=jnp.float32)


def product_tn(left_mat, right_mat):
    return lax.dot_general(
        left_mat, right_mat, (((0,), (0,)), ((), ())), preferred_element_type=jnp.float32
    )


def product_nt(left_mat, right_mat):
    return lax.dot_general(
        left_mat, right_mat, (((1,), (1,)), ((), ())), preferred_element_type=jnp.float32
    )


def low(values):
    return values.astype(jnp.bfloat16)


def exchange(blocks, axes):
    return lax.all_to_all(blocks, axes, split_axis=0, concat_axis=0, tiled=True)


def spread(block, axes):
    count = lax.axis_size(axes)
    return exchange(jnp.broadcast_to(block[None], (count,) + block.shape), axes)


def gather_rows(block):
    return lax.all_gather(block, DP, axis=0, tiled=True)


def sum_blocks(blocks):
    return jnp.sum(blocks.astype(jnp.float32), axis=0)


def row_blocks(partial_rows):
    return low(partial_rows).reshape(lax.axis_size(DP), -1, partial_rows.shape[-1])


def beside(move, blocks, work, operands, late=()):
    blocks, operands = lax.optimization_barrier((blocks, operands))
    return lax.optimization_barrier((move(blocks), work(*operands, *late)))


def started(operands, blocks):
    tile = blocks[0, :16, :128]
    return after(operands, other_core(tile))


def over_dp(blocks):
    return exchange(blocks, DP)


def over_homes(blocks):
    return exchange(blocks, HOMES)


def after(values, event):
    return lax.optimization_barrier((values, event))[0]


def permute_copies(block, axis):
    count = lax.axis_size(axis)
    blocks = [block]
    for step in range(1, count):
        route = [((i - step) % count, i) for i in range(count)]
        blocks.append(lax.ppermute(block, axis, route))
    return blocks


def own_parts(blocks, axis):
    count = lax.axis_size(axis)
    place = lax.axis_index(axis)
    return [
        lax.dynamic_index_in_dim(blocks, (place + step) % count, 0, keepdims=False)
        for step in range(count)
    ]


def sent_parts(parts, axis):
    count = len(parts)
    return [parts[0]] + [
        lax.ppermute(parts[step], axis, [((i - step) % count, i) for i in range(count)])
        for step in range(1, count)
    ]


def permute_parts(blocks, axis):
    return sent_parts(own_parts(blocks, axis), axis)


SCALAR = pl.BlockSpec(memory_space=pltpu.SMEM)
WHOLE = pl.BlockSpec(memory_space=pltpu.VMEM)


def in_order(blocks, axis):
    count = lax.axis_size(axis)

    def kernel(place, *refs):
        for step in range(count):
            refs[-1][(place[0] + count - step) % count] = refs[step][...]

    return pl.pallas_call(
        kernel,
        out_shape=jax.ShapeDtypeStruct((count,) + blocks[0].shape, blocks[0].dtype),
        in_specs=[SCALAR] + [WHOLE] * count,
        compiler_params=pltpu.CompilerParams(vmem_limit_bytes=32 << 20),
        name="in_order",
    )(lax.axis_index(axis).reshape(1), *blocks)


def finish_weights(section_id, ups, attns, down_sums, hidden_rows):
    dp_size, rows, half_hidden = ups[0].shape
    down_rows, half_width = down_sums[0].shape
    width = 2 * half_width
    head_width = width // dp_size
    qkv_half = 3 * head_width // 2

    def kernel(place, *refs):
        qkv_ref, proj_ref, up_ref, down_ref = refs[12:]

        def write(up_halves, attn_halves, down_halves):
            for half in range(2):
                up, attn = up_halves[half], attn_halves[half]
                here = slice(half * half_width, (half + 1) * half_width)
                proj_sum = attn[0, :, :half_width].astype(jnp.float32)
                for z in range(1, dp_size):
                    proj_sum = proj_sum + attn[z, :, :half_width].astype(jnp.float32)
                proj_ref[:, here] = proj_sum
                down_ref[:, here] = down_halves[half][...].astype(jnp.float32)
                for z in range(dp_size):
                    for piece in range(half_hidden // hidden_rows):
                        group = half * (half_hidden // hidden_rows) + piece
                        start = (group * dp_size + z) * hidden_rows
                        up_ref[:, start : start + hidden_rows] = up[
                            z, :, piece * hidden_rows : (piece + 1) * hidden_rows
                        ].astype(jnp.float32)
                    at = 0
                    while at < qkv_half:
                        column = half * qkv_half + at
                        part, inner = column // head_width, column % head_width
                        size = min(head_width - inner, qkv_half - at)
                        first = half_width + at
                        start = part * width + z * head_width + inner
                        qkv_ref[:, start : start + size] = attn[
                            z, :, first : first + size
                        ].astype(jnp.float32)
                        at = at + size

        @pl.when(place[0] == 0)
        def _():
            write(refs[0:2], refs[4:6], refs[8:10])

        @pl.when(place[0] != 0)
        def _():
            write(refs[3:1:-1], refs[7:5:-1], refs[11:9:-1])

    shapes = ((rows, 3 * width), (rows, width), (rows, 2 * half_hidden * dp_size), (down_rows, width))
    return pl.pallas_call(
        kernel,
        out_shape=[jax.ShapeDtypeStruct(shape, jnp.float32) for shape in shapes],
        in_specs=[SCALAR] + [WHOLE] * 12,
        compiler_params=pltpu.CompilerParams(vmem_limit_bytes=32 << 20),
        name="finish_weights",
    )(section_id.reshape(1), *ups, *attns, *down_sums)


def finish_rows(section_id, *arrays):
    count = len(arrays)

    def kernel(place, *refs):
        outs = refs[4 * count :]
        for index in range(count):
            own_zero, other_zero, own_one, other_one = refs[4 * index : 4 * index + 4]

            @pl.when(place[0] == 0)
            def _():
                outs[index][0] = own_zero[...]
                outs[index][1] = other_zero[...]

            @pl.when(place[0] != 0)
            def _():
                outs[index][0] = other_one[...]
                outs[index][1] = own_one[...]

    return pl.pallas_call(
        kernel,
        out_shape=[
            jax.ShapeDtypeStruct((2,) + array[0].shape, array[0].dtype) for array in arrays
        ],
        in_specs=[SCALAR] + [WHOLE] * (4 * count),
        compiler_params=pltpu.CompilerParams(vmem_limit_bytes=32 << 20),
        name="finish_rows",
    )(section_id.reshape(1), *[rows for array in arrays for rows in array])


def sum_parts(parts):
    return sum(part.astype(jnp.float32) for part in parts)


def softmax_rows(queries, keys, allowed):
    scores = product_nt(queries, keys) * 0.125
    scores = jnp.where(allowed, scores, -jnp.inf)
    exp_scores = jnp.exp(scores - jnp.max(scores, axis=-1, keepdims=True))
    return exp_scores / jnp.sum(exp_scores, axis=-1, keepdims=True)


def allowed_keys(seg_column, seg_row):
    rows, columns = seg_column.shape[0], seg_row.shape[1]
    query_at = lax.broadcasted_iota(jnp.int32, (rows, columns), 0)
    key_at = lax.broadcasted_iota(jnp.int32, (rows, columns), 1)
    return (seg_column == seg_row) & (key_at <= query_at)


def head_slices(packed, head, head_width):
    start = head * HEAD_DIM
    return [
        packed[:, part * head_width + start : part * head_width + start + HEAD_DIM]
        for part in range(3)
    ]


def attention_kernel(seg_column, seg_row, qkv_ref, mixed_ref):
    head_width = mixed_ref.shape[1]
    allowed = allowed_keys(seg_column[...], seg_row[...])
    packed = qkv_ref[...]
    mixed = []
    for head in range(head_width // HEAD_DIM):
        queries, keys, values = head_slices(packed, head, head_width)
        probs = softmax_rows(queries, keys, allowed)
        mixed.append(low(product(low(probs), values)))
    mixed_ref[...] = jnp.concatenate(mixed, axis=1)


def attention_back_kernel(seg_column, seg_row, qkv_ref, d_mixed_ref, d_qkv_ref):
    head_width = d_mixed_ref.shape[1]
    allowed = allowed_keys(seg_column[...], seg_row[...])
    packed = qkv_ref[...]
    d_mixed_all = d_mixed_ref[...]
    grads = [[], [], []]
    for head in range(head_width // HEAD_DIM):
        queries, keys, values = head_slices(packed, head, head_width)
        d_mixed = d_mixed_all[:, head * HEAD_DIM : (head + 1) * HEAD_DIM]
        probs = softmax_rows(queries, keys, allowed)
        d_probs = product_nt(d_mixed, values)
        d_scores = low(probs * (d_probs - jnp.sum(probs * d_probs, axis=-1, keepdims=True)))
        grads[0].append(low(product(d_scores, keys) * 0.125))
        grads[1].append(low(product_tn(d_scores, queries) * 0.125))
        grads[2].append(low(product_tn(low(probs), d_mixed)))
    d_qkv_ref[...] = jnp.concatenate(grads[0] + grads[1] + grads[2], axis=1)


def attention(segments, qkv):
    head_width = qkv.shape[1] // 3
    return pl.pallas_call(
        attention_kernel,
        out_shape=jax.ShapeDtypeStruct((qkv.shape[0], head_width), jnp.bfloat16),
        compiler_params=pltpu.CompilerParams(vmem_limit_bytes=32 << 20),
        name="attention",
    )(segments[:, None], segments[None, :], qkv)


def attention_back(segments, qkv, d_mixed):
    return pl.pallas_call(
        attention_back_kernel,
        out_shape=jax.ShapeDtypeStruct(qkv.shape, jnp.bfloat16),
        compiler_params=pltpu.CompilerParams(vmem_limit_bytes=32 << 20),
        name="attention_back",
    )(segments[:, None], segments[None, :], qkv, d_mixed)


IN_HBM = pl.BlockSpec(memory_space=pltpu.HBM)


def in_hbm(mat):
    return pltpu.with_memory_space_constraint(mat, pltpu.HBM)


def expert_call(kernel, name, outs, section_id, operands, up_pair, down_pair, extra=()):
    width, hidden = up_pair[0].shape
    half = hidden // 2
    return pl.pallas_call(
        kernel,
        out_shape=[pltpu.HBM(shape, dtype) for shape, dtype in outs],
        out_specs=[WHOLE for _ in outs],
        in_specs=[SCALAR] + [WHOLE] * len(operands) + [IN_HBM] * (4 + len(extra)),
        scratch_shapes=[
            pltpu.VMEM((2, width, half), jnp.bfloat16),
            pltpu.VMEM((2, half, width), jnp.bfloat16),
            pltpu.SemaphoreType.DMA((2, 2)),
        ]
        + [pltpu.VMEM((2, mat.shape[0], half), mat.dtype) for mat in extra]
        + [pltpu.SemaphoreType.DMA((2,)) for _ in extra],
        compiler_params=pltpu.CompilerParams(vmem_limit_bytes=40 << 20),
        name=name,
    )(section_id.reshape(1), *operands, *[in_hbm(mat) for mat in (*up_pair, *down_pair, *extra)])


def expert_weights_in(layer, place, sources, up_here, down_here, arrived):
    half = up_here.shape[2]

    def copies(which, part):
        columns = pl.ds(part * half, half)
        return (
            pltpu.make_async_copy(
                sources[which].at[:, columns], up_here.at[part], arrived.at[0, part]
            ),
            pltpu.make_async_copy(
                sources[2 + which].at[columns], down_here.at[part], arrived.at[1, part]
            ),
        )

    for which in range(2):

        @pl.when((place[0] == layer) if which == 0 else (place[0] != layer))
        def _():
            for part in range(2):
                for copy in copies(which, part):
                    copy.start()

    return [copies(0, part) for part in range(2)]


def row_scales(logits, expert):
    lane = lax.broadcasted_iota(jnp.int32, logits.shape, 1)
    experts = logits.shape[1] - 2

    def share(among, one):
        chosen = jnp.where(among, logits, -jnp.inf)
        weights = jnp.exp(chosen - jnp.max(chosen, axis=1, keepdims=True))
        part = jnp.sum(jnp.where(one, weights, 0.0), axis=1, keepdims=True)
        return part / jnp.sum(weights, axis=1, keepdims=True)

    return share(lane >= experts, lane == experts + 1) * share(lane < experts, lane == expert)


def expert_forward(layer, section_id, expert, rows, small_weights, up_pair, down_pair):
    def kernel(place, expert_ref, rows_ref, small_ref, *refs):
        scale_ref, hidden_ref, low_ref, part_ref, up_here, down_here, arrived = refs[4:]
        waits = expert_weights_in(layer, place, refs[:4], up_here, down_here, arrived)
        scale_ref[...] = row_scales(product_nt(rows_ref[...], small_ref[...]), expert_ref[0, 0])
        half = up_here.shape[2]
        total = None
        for part in range(2):
            here = slice(part * half, (part + 1) * half)
            waits[part][0].wait()
            hidden = product(rows_ref[...], up_here[part])
            hidden_ref[:, here] = hidden
            hidden_low = low(gelu_tanh(hidden))
            low_ref[:, here] = hidden_low
            waits[part][1].wait()
            added = product(hidden_low, down_here[part])
            total = added if total is None else total + added
        part_ref[...] = low(total)

    count, width = rows.shape
    hidden = up_pair[0].shape[1]
    outs = [((count, 1), jnp.float32), ((count, hidden), jnp.float32)]
    outs += [((count, hidden), jnp.bfloat16), ((count, width), jnp.bfloat16)]
    return expert_call(
        kernel,
        "expert_forward",
        outs,
        section_id,
        (expert.reshape(1, 1), rows, small_weights),
        up_pair,
        down_pair,
    )


def expert_backward(layer, section_id, grad_rows, scale, hidden, up_pair, down_pair):
    def kernel(place, rows_ref, scale_ref, *refs):
        scaled_ref, d_hidden_ref, back_ref, up_here, down_here, arrived = refs[5:11]
        hidden_here, hidden_arrived = refs[11:]
        waits = expert_weights_in(layer, place, refs[:4], up_here, down_here, arrived)
        half = up_here.shape[2]
        fetches = [
            pltpu.make_async_copy(
                refs[4].at[:, pl.ds(part * half, half)], hidden_here.at[part], hidden_arrived.at[part]
            )
            for part in range(2)
        ]
        for fetch in fetches:
            fetch.start()
        scaled = low(scale_ref[...] * rows_ref[...].astype(jnp.float32))
        scaled_ref[...] = scaled
        total = None
        for part in range(2):
            here = slice(part * half, (part + 1) * half)
            waits[part][1].wait()
            d_low = product_nt(scaled, down_here[part])
            fetches[part].wait()
            d_hidden = low(gelu_grad(hidden_here[part], d_low))
            d_hidden_ref[:, here] = d_hidden
            waits[part][0].wait()
            added = product_nt(d_hidden, up_here[part])
            total = added if total is None else total + added
        back_ref[...] = low(total)

    shape = ((grad_rows.shape), jnp.bfloat16)
    outs = [shape, (hidden.shape, jnp.bfloat16), shape]
    return expert_call(
        kernel,
        "expert_backward",
        outs,
        section_id,
        (grad_rows, scale),
        up_pair,
        down_pair,
        (hidden,),
    )


def pair_grads(section_id, *pairs):
    mats = [side for left, right in pairs for side in (left, other_core(left), right, other_core(right))]
    left_width = pairs[0][0].shape[1]
    halves = [right.shape[1] // 2 for _, right in pairs]

    def kernel(place, *refs):
        start = 0
        for index, half in enumerate(halves):
            left_own, left_other, right_own, right_other = refs[4 * index : 4 * index + 4]
            here = pl.ds(pl.multiple_of(place[0] * half, LANES), half)
            total = product_tn(left_own[...], right_own[:, here])
            total = total + product_tn(left_other[...], right_other[:, here])
            refs[-1][:, start : start + half] = low(total)
            start = start + half

    return pl.pallas_call(
        kernel,
        out_shape=jax.ShapeDtypeStruct((left_width, sum(halves)), jnp.bfloat16),
        in_specs=[SCALAR] + [WHOLE] * len(mats),
        compiler_params=pltpu.CompilerParams(vmem_limit_bytes=40 << 20),
        name="pair_grads",
    )(section_id.reshape(1), *mats)


OWNER_TILE = 512


def owner_grads(section_id, left_mats, right_mats):
    rows, left_width = left_mats[0].shape
    right_width = right_mats[0].shape[1]
    tiles = left_width // OWNER_TILE

    def kernel(place, *refs):
        out_ref, left_here, right_here, arrived = refs[8:]
        expert, tile = pl.program_id(0), pl.program_id(1)

        def copies(source, slot):
            return (
                pltpu.make_async_copy(refs[source], left_here.at[slot], arrived.at[0, slot]),
                pltpu.make_async_copy(refs[4 + source], right_here.at[slot], arrived.at[1, slot]),
            )

        for first, sources in ((True, (0, 1)), (False, (3, 2))):
            here = (place[0] == 0) if first else (place[0] != 0)

            @pl.when(here & (expert == 0) & (tile == 0))
            def _():
                for slot, source in enumerate(sources):
                    for copy in copies(source, slot):
                        copy.start()

        @pl.when(tile == 0)
        def _():
            for copy in copies(0, expert):
                copy.wait()

        left = left_here[expert, :, pl.ds(tile * OWNER_TILE, OWNER_TILE)]
        out_ref[0] = product_tn(left, right_here[expert])

    return pl.pallas_call(
        kernel,
        out_shape=jax.ShapeDtypeStruct((2, left_width, right_width), jnp.float32),
        grid=(2, tiles),
        in_specs=[SCALAR] + [IN_HBM] * 8,
        out_specs=pl.BlockSpec((1, OWNER_TILE, right_width), lambda expert, tile: (expert, tile, 0)),
        scratch_shapes=[
            pltpu.VMEM((2, rows, left_width), jnp.bfloat16),
            pltpu.VMEM((2, rows, right_width), jnp.bfloat16),
            pltpu.SemaphoreType.DMA((2, 2)),
        ],
        compiler_params=pltpu.CompilerParams(vmem_limit_bytes=40 << 20),
        name="owner_grads",
    )(section_id.reshape(1), *[in_hbm(mat) for mat in (*left_mats, *right_mats)])


def statistics(value_rows):
    centre = jnp.mean(value_rows, axis=-1, keepdims=True)
    centred = value_rows - centre
    variance = jnp.mean(centred * centred, axis=-1, keepdims=True)
    spread_inverse = lax.rsqrt(variance + 1e-05)
    return centred * spread_inverse, spread_inverse


def column_sums(value_rows):
    return jnp.sum(value_rows, axis=0, keepdims=True)


def block_sum(blocks_ref):
    total = blocks_ref[0].astype(jnp.float32)
    for place in range(1, blocks_ref.shape[0]):
        total = total + blocks_ref[place].astype(jnp.float32)
    return total


def call(kernel, name, outs, *operands):
    specs = [
        pl.BlockSpec(memory_space=pltpu.HBM)
        if operand.shape[1:] == (operand.shape[-1],) * 2
        else WHOLE
        for operand in operands
    ]
    operands = [
        operand if spec is WHOLE else pltpu.with_memory_space_constraint(operand, pltpu.HBM)
        for operand, spec in zip(operands, specs)
    ]
    mats = [operand.shape[1:] for operand, spec in zip(operands, specs) if spec is not WHOLE]
    scratch = [pltpu.VMEM(shape, jnp.bfloat16) for shape in mats]
    scratch += [pltpu.SemaphoreType.DMA for _ in mats]
    return pl.pallas_call(
        kernel,
        in_specs=specs,
        out_shape=[jax.ShapeDtypeStruct(shape, dtype) for shape, dtype in outs],
        scratch_shapes=scratch,
        compiler_params=pltpu.CompilerParams(vmem_limit_bytes=32 << 20),
        name=name,
    )(*operands)


def project(layer, mixed_blocks, proj_mat, layer_in, gain, shift):
    def kernel(mixed_ref, proj_ref, in_ref, gain_ref, shift_ref, *outs):
        rows_ref, res_ref, mid_ref, sq_ref, proj_here, arrived = outs
        fetch = pltpu.make_async_copy(proj_ref.at[layer], proj_here, arrived)
        fetch.start()
        places = mixed_ref.shape[0]
        mixed = jnp.concatenate([mixed_ref[place] for place in range(places)], axis=1)
        rows_ref[...] = mixed
        fetch.wait()
        branch = product(mixed, proj_here[...])
        residual = in_ref[...].astype(jnp.float32) + branch
        res_ref[...] = residual
        mid_ref[...] = low(statistics(residual)[0] * gain_ref[...] + shift_ref[...])
        sq_ref[...] = column_sums(branch * branch)

    rows, width = layer_in.shape
    outs = [((rows, width), jnp.bfloat16), ((rows, width), jnp.float32)]
    outs += [((rows, width), jnp.bfloat16), ((1, width), jnp.float32)]
    return call(kernel, "project", outs, mixed_blocks, proj_mat, layer_in, gain, shift)


def layer_end(branch_blocks, residual, gain, shift):
    def kernel(blocks_ref, res_ref, gain_ref, shift_ref, out_ref, normed_ref, sq_ref):
        branch = block_sum(blocks_ref)
        layer_out = res_ref[...] + branch
        rounded = low(layer_out)
        out_ref[...] = rounded
        normed = statistics(rounded.astype(jnp.float32))[0]
        normed_ref[...] = low(normed * gain_ref[...] + shift_ref[...])
        sq_ref[0:1] = column_sums(branch * branch)
        sq_ref[1:2] = column_sums(layer_out * layer_out)

    shape = residual.shape
    outs = [(shape, jnp.bfloat16), (shape, jnp.bfloat16), ((2, shape[1]), jnp.float32)]
    return call(kernel, "layer_end", outs, branch_blocks, residual, gain, shift)


def norm_back(blocks_ref, value_ref, gain_ref, grad_ref, gain_grad_ref, shift_grad_ref):
    d_normed = block_sum(blocks_ref)
    normed, spread_inverse = statistics(value_ref[...].astype(jnp.float32))
    gain_grad_ref[...] = column_sums(d_normed * normed)
    shift_grad_ref[...] = column_sums(d_normed)
    d_centred = d_normed * gain_ref[...]
    along = jnp.mean(d_centred * normed, axis=-1, keepdims=True)
    d_value = d_centred - jnp.mean(d_centred, axis=-1, keepdims=True) - normed * along
    return grad_ref[...].astype(jnp.float32) + d_value * spread_inverse


def mid_back(layer, mid_blocks, residual, gain, grad_out, proj_mat, dp_size):
    def kernel(blocks_ref, res_ref, gain_ref, grad_ref, proj_ref, *outs):
        sum_ref, low_ref, mixed_ref, gain_grad_ref, shift_grad_ref, proj_here, arrived = outs
        fetch = pltpu.make_async_copy(proj_ref.at[layer], proj_here, arrived)
        fetch.start()
        grad = norm_back(blocks_ref, res_ref, gain_ref, grad_ref, gain_grad_ref, shift_grad_ref)
        sum_ref[...] = grad
        low_ref[...] = low(grad)
        fetch.wait()
        d_mixed = low(product_nt(low(grad), proj_here[...]))
        part = d_mixed.shape[1] // dp_size
        for place in range(dp_size):
            mixed_ref[place] = d_mixed[:, place * part : (place + 1) * part]

    rows, width = residual.shape
    row = ((1, width), jnp.float32)
    outs = [((rows, width), jnp.float32), ((rows, width), jnp.bfloat16)]
    outs += [((dp_size, rows, width // dp_size), jnp.bfloat16), row, row]
    return call(kernel, "mid_back", outs, mid_blocks, residual, gain, grad_out, proj_mat)


def input_back(in_blocks, layer_in, gain, grad_resid):
    def kernel(blocks_ref, in_ref, gain_ref, grad_ref, sum_ref, low_ref, gain_grad_ref, shift_grad_ref):
        grad = norm_back(blocks_ref, in_ref, gain_ref, grad_ref, gain_grad_ref, shift_grad_ref)
        sum_ref[...] = grad
        low_ref[...] = low(grad)

    shape = layer_in.shape
    row = ((1, shape[1]), jnp.float32)
    outs = [(shape, jnp.float32), (shape, jnp.bfloat16), row, row]
    return call(kernel, "input_back", outs, in_blocks, layer_in, gain, grad_resid)


def pack_small(parts_of_layers, squares_of_layers, weight_rows):
    layers = len(parts_of_layers)
    flat = [part for parts in parts_of_layers for part in parts] + list(squares_of_layers)
    width = flat[0].shape[1]
    used = sum(part.shape[0] for part in parts_of_layers[0])
    height = -(-(used + 1) // 8) * 8
    places = width // weight_rows

    def kernel(*refs):
        out_ref, rows_ref = refs[-2], refs[-1]
        per_layer = len(parts_of_layers[0])
        for layer in range(layers):
            rows_ref[...] = jnp.zeros(rows_ref.shape, jnp.float32)
            start = 0
            for part in refs[layer * per_layer : (layer + 1) * per_layer]:
                rows_ref[start : start + part.shape[0]] = part[...]
                start = start + part.shape[0]
            lane = lax.broadcasted_iota(jnp.int32, (1, width), 1) % LANES
            marked = jnp.zeros((1, width), jnp.float32)
            sums = jnp.sum(refs[layers * per_layer + layer][...], axis=1, keepdims=True)
            for kind in range(3):
                marked = jnp.where(lane == kind, sums[kind : kind + 1], marked)
            rows_ref[start : start + 1] = marked
            for place in range(places):
                column = place * weight_rows // LANES * LANES
                out_ref[layer * places + place] = rows_ref[:, column : column + LANES]

    return pl.pallas_call(
        kernel,
        out_shape=jax.ShapeDtypeStruct((layers * places, height, LANES), jnp.float32),
        scratch_shapes=[pltpu.VMEM((height, width), jnp.float32)],
        name="pack_small",
    )(*flat)


def other_core(block):
    return lax.ppermute(block, SEC, [(0, 1), (1, 0)])


def shards(
    inputs,
    cotangent,
    segment_ids,
    routes,
    norm_gains,
    norm_shifts,
    attn_qkv,
    attn_proj,
    dense_up,
    dense_down,
    router,
    mixer,
    expert_up,
    expert_down,
):
    sections = lax.axis_size(SEC)
    groups = lax.axis_size(EX)
    dp_size = lax.axis_size(DP)
    section_id = lax.axis_index(SEC)
    expert_id = lax.axis_index(EX)
    micro_count = inputs.shape[0]
    seq_rows = inputs.shape[2]
    width = inputs.shape[3]
    full_len = segment_ids.shape[2]
    experts_total = router.shape[2]
    hidden_rows = dense_down.shape[1]
    weight_rows = attn_qkv.shape[1]
    heads_here = HEADS // dp_size
    head_width = heads_here * HEAD_DIM
    capacity = max(2, 5 * seq_rows // (4 * experts_total))
    slots = dp_size * capacity
    devices = sections * groups * dp_size

    small_parts = jnp.concatenate([norm_gains[0], norm_shifts[0], router[0].T, mixer[0].T], axis=0)
    small_count = small_parts.shape[0]
    route_row = low(routes[0, :, 0, :, 0])
    message = jnp.concatenate([small_parts.reshape(-1), route_row.reshape(-1)])
    filled = message.shape[0]
    padded = -(-filled // 1024) * 1024
    message = jnp.pad(message, (0, padded - filled)).reshape(padded // 128, 128)

    def expert_parts(*own_layers):
        return [
            (
                lax.dynamic_index_in_dim(own_layer, section_id, 0, keepdims=False),
                lax.dynamic_index_in_dim(own_layer, 1 - section_id, 0, keepdims=False),
            )
            for own_layer in own_layers
        ]

    hidden_here = groups * hidden_rows
    small_all, (proj_rows, up_parts) = beside(
        lambda blocks: exchange(blocks, EVERY),
        jnp.broadcast_to(message[None], (devices,) + message.shape),
        lambda proj_shard, up_cols: (
            in_order(permute_copies(proj_shard, DP), DP),
            own_parts(
                up_cols.reshape(weight_rows, groups, dp_size, hidden_rows)
                .transpose(2, 0, 1, 3)
                .reshape(dp_size, weight_rows, hidden_here),
                DP,
            ),
        ),
        (attn_proj[0], dense_up[0]),
    )
    small_all = small_all.reshape(sections, groups, dp_size, padded)

    def params_of(small_all):
        params_all = small_all[..., : small_count * weight_rows].reshape(
            sections, groups * dp_size, small_count, weight_rows
        )
        return params_all.transpose(0, 2, 1, 3).reshape(sections, small_count, width)

    def routes_of(small_all):
        routes_all = lax.dynamic_index_in_dim(
            small_all[..., small_count * weight_rows : filled], expert_id, 1, keepdims=False
        ).reshape(sections, dp_size, micro_count, seq_rows)
        routes_all = lax.dynamic_index_in_dim(routes_all, section_id, 2, keepdims=False)
        return routes_all.astype(jnp.int32)

    on_first = section_id == 0

    def by_layer(pair):
        of_own_layer, of_other_layer = pair
        return (
            jnp.where(on_first, of_own_layer, of_other_layer),
            jnp.where(on_first, of_other_layer, of_own_layer),
        )

    proj_both = lax.all_gather(proj_rows.reshape(-1, width), HOMES, axis=0, tiled=True)
    proj_both = proj_both.reshape(sections, width, width)
    qkv_cols = attn_qkv[0].reshape(weight_rows, 3, dp_size, head_width).transpose(2, 0, 1, 3)
    qkv_cols, small_all = lax.optimization_barrier(
        (qkv_cols.reshape(dp_size, weight_rows, 3 * head_width), small_all)
    )
    qkv_cols, expert_weights = beside(
        over_dp, qkv_cols, expert_parts, (expert_up[0], expert_down[0])
    )
    params_all = params_of(small_all)
    routes_all = routes_of(small_all)
    own_input = lax.dynamic_index_in_dim(inputs[:, 0], section_id, 0, keepdims=False)
    first_params = params_all[0].astype(jnp.float32)
    first_normed = low(
        layer_norm(own_input.astype(jnp.float32), first_params[0:1], first_params[2:3])
    )
    down_both = lax.all_gather(dense_down[0], HOMES, axis=0, tiled=True)
    qkv_own, (first_seq, up_rows, down_both) = beside(
        lambda blocks: exchange(blocks, EX),
        jnp.broadcast_to(qkv_cols[None], (groups,) + qkv_cols.shape),
        lambda rows, parts, down_both: (
            in_order(permute_copies(rows, DP), DP),
            in_order(sent_parts(parts, DP), DP),
            down_both,
        ),
        (first_normed, up_parts),
        (down_both,),
    )
    first_seq = first_seq.reshape(full_len, width)
    qkv_own = qkv_own.reshape(width, 3 * head_width)
    qkv_pair = (qkv_own, other_core(qkv_own))
    exp_up_pair, exp_down_pair = [(kept, other_core(sent)) for kept, sent in expert_weights]
    first_qkv = low(product(first_seq, by_layer(qkv_pair)[0]))
    up_both = lax.all_gather(up_rows.reshape(-1, hidden_here), HOMES, axis=0, tiled=True)
    up_both = up_both.reshape(sections, width, hidden_here)
    down_both = down_both.reshape(sections, hidden_here, width)

    segments = lax.dynamic_index_in_dim(segment_ids[:, 0], section_id, 0, keepdims=False)
    places = jnp.arange(full_len, dtype=jnp.int32)
    earlier = (places[None, :] < places[:, None]) & (
        places[None, :] // seq_rows == places[:, None] // seq_rows
    )

    def slot_table(route_now):
        rank = jnp.sum(
            ((route_now[:, None] == route_now[None, :]) & earlier).astype(jnp.int32), axis=1
        )
        home = route_now % sections * groups + route_now // sections
        target = home * slots + places // seq_rows * capacity + rank
        slot_ids = jnp.arange(sections * groups * slots, dtype=jnp.int32)
        table = low(slot_ids[:, None] == target[None, :])
        hot = route_now[:, None] == jnp.arange(experts_total, dtype=jnp.int32)[None, :]
        return table, hot.astype(jnp.float32)

    def packed_rows(token_rows, table):
        return low(product(table, token_rows)).reshape(sections * groups, slots, width)

    def coefficients(mid_seq, small_weights, hot):
        small_logits = product_nt(mid_seq, small_weights)
        gate_probs = jax.nn.softmax(small_logits[:, :experts_total], axis=-1)
        gate = jnp.sum(gate_probs * hot, axis=-1, keepdims=True)
        coef = jax.nn.softmax(small_logits[:, experts_total:], axis=-1)
        return gate_probs, gate, coef

    own_expert = expert_id * sections + section_id

    def dense_in(mid_seq, up_mat):
        hidden = product(mid_seq, up_mat)
        return hidden, low(gelu_tanh(hidden))

    def attended(qkv):
        return attention(segments, qkv).reshape(dp_size, seq_rows, head_width)

    def forward_zero():
        params = first_params
        table, hot = slot_table(routes_all[0].reshape(full_len))
        mixed, residual, mid, attn_squares = project(
            0, over_dp(attended(first_qkv)), proj_both, own_input, params[1:2], params[3:4]
        )
        mid_seq = gather_rows(mid)
        small_weights = params_all[0, 4:]

        expert_rows, ((gate_probs, gate, coef), own_grad_seq) = beside(
            over_homes,
            packed_rows(mid_seq, table),
            lambda mid_seq, small_weights, grad: (
                coefficients(mid_seq, small_weights, hot),
                in_order(permute_copies(grad, DP), DP).reshape(full_len, width),
            ),
            (mid_seq, small_weights, own_grad),
        )
        expert_rows = expert_rows.reshape(-1, width)
        scale, exp_hidden, exp_hidden_low, exp_out = expert_forward(
            0, section_id, own_expert, expert_rows, small_weights, exp_up_pair, exp_down_pair
        )

        def return_work(mid_seq, up_mat, down_mat):
            hidden, hidden_low = dense_in(mid_seq, up_mat)
            return hidden, hidden_low, product(hidden_low, down_mat)

        returned, (hidden, hidden_low, dense_part) = beside(
            over_homes,
            exp_out.reshape(-1, slots, width),
            return_work,
            (mid_seq,),
            (up_both[0], down_both[0]),
        )
        expert_part = product_tn(table, returned.reshape(-1, width))
        branch_part = coef[:, 0:1] * dense_part + coef[:, 1:2] * gate * expert_part
        branch, settled = beside(
            over_dp,
            row_blocks(branch_part),
            lambda qkv_pair, down_both: (by_layer(qkv_pair), (down_both[0], down_both[1])),
            (qkv_pair, down_both),
        )
        next_params = params_all[1].astype(jnp.float32)
        out_low, next_normed, squares = layer_end(
            branch, residual, next_params[0:1], next_params[2:3]
        )
        record = SimpleNamespace(
            params=params,
            small_weights=small_weights,
            table=table,
            hot=hot,
            layer_in=own_input,
            normed_seq=first_seq,
            qkv=first_qkv,
            mixed=mixed,
            residual=residual,
            mid_seq=mid_seq,
            expert_rows=expert_rows,
            scale=scale,
            gate_probs=gate_probs,
            gate=gate,
            coef=coef,
            hidden=hidden,
            hidden_low=hidden_low,
            dense_part=dense_part,
            exp_hidden=exp_hidden,
            exp_hidden_low=exp_hidden_low,
            expert_part=expert_part,
        )
        squares = jnp.concatenate([attn_squares, squares], axis=0)
        return out_low, next_normed, squares, record, (*settled, own_grad_seq)

    def forward_one(layer_in, normed, own_grad_seq):
        params = params_all[1].astype(jnp.float32)
        table, hot = slot_table(routes_all[1].reshape(full_len))
        normed_seq = gather_rows(normed)
        qkv = low(product(normed_seq, qkv_both[1]))
        mixed, up_apart = beside(
            over_dp, attended(qkv), lambda mats: (mats[0], mats[1]), (up_both,)
        )
        mixed, residual, mid, attn_squares = project(
            1, mixed, proj_both, layer_in, params[1:2], params[3:4]
        )
        grad_rows, mid_seq = beside(
            over_homes, packed_rows(own_grad_seq, table), gather_rows, (mid,)
        )
        small_weights = params_all[1, 4:]

        def dispatch_work(mid_seq, small_weights, up_mat):
            return coefficients(mid_seq, small_weights, hot), dense_in(mid_seq, up_mat)

        expert_rows, ((gate_probs, gate, coef), (hidden, hidden_low)) = beside(
            over_homes,
            packed_rows(mid_seq, table),
            dispatch_work,
            (mid_seq, small_weights, up_apart[1]),
        )
        expert_rows = expert_rows.reshape(-1, width)
        scale, exp_hidden, exp_hidden_low, exp_out = expert_forward(
            1, section_id, own_expert, expert_rows, small_weights, exp_up_pair, exp_down_pair
        )
        returned, dense_part = beside(
            over_homes, exp_out.reshape(-1, slots, width), product, (hidden_low, down_apart[1])
        )
        expert_part = product_tn(table, returned.reshape(-1, width))
        branch_part = coef[:, 0:1] * dense_part + coef[:, 1:2] * gate * expert_part
        branch = lax.psum_scatter(low(branch_part), DP, scatter_dimension=0, tiled=True)
        record = SimpleNamespace(
            params=params,
            small_weights=small_weights,
            table=table,
            hot=hot,
            layer_in=layer_in,
            normed_seq=normed_seq,
            qkv=qkv,
            mixed=mixed,
            residual=residual,
            mid_seq=mid_seq,
            expert_rows=expert_rows,
            scale=scale,
            gate_probs=gate_probs,
            gate=gate,
            coef=coef,
            hidden=hidden,
            hidden_low=hidden_low,
            dense_part=dense_part,
            exp_hidden=exp_hidden,
            exp_hidden_low=exp_hidden_low,
            expert_part=expert_part,
        )
        return branch, attn_squares, record, grad_rows, up_apart

    def over_expert(grad_mat):
        return lax.psum_scatter(grad_mat, EX, scatter_dimension=0, tiled=True)

    def by_rows(grad_mat, count):
        return low(grad_mat).reshape(count, -1, grad_mat.shape[-1])

    def dp_blocks(*grad_mats):
        blocks = [by_rows(grad_mat, dp_size) for grad_mat in grad_mats]
        return own_parts(jnp.concatenate(blocks, axis=2), DP)

    half_hidden, half_width = hidden_here // 2, width // 2

    def backward_layer(layer, grad_low, grad_seq, record, sums_one=(), operands_one=None, settle=(), grad_rows=None):
        params = record.params
        coef, gate, table = record.coef, record.gate, record.table
        def dense_back(grad_seq, coef, down_mat, up_mat, *sums_one):
            grad_seq = grad_seq.astype(jnp.float32)
            early = dp_blocks(*sums_one) if sums_one else ()
            d_dense = low(coef[:, 0:1] * grad_seq)
            dense_dot = jnp.sum(grad_seq * record.dense_part, axis=-1, keepdims=True)
            expert_dot = jnp.sum(grad_seq * record.expert_part, axis=-1, keepdims=True)
            d_coef = jnp.concatenate([dense_dot, gate * expert_dot], axis=1)
            d_mix = coef * (d_coef - jnp.sum(coef * d_coef, axis=-1, keepdims=True))
            d_logits = record.gate_probs * (record.hot - gate) * (coef[:, 1:2] * expert_dot)
            d_small = low(jnp.concatenate([d_logits, d_mix], axis=1))
            d_up = low(gelu_grad(record.hidden, product_nt(d_dense, down_mat)))
            d_mid_part = product_nt(d_up, up_mat) + product(d_small, record.small_weights)
            return d_dense, d_small, d_up, d_mid_part, early

        dense_operands = (grad_seq, coef, down_apart[layer], up_apart[layer])
        if layer == 0:
            grad_rows, dense_grad = beside(
                over_homes,
                packed_rows(grad_seq, table),
                dense_back,
                dense_operands,
                tuple(sums_one),
            )
        expert_grad_rows, d_exp_hidden, expert_back = expert_backward(
            layer,
            section_id,
            grad_rows.reshape(-1, width),
            record.scale,
            record.exp_hidden,
            exp_up_pair,
            exp_down_pair,
        )
        expert_operands = (
            record.expert_rows,
            d_exp_hidden,
            record.exp_hidden_low,
            expert_grad_rows,
        )

        swapped = tuple(other_core(operand) for operand in expert_operands)

        def owner_mats(index):
            return (
                expert_operands[index],
                swapped[index],
                operands_one[0][index],
                operands_one[1][index],
            )

        def dense_grads(hidden_low, d_dense, mid_seq, d_up, d_small):
            g_dense = pair_grads(section_id, (mid_seq, d_up), (hidden_low, d_dense))
            return g_dense, product_tn(d_small, mid_seq)

        expert_back = expert_back.reshape(-1, slots, width)
        if layer == 0:
            returned, (parts_one, g_exp_down) = beside(
                over_homes,
                expert_back,
                lambda early, *mats: (sent_parts(early, DP), owner_grads(section_id, *mats)),
                (dense_grad[4], owner_mats(2), owner_mats(3)),
            )
        else:
            returned, dense_grad = beside(
                over_homes,
                expert_back,
                lambda blocks, *operands: dense_back(*started(operands, blocks)),
                (expert_back, *dense_operands),
            )
        d_dense, d_small, d_up, d_mid_part, _ = dense_grad
        d_mid_part = d_mid_part + product_tn(table, returned.reshape(-1, width))
        mid_blocks, operands = lax.optimization_barrier(
            (
                row_blocks(d_mid_part),
                (record.hidden_low, d_dense, record.mid_seq, d_up, d_small),
            )
        )
        g_dense, g_small = dense_grads(*operands)
        if layer == 1:
            dense_sum = over_expert(g_dense)
        d_mid, g_dense, g_small = lax.optimization_barrier(
            (over_dp(mid_blocks), g_dense, g_small)
        )
        if layer == 0:
            dense_sum = over_expert(g_dense)
        d_resid, d_attn, d_mixed, d_gain_one, d_shift_one = mid_back(
            layer, d_mid, record.residual, params[1:2], grad_low, proj_both, dp_size
        )
        d_mixed = over_dp(d_mixed)

        def attention_grads(d_mixed):
            d_qkv = attention_back(segments, record.qkv, d_mixed.reshape(full_len, head_width))
            return d_qkv, row_blocks(product_nt(d_qkv, qkv_both[layer]))

        d_qkv, in_blocks = attention_grads(d_mixed)
        in_blocks, normed_seq, d_qkv = lax.optimization_barrier(
            (in_blocks, record.normed_seq, d_qkv)
        )
        g_attn = pair_grads(section_id, (record.mixed, d_attn), (normed_seq, d_qkv))
        attn_sum = over_expert(g_attn)
        beside_it = (g_attn, settle)
        d_normed, beside_it = lax.optimization_barrier((over_dp(in_blocks), beside_it))
        d_input, d_input_low, d_gain_zero, d_shift_zero = input_back(
            d_normed, record.layer_in, params[0:1], d_resid
        )
        small_grads = (d_gain_zero, d_gain_one, d_shift_zero, d_shift_one, g_small)
        if layer == 0:
            extra = (parts_one, owner_mats, g_exp_down)
        else:
            extra = (expert_operands, swapped, beside_it[1])
        return d_input, d_input_low, (dense_sum, attn_sum), small_grads, extra

    own_grad = lax.dynamic_index_in_dim(cotangent[:, 0], section_id, 0, keepdims=False)
    out_zero, next_normed, squares_zero, record_zero, settled = forward_zero()
    qkv_both, down_apart, own_grad_seq = settled
    branch_one, attn_squares_one, record_one, grad_rows, up_apart = forward_one(
        out_zero, next_normed, own_grad_seq
    )
    grad_one, grad_one_low, sums_one, small_one, operands_one = backward_layer(
        1, own_grad, own_grad_seq, record_one, settle=branch_one, grad_rows=grad_rows
    )
    dense_one, attn_one = sums_one
    branch_one = operands_one[2].astype(jnp.float32)
    out_one = record_one.residual + branch_one
    squares_one = jnp.concatenate(
        [attn_squares_one, column_sums(branch_one * branch_one), column_sums(out_one * out_one)]
    )
    out_one = low(out_one)
    grad_zero, _, (dense_zero, attn_zero), small_zero, extra = backward_layer(
        0,
        grad_one_low,
        gather_rows(grad_one_low),
        record_zero,
        (dense_one[:, :half_hidden], attn_one),
        operands_one,
    )
    parts_one, owner_mats, grad_exp_down = extra

    moved_one = in_order(after(parts_one, grad_zero), DP)
    small_message = pack_small(
        (small_zero, small_one), (squares_zero, squares_one), weight_rows
    )
    small_moved, grad_exp_up = beside(
        lambda blocks: exchange(blocks, EVERY),
        small_message,
        lambda *mats: owner_grads(section_id, *mats),
        (owner_mats(0), owner_mats(1)),
    )
    up_zero = over_dp(by_rows(after(dense_zero[:, :half_hidden], small_moved), dp_size))
    attn_zero = over_dp(by_rows(after(attn_zero, up_zero), dp_size))
    up_one, attn_one = moved_one[..., :half_hidden], moved_one[..., half_hidden:]
    down_zero, down_one = dense_zero[:, half_hidden:], dense_one[:, half_hidden:]

    def of_both(of_zero, of_one):
        return of_zero, other_core(of_zero), of_one, other_core(of_one)

    grad_qkv, grad_proj, grad_up, grad_down = finish_weights(
        section_id,
        of_both(up_zero, up_one),
        of_both(attn_zero, attn_one),
        of_both(down_zero, down_one),
        hidden_rows,
    )
    activations, input_grads = finish_rows(
        section_id, of_both(out_zero, out_one), of_both(grad_zero, grad_one)
    )
    small_sum = jnp.sum(small_moved, axis=0)
    place = expert_id * dp_size + lax.axis_index(DP)
    sums = lax.dynamic_slice_in_dim(
        small_sum[:small_count], place * weight_rows % LANES, weight_rows, axis=1
    )
    totals = small_sum[small_count, :3]
    element_count = micro_count * seq_rows * width * groups * dp_size
    branch_rms = jnp.sqrt(totals / element_count)[None]
    return (
        activations[None, :, None],
        input_grads[None, :, None],
        sums[None, 0:2],
        sums[None, 2:4],
        grad_qkv[None],
        grad_proj[None],
        grad_up[None],
        grad_down[None],
        sums[4 : 4 + experts_total].T[None],
        sums[4 + experts_total :].T[None],
        grad_exp_up[None],
        grad_exp_down[None],
        branch_rms,
    )


def solution(mesh):
    placed = (
        P(None, EX, DP, None),
        P(None, EX, DP, None),
        P(None, EX, None),
        P(SEC, None, EX, DP, None),
        P(SEC, None, (EX, DP)),
        P(SEC, None, (EX, DP)),
        P(SEC, (EX, DP), None),
        P(SEC, (EX, DP), None),
        P(SEC, (EX, DP), None),
        P(SEC, (EX, DP), None),
        P(SEC, (EX, DP), None),
        P(SEC, (EX, DP), None),
        P(SEC, EX, None, DP),
        P(SEC, EX, DP, None),
    )
    return jax.shard_map(
        shards,
        mesh=mesh,
        in_specs=placed,
        out_specs=(
            P(SEC, None, EX, DP, None),
            P(SEC, None, EX, DP, None),
            P(SEC, None, (EX, DP)),
            P(SEC, None, (EX, DP)),
            P(SEC, (EX, DP), None),
            P(SEC, (EX, DP), None),
            P(SEC, (EX, DP), None),
            P(SEC, (EX, DP), None),
            P(SEC, (EX, DP), None),
            P(SEC, (EX, DP), None),
            P(SEC, EX, None, DP),
            P(SEC, EX, DP, None),
            P(SEC, None),
        ),
        check_vma=False,
    )
```

```python
from types import SimpleNamespace

import jax
import jax.numpy as jnp
from jax import lax
from jax.experimental import pallas as pl
from jax.experimental.pallas import tpu as pltpu
from jax.sharding import PartitionSpec as P

HEADS = 16
HEAD_DIM = 64
SEC, EX, DP = "section", "expert", "dp"
EVERY = (SEC, EX, DP)
HOMES = (SEC, EX)
LANES = 128


def layer_norm(value_rows, gain_vec, shift_vec):
    centre = jnp.mean(value_rows, axis=-1, keepdims=True)
    centred = value_rows - centre
    variance = jnp.mean(centred * centred, axis=-1, keepdims=True)
    return centred * lax.rsqrt(variance + 1e-05) * gain_vec + shift_vec


def gelu_tanh(value_rows):
    return jax.nn.gelu(value_rows, approximate=True)


def gelu_grad(value_rows, grad_in):
    return jax.vjp(gelu_tanh, value_rows)[1](grad_in)[0]


def product(left_mat, right_mat):
    return jnp.dot(left_mat, right_mat, preferred_element_type=jnp.float32)


def product_tn(left_mat, right_mat):
    return lax.dot_general(
        left_mat, right_mat, (((0,), (0,)), ((), ())), preferred_element_type=jnp.float32
    )


def product_nt(left_mat, right_mat):
    return lax.dot_general(
        left_mat, right_mat, (((1,), (1,)), ((), ())), preferred_element_type=jnp.float32
    )


def low(values):
    return values.astype(jnp.bfloat16)


def exchange(blocks, axes):
    return lax.all_to_all(blocks, axes, split_axis=0, concat_axis=0, tiled=True)


def spread(block, axes):
    count = lax.axis_size(axes)
    return exchange(jnp.broadcast_to(block[None], (count,) + block.shape), axes)


def gather_rows(block):
    return lax.all_gather(block, DP, axis=0, tiled=True)


def sum_blocks(blocks):
    return jnp.sum(blocks.astype(jnp.float32), axis=0)


def row_blocks(partial_rows):
    return low(partial_rows).reshape(lax.axis_size(DP), -1, partial_rows.shape[-1])


def beside(move, blocks, work, operands, late=()):
    blocks, operands = lax.optimization_barrier((blocks, operands))
    return lax.optimization_barrier((move(blocks), work(*operands, *late)))


def started(operands, blocks):
    tile = blocks[0, :16, :128]
    return after(operands, other_core(tile))


def over_dp(blocks):
    return exchange(blocks, DP)


def over_homes(blocks):
    return exchange(blocks, HOMES)


def after(values, event):
    return lax.optimization_barrier((values, event))[0]


def permute_copies(block, axis):
    count = lax.axis_size(axis)
    blocks = [block]
    for step in range(1, count):
        route = [((i - step) % count, i) for i in range(count)]
        blocks.append(lax.ppermute(block, axis, route))
    return blocks


def own_parts(blocks, axis):
    count = lax.axis_size(axis)
    place = lax.axis_index(axis)
    return [
        lax.dynamic_index_in_dim(blocks, (place + step) % count, 0, keepdims=False)
        for step in range(count)
    ]


def sent_parts(parts, axis):
    count = len(parts)
    return [parts[0]] + [
        lax.ppermute(parts[step], axis, [((i - step) % count, i) for i in range(count)])
        for step in range(1, count)
    ]


def permute_parts(blocks, axis):
    return sent_parts(own_parts(blocks, axis), axis)


SCALAR = pl.BlockSpec(memory_space=pltpu.SMEM)
WHOLE = pl.BlockSpec(memory_space=pltpu.VMEM)


def in_order(blocks, axis):
    count = lax.axis_size(axis)

    def kernel(place, *refs):
        for step in range(count):
            refs[-1][(place[0] + count - step) % count] = refs[step][...]

    return pl.pallas_call(
        kernel,
        out_shape=jax.ShapeDtypeStruct((count,) + blocks[0].shape, blocks[0].dtype),
        in_specs=[SCALAR] + [WHOLE] * count,
        compiler_params=pltpu.CompilerParams(vmem_limit_bytes=32 << 20),
        name="in_order",
    )(lax.axis_index(axis).reshape(1), *blocks)


def finish_weights(section_id, ups, attns, down_sums, hidden_rows):
    dp_size, rows, half_hidden = ups[0].shape
    down_rows, half_width = down_sums[0].shape
    width = 2 * half_width
    head_width = width // dp_size
    qkv_half = 3 * head_width // 2

    def kernel(place, *refs):
        qkv_ref, proj_ref, up_ref, down_ref = refs[12:]

        def write(up_halves, attn_halves, down_halves):
            for half in range(2):
                up, attn = up_halves[half], attn_halves[half]
                here = slice(half * half_width, (half + 1) * half_width)
                proj_sum = attn[0, :, :half_width].astype(jnp.float32)
                for z in range(1, dp_size):
                    proj_sum = proj_sum + attn[z, :, :half_width].astype(jnp.float32)
                proj_ref[:, here] = proj_sum
                down_ref[:, here] = down_halves[half][...].astype(jnp.float32)
                for z in range(dp_size):
                    for piece in range(half_hidden // hidden_rows):
                        group = half * (half_hidden // hidden_rows) + piece
                        start = (group * dp_size + z) * hidden_rows
                        up_ref[:, start : start + hidden_rows] = up[
                            z, :, piece * hidden_rows : (piece + 1) * hidden_rows
                        ].astype(jnp.float32)
                    at = 0
                    while at < qkv_half:
                        column = half * qkv_half + at
                        part, inner = column // head_width, column % head_width
                        size = min(head_width - inner, qkv_half - at)
                        first = half_width + at
                        start = part * width + z * head_width + inner
                        qkv_ref[:, start : start + size] = attn[
                            z, :, first : first + size
                        ].astype(jnp.float32)
                        at = at + size

        @pl.when(place[0] == 0)
        def _():
            write(refs[0:2], refs[4:6], refs[8:10])

        @pl.when(place[0] != 0)
        def _():
            write(refs[3:1:-1], refs[7:5:-1], refs[11:9:-1])

    shapes = ((rows, 3 * width), (rows, width), (rows, 2 * half_hidden * dp_size), (down_rows, width))
    return pl.pallas_call(
        kernel,
        out_shape=[jax.ShapeDtypeStruct(shape, jnp.float32) for shape in shapes],
        in_specs=[SCALAR] + [WHOLE] * 12,
        compiler_params=pltpu.CompilerParams(vmem_limit_bytes=32 << 20),
        name="finish_weights",
    )(section_id.reshape(1), *ups, *attns, *down_sums)


def finish_rows(section_id, *arrays):
    count = len(arrays)

    def kernel(place, *refs):
        outs = refs[4 * count :]
        for index in range(count):
            own_zero, other_zero, own_one, other_one = refs[4 * index : 4 * index + 4]

            @pl.when(place[0] == 0)
            def _():
                outs[index][0] = own_zero[...]
                outs[index][1] = other_zero[...]

            @pl.when(place[0] != 0)
            def _():
                outs[index][0] = other_one[...]
                outs[index][1] = own_one[...]

    return pl.pallas_call(
        kernel,
        out_shape=[
            jax.ShapeDtypeStruct((2,) + array[0].shape, array[0].dtype) for array in arrays
        ],
        in_specs=[SCALAR] + [WHOLE] * (4 * count),
        compiler_params=pltpu.CompilerParams(vmem_limit_bytes=32 << 20),
        name="finish_rows",
    )(section_id.reshape(1), *[rows for array in arrays for rows in array])


def sum_parts(parts):
    return sum(part.astype(jnp.float32) for part in parts)


def softmax_rows(queries, keys, allowed):
    scores = product_nt(queries, keys) * 0.125
    scores = jnp.where(allowed, scores, -jnp.inf)
    exp_scores = jnp.exp(scores - jnp.max(scores, axis=-1, keepdims=True))
    return exp_scores / jnp.sum(exp_scores, axis=-1, keepdims=True)


def allowed_keys(seg_column, seg_row):
    rows, columns = seg_column.shape[0], seg_row.shape[1]
    query_at = lax.broadcasted_iota(jnp.int32, (rows, columns), 0)
    key_at = lax.broadcasted_iota(jnp.int32, (rows, columns), 1)
    return (seg_column == seg_row) & (key_at <= query_at)


def head_slices(packed, head, head_width):
    start = head * HEAD_DIM
    return [
        packed[:, part * head_width + start : part * head_width + start + HEAD_DIM]
        for part in range(3)
    ]


def attention_kernel(seg_column, seg_row, qkv_ref, mixed_ref):
    head_width = mixed_ref.shape[1]
    allowed = allowed_keys(seg_column[...], seg_row[...])
    packed = qkv_ref[...]
    mixed = []
    for head in range(head_width // HEAD_DIM):
        queries, keys, values = head_slices(packed, head, head_width)
        probs = softmax_rows(queries, keys, allowed)
        mixed.append(low(product(low(probs), values)))
    mixed_ref[...] = jnp.concatenate(mixed, axis=1)


def attention_back_kernel(seg_column, seg_row, qkv_ref, d_mixed_ref, d_qkv_ref):
    head_width = d_mixed_ref.shape[1]
    allowed = allowed_keys(seg_column[...], seg_row[...])
    packed = qkv_ref[...]
    d_mixed_all = d_mixed_ref[...]
    grads = [[], [], []]
    for head in range(head_width // HEAD_DIM):
        queries, keys, values = head_slices(packed, head, head_width)
        d_mixed = d_mixed_all[:, head * HEAD_DIM : (head + 1) * HEAD_DIM]
        probs = softmax_rows(queries, keys, allowed)
        d_probs = product_nt(d_mixed, values)
        d_scores = low(probs * (d_probs - jnp.sum(probs * d_probs, axis=-1, keepdims=True)))
        grads[0].append(low(product(d_scores, keys) * 0.125))
        grads[1].append(low(product_tn(d_scores, queries) * 0.125))
        grads[2].append(low(product_tn(low(probs), d_mixed)))
    d_qkv_ref[...] = jnp.concatenate(grads[0] + grads[1] + grads[2], axis=1)


def attention(segments, qkv):
    head_width = qkv.shape[1] // 3
    return pl.pallas_call(
        attention_kernel,
        out_shape=jax.ShapeDtypeStruct((qkv.shape[0], head_width), jnp.bfloat16),
        compiler_params=pltpu.CompilerParams(vmem_limit_bytes=32 << 20),
        name="attention",
    )(segments[:, None], segments[None, :], qkv)


def attention_back(segments, qkv, d_mixed):
    return pl.pallas_call(
        attention_back_kernel,
        out_shape=jax.ShapeDtypeStruct(qkv.shape, jnp.bfloat16),
        compiler_params=pltpu.CompilerParams(vmem_limit_bytes=32 << 20),
        name="attention_back",
    )(segments[:, None], segments[None, :], qkv, d_mixed)


IN_HBM = pl.BlockSpec(memory_space=pltpu.HBM)


def in_hbm(mat):
    return pltpu.with_memory_space_constraint(mat, pltpu.HBM)


def expert_call(kernel, name, outs, section_id, operands, up_pair, down_pair, extra=()):
    width, hidden = up_pair[0].shape
    half = hidden // 2
    return pl.pallas_call(
        kernel,
        out_shape=[pltpu.HBM(shape, dtype) for shape, dtype in outs],
        out_specs=[WHOLE for _ in outs],
        in_specs=[SCALAR] + [WHOLE] * len(operands) + [IN_HBM] * (4 + len(extra)),
        scratch_shapes=[
            pltpu.VMEM((2, width, half), jnp.bfloat16),
            pltpu.VMEM((2, half, width), jnp.bfloat16),
            pltpu.SemaphoreType.DMA((2, 2)),
        ]
        + [pltpu.VMEM((2, mat.shape[0], half), mat.dtype) for mat in extra]
        + [pltpu.SemaphoreType.DMA((2,)) for _ in extra],
        compiler_params=pltpu.CompilerParams(vmem_limit_bytes=40 << 20),
        name=name,
    )(section_id.reshape(1), *operands, *[in_hbm(mat) for mat in (*up_pair, *down_pair, *extra)])


def expert_weights_in(layer, place, sources, up_here, down_here, arrived):
    half = up_here.shape[2]

    def copies(which, part):
        columns = pl.ds(part * half, half)
        return (
            pltpu.make_async_copy(
                sources[which].at[:, columns], up_here.at[part], arrived.at[0, part]
            ),
            pltpu.make_async_copy(
                sources[2 + which].at[columns], down_here.at[part], arrived.at[1, part]
            ),
        )

    for which in range(2):

        @pl.when((place[0] == layer) if which == 0 else (place[0] != layer))
        def _():
            for part in range(2):
                for copy in copies(which, part):
                    copy.start()

    return [copies(0, part) for part in range(2)]


def row_scales(logits, expert):
    lane = lax.broadcasted_iota(jnp.int32, logits.shape, 1)
    experts = logits.shape[1] - 2

    def share(among, one):
        chosen = jnp.where(among, logits, -jnp.inf)
        weights = jnp.exp(chosen - jnp.max(chosen, axis=1, keepdims=True))
        part = jnp.sum(jnp.where(one, weights, 0.0), axis=1, keepdims=True)
        return part / jnp.sum(weights, axis=1, keepdims=True)

    return share(lane >= experts, lane == experts + 1) * share(lane < experts, lane == expert)


def expert_forward(layer, section_id, expert, rows, small_weights, up_pair, down_pair):
    def kernel(place, expert_ref, rows_ref, small_ref, *refs):
        scale_ref, hidden_ref, low_ref, part_ref, up_here, down_here, arrived = refs[4:]
        waits = expert_weights_in(layer, place, refs[:4], up_here, down_here, arrived)
        scale_ref[...] = row_scales(product_nt(rows_ref[...], small_ref[...]), expert_ref[0, 0])
        half = up_here.shape[2]
        total = None
        for part in range(2):
            here = slice(part * half, (part + 1) * half)
            waits[part][0].wait()
            hidden = product(rows_ref[...], up_here[part])
            hidden_ref[:, here] = hidden
            hidden_low = low(gelu_tanh(hidden))
            low_ref[:, here] = hidden_low
            waits[part][1].wait()
            added = product(hidden_low, down_here[part])
            total = added if total is None else total + added
        part_ref[...] = low(total)

    count, width = rows.shape
    hidden = up_pair[0].shape[1]
    outs = [((count, 1), jnp.float32), ((count, hidden), jnp.float32)]
    outs += [((count, hidden), jnp.bfloat16), ((count, width), jnp.bfloat16)]
    return expert_call(
        kernel,
        "expert_forward",
        outs,
        section_id,
        (expert.reshape(1, 1), rows, small_weights),
        up_pair,
        down_pair,
    )


def expert_backward(layer, section_id, grad_rows, scale, hidden, up_pair, down_pair):
    def kernel(place, rows_ref, scale_ref, *refs):
        scaled_ref, d_hidden_ref, back_ref, up_here, down_here, arrived = refs[5:11]
        hidden_here, hidden_arrived = refs[11:]
        waits = expert_weights_in(layer, place, refs[:4], up_here, down_here, arrived)
        half = up_here.shape[2]
        fetches = [
            pltpu.make_async_copy(
                refs[4].at[:, pl.ds(part * half, half)], hidden_here.at[part], hidden_arrived.at[part]
            )
            for part in range(2)
        ]
        for fetch in fetches:
            fetch.start()
        scaled = low(scale_ref[...] * rows_ref[...].astype(jnp.float32))
        scaled_ref[...] = scaled
        total = None
        for part in range(2):
            here = slice(part * half, (part + 1) * half)
            waits[part][1].wait()
            d_low = product_nt(scaled, down_here[part])
            fetches[part].wait()
            d_hidden = low(gelu_grad(hidden_here[part], d_low))
            d_hidden_ref[:, here] = d_hidden
            waits[part][0].wait()
            added = product_nt(d_hidden, up_here[part])
            total = added if total is None else total + added
        back_ref[...] = low(total)

    shape = ((grad_rows.shape), jnp.bfloat16)
    outs = [shape, (hidden.shape, jnp.bfloat16), shape]
    return expert_call(
        kernel,
        "expert_backward",
        outs,
        section_id,
        (grad_rows, scale),
        up_pair,
        down_pair,
        (hidden,),
    )


def pair_grads(section_id, *pairs):
    mats = [side for left, right in pairs for side in (left, other_core(left), right, other_core(right))]
    left_width = pairs[0][0].shape[1]
    halves = [right.shape[1] // 2 for _, right in pairs]

    def kernel(place, *refs):
        start = 0
        for index, half in enumerate(halves):
            left_own, left_other, right_own, right_other = refs[4 * index : 4 * index + 4]
            here = pl.ds(pl.multiple_of(place[0] * half, LANES), half)
            total = product_tn(left_own[...], right_own[:, here])
            total = total + product_tn(left_other[...], right_other[:, here])
            refs[-1][:, start : start + half] = low(total)
            start = start + half

    return pl.pallas_call(
        kernel,
        out_shape=jax.ShapeDtypeStruct((left_width, sum(halves)), jnp.bfloat16),
        in_specs=[SCALAR] + [WHOLE] * len(mats),
        compiler_params=pltpu.CompilerParams(vmem_limit_bytes=40 << 20),
        name="pair_grads",
    )(section_id.reshape(1), *mats)


OWNER_TILE = 512


def owner_grads(section_id, left_mats, right_mats):
    rows, left_width = left_mats[0].shape
    right_width = right_mats[0].shape[1]
    tiles = left_width // OWNER_TILE

    def kernel(place, *refs):
        out_ref, left_here, right_here, arrived = refs[8:]
        expert, tile = pl.program_id(0), pl.program_id(1)

        def copies(source, slot):
            return (
                pltpu.make_async_copy(refs[source], left_here.at[slot], arrived.at[0, slot]),
                pltpu.make_async_copy(refs[4 + source], right_here.at[slot], arrived.at[1, slot]),
            )

        for first, sources in ((True, (0, 1)), (False, (3, 2))):
            here = (place[0] == 0) if first else (place[0] != 0)

            @pl.when(here & (expert == 0) & (tile == 0))
            def _():
                for slot, source in enumerate(sources):
                    for copy in copies(source, slot):
                        copy.start()

        @pl.when(tile == 0)
        def _():
            for copy in copies(0, expert):
                copy.wait()

        left = left_here[expert, :, pl.ds(tile * OWNER_TILE, OWNER_TILE)]
        out_ref[0] = product_tn(left, right_here[expert])

    return pl.pallas_call(
        kernel,
        out_shape=jax.ShapeDtypeStruct((2, left_width, right_width), jnp.float32),
        grid=(2, tiles),
        in_specs=[SCALAR] + [IN_HBM] * 8,
        out_specs=pl.BlockSpec((1, OWNER_TILE, right_width), lambda expert, tile: (expert, tile, 0)),
        scratch_shapes=[
            pltpu.VMEM((2, rows, left_width), jnp.bfloat16),
            pltpu.VMEM((2, rows, right_width), jnp.bfloat16),
            pltpu.SemaphoreType.DMA((2, 2)),
        ],
        compiler_params=pltpu.CompilerParams(vmem_limit_bytes=40 << 20),
        name="owner_grads",
    )(section_id.reshape(1), *[in_hbm(mat) for mat in (*left_mats, *right_mats)])


def statistics(value_rows):
    centre = jnp.mean(value_rows, axis=-1, keepdims=True)
    centred = value_rows - centre
    variance = jnp.mean(centred * centred, axis=-1, keepdims=True)
    spread_inverse = lax.rsqrt(variance + 1e-05)
    return centred * spread_inverse, spread_inverse


def column_sums(value_rows):
    return jnp.sum(value_rows, axis=0, keepdims=True)


def block_sum(blocks_ref):
    total = blocks_ref[0].astype(jnp.float32)
    for place in range(1, blocks_ref.shape[0]):
        total = total + blocks_ref[place].astype(jnp.float32)
    return total


def call(kernel, name, outs, *operands):
    specs = [
        pl.BlockSpec(memory_space=pltpu.HBM)
        if operand.shape[1:] == (operand.shape[-1],) * 2
        else WHOLE
        for operand in operands
    ]
    operands = [
        operand if spec is WHOLE else pltpu.with_memory_space_constraint(operand, pltpu.HBM)
        for operand, spec in zip(operands, specs)
    ]
    mats = [operand.shape[1:] for operand, spec in zip(operands, specs) if spec is not WHOLE]
    scratch = [pltpu.VMEM(shape, jnp.bfloat16) for shape in mats]
    scratch += [pltpu.SemaphoreType.DMA for _ in mats]
    return pl.pallas_call(
        kernel,
        in_specs=specs,
        out_shape=[jax.ShapeDtypeStruct(shape, dtype) for shape, dtype in outs],
        scratch_shapes=scratch,
        compiler_params=pltpu.CompilerParams(vmem_limit_bytes=32 << 20),
        name=name,
    )(*operands)


def project(layer, mixed_blocks, proj_mat, layer_in, gain, shift):
    def kernel(mixed_ref, proj_ref, in_ref, gain_ref, shift_ref, *outs):
        rows_ref, res_ref, mid_ref, sq_ref, proj_here, arrived = outs
        fetch = pltpu.make_async_copy(proj_ref.at[layer], proj_here, arrived)
        fetch.start()
        places = mixed_ref.shape[0]
        mixed = jnp.concatenate([mixed_ref[place] for place in range(places)], axis=1)
        rows_ref[...] = mixed
        fetch.wait()
        branch = product(mixed, proj_here[...])
        residual = in_ref[...].astype(jnp.float32) + branch
        res_ref[...] = residual
        mid_ref[...] = low(statistics(residual)[0] * gain_ref[...] + shift_ref[...])
        sq_ref[...] = column_sums(branch * branch)

    rows, width = layer_in.shape
    outs = [((rows, width), jnp.bfloat16), ((rows, width), jnp.float32)]
    outs += [((rows, width), jnp.bfloat16), ((1, width), jnp.float32)]
    return call(kernel, "project", outs, mixed_blocks, proj_mat, layer_in, gain, shift)


def layer_end(branch_blocks, residual, gain, shift):
    def kernel(blocks_ref, res_ref, gain_ref, shift_ref, out_ref, normed_ref, sq_ref):
        branch = block_sum(blocks_ref)
        layer_out = res_ref[...] + branch
        rounded = low(layer_out)
        out_ref[...] = rounded
        normed = statistics(rounded.astype(jnp.float32))[0]
        normed_ref[...] = low(normed * gain_ref[...] + shift_ref[...])
        sq_ref[0:1] = column_sums(branch * branch)
        sq_ref[1:2] = column_sums(layer_out * layer_out)

    shape = residual.shape
    outs = [(shape, jnp.bfloat16), (shape, jnp.bfloat16), ((2, shape[1]), jnp.float32)]
    return call(kernel, "layer_end", outs, branch_blocks, residual, gain, shift)


def norm_back(blocks_ref, value_ref, gain_ref, grad_ref, gain_grad_ref, shift_grad_ref):
    d_normed = block_sum(blocks_ref)
    normed, spread_inverse = statistics(value_ref[...].astype(jnp.float32))
    gain_grad_ref[...] = column_sums(d_normed * normed)
    shift_grad_ref[...] = column_sums(d_normed)
    d_centred = d_normed * gain_ref[...]
    along = jnp.mean(d_centred * normed, axis=-1, keepdims=True)
    d_value = d_centred - jnp.mean(d_centred, axis=-1, keepdims=True) - normed * along
    return grad_ref[...].astype(jnp.float32) + d_value * spread_inverse


def mid_back(layer, mid_blocks, residual, gain, grad_out, proj_mat, dp_size):
    def kernel(blocks_ref, res_ref, gain_ref, grad_ref, proj_ref, *outs):
        sum_ref, low_ref, mixed_ref, gain_grad_ref, shift_grad_ref, proj_here, arrived = outs
        fetch = pltpu.make_async_copy(proj_ref.at[layer], proj_here, arrived)
        fetch.start()
        grad = norm_back(blocks_ref, res_ref, gain_ref, grad_ref, gain_grad_ref, shift_grad_ref)
        sum_ref[...] = grad
        low_ref[...] = low(grad)
        fetch.wait()
        d_mixed = low(product_nt(low(grad), proj_here[...]))
        part = d_mixed.shape[1] // dp_size
        for place in range(dp_size):
            mixed_ref[place] = d_mixed[:, place * part : (place + 1) * part]

    rows, width = residual.shape
    row = ((1, width), jnp.float32)
    outs = [((rows, width), jnp.float32), ((rows, width), jnp.bfloat16)]
    outs += [((dp_size, rows, width // dp_size), jnp.bfloat16), row, row]
    return call(kernel, "mid_back", outs, mid_blocks, residual, gain, grad_out, proj_mat)


def input_back(in_blocks, layer_in, gain, grad_resid):
    def kernel(blocks_ref, in_ref, gain_ref, grad_ref, sum_ref, low_ref, gain_grad_ref, shift_grad_ref):
        grad = norm_back(blocks_ref, in_ref, gain_ref, grad_ref, gain_grad_ref, shift_grad_ref)
        sum_ref[...] = grad
        low_ref[...] = low(grad)

    shape = layer_in.shape
    row = ((1, shape[1]), jnp.float32)
    outs = [(shape, jnp.float32), (shape, jnp.bfloat16), row, row]
    return call(kernel, "input_back", outs, in_blocks, layer_in, gain, grad_resid)


def pack_small(parts_of_layers, squares_of_layers, weight_rows):
    layers = len(parts_of_layers)
    flat = [part for parts in parts_of_layers for part in parts] + list(squares_of_layers)
    width = flat[0].shape[1]
    used = sum(part.shape[0] for part in parts_of_layers[0])
    height = -(-(used + 1) // 8) * 8
    places = width // weight_rows

    def kernel(*refs):
        out_ref, rows_ref = refs[-2], refs[-1]
        per_layer = len(parts_of_layers[0])
        for layer in range(layers):
            rows_ref[...] = jnp.zeros(rows_ref.shape, jnp.float32)
            start = 0
            for part in refs[layer * per_layer : (layer + 1) * per_layer]:
                rows_ref[start : start + part.shape[0]] = part[...]
                start = start + part.shape[0]
            lane = lax.broadcasted_iota(jnp.int32, (1, width), 1) % LANES
            marked = jnp.zeros((1, width), jnp.float32)
            sums = jnp.sum(refs[layers * per_layer + layer][...], axis=1, keepdims=True)
            for kind in range(3):
                marked = jnp.where(lane == kind, sums[kind : kind + 1], marked)
            rows_ref[start : start + 1] = marked
            for place in range(places):
                column = place * weight_rows // LANES * LANES
                out_ref[layer * places + place] = rows_ref[:, column : column + LANES]

    return pl.pallas_call(
        kernel,
        out_shape=jax.ShapeDtypeStruct((layers * places, height, LANES), jnp.float32),
        scratch_shapes=[pltpu.VMEM((height, width), jnp.float32)],
        name="pack_small",
    )(*flat)


def other_core(block):
    return lax.ppermute(block, SEC, [(0, 1), (1, 0)])


def shards(
    inputs,
    cotangent,
    segment_ids,
    routes,
    norm_gains,
    norm_shifts,
    attn_qkv,
    attn_proj,
    dense_up,
    dense_down,
    router,
    mixer,
    expert_up,
    expert_down,
):
    sections = lax.axis_size(SEC)
    groups = lax.axis_size(EX)
    dp_size = lax.axis_size(DP)
    section_id = lax.axis_index(SEC)
    expert_id = lax.axis_index(EX)
    micro_count = inputs.shape[0]
    seq_rows = inputs.shape[2]
    width = inputs.shape[3]
    full_len = segment_ids.shape[2]
    experts_total = router.shape[2]
    hidden_rows = dense_down.shape[1]
    weight_rows = attn_qkv.shape[1]
    heads_here = HEADS // dp_size
    head_width = heads_here * HEAD_DIM
    capacity = max(2, 5 * seq_rows // (4 * experts_total))
    slots = dp_size * capacity
    devices = sections * groups * dp_size

    small_parts = jnp.concatenate([norm_gains[0], norm_shifts[0], router[0].T, mixer[0].T], axis=0)
    small_count = small_parts.shape[0]
    route_row = low(routes[0, :, 0, :, 0])
    message = jnp.concatenate([small_parts.reshape(-1), route_row.reshape(-1)])
    filled = message.shape[0]
    padded = -(-filled // 1024) * 1024
    message = jnp.pad(message, (0, padded - filled)).reshape(padded // 128, 128)

    def expert_parts(*own_layers):
        return [
            (
                lax.dynamic_index_in_dim(own_layer, section_id, 0, keepdims=False),
                lax.dynamic_index_in_dim(own_layer, 1 - section_id, 0, keepdims=False),
            )
            for own_layer in own_layers
        ]

    hidden_here = groups * hidden_rows
    small_all, (proj_rows, up_parts) = beside(
        lambda blocks: exchange(blocks, EVERY),
        jnp.broadcast_to(message[None], (devices,) + message.shape),
        lambda proj_shard, up_cols: (
            in_order(permute_copies(proj_shard, DP), DP),
            own_parts(
                up_cols.reshape(weight_rows, groups, dp_size, hidden_rows)
                .transpose(2, 0, 1, 3)
                .reshape(dp_size, weight_rows, hidden_here),
                DP,
            ),
        ),
        (attn_proj[0], dense_up[0]),
    )
    small_all = small_all.reshape(sections, groups, dp_size, padded)

    def params_of(small_all):
        params_all = small_all[..., : small_count * weight_rows].reshape(
            sections, groups * dp_size, small_count, weight_rows
        )
        return params_all.transpose(0, 2, 1, 3).reshape(sections, small_count, width)

    def routes_of(small_all):
        routes_all = lax.dynamic_index_in_dim(
            small_all[..., small_count * weight_rows : filled], expert_id, 1, keepdims=False
        ).reshape(sections, dp_size, micro_count, seq_rows)
        routes_all = lax.dynamic_index_in_dim(routes_all, section_id, 2, keepdims=False)
        return routes_all.astype(jnp.int32)

    on_first = section_id == 0

    def by_layer(pair):
        of_own_layer, of_other_layer = pair
        return (
            jnp.where(on_first, of_own_layer, of_other_layer),
            jnp.where(on_first, of_other_layer, of_own_layer),
        )

    proj_both = lax.all_gather(proj_rows.reshape(-1, width), HOMES, axis=0, tiled=True)
    proj_both = proj_both.reshape(sections, width, width)
    qkv_cols = attn_qkv[0].reshape(weight_rows, 3, dp_size, head_width).transpose(2, 0, 1, 3)
    qkv_cols, small_all = lax.optimization_barrier(
        (qkv_cols.reshape(dp_size, weight_rows, 3 * head_width), small_all)
    )
    qkv_cols, expert_weights = beside(
        over_dp, qkv_cols, expert_parts, (expert_up[0], expert_down[0])
    )
    params_all = params_of(small_all)
    routes_all = routes_of(small_all)
    own_input = lax.dynamic_index_in_dim(inputs[:, 0], section_id, 0, keepdims=False)
    first_params = params_all[0].astype(jnp.float32)
    first_normed = low(
        layer_norm(own_input.astype(jnp.float32), first_params[0:1], first_params[2:3])
    )
    down_both = lax.all_gather(dense_down[0], HOMES, axis=0, tiled=True)
    qkv_own, (first_seq, up_rows, down_both) = beside(
        lambda blocks: exchange(blocks, EX),
        jnp.broadcast_to(qkv_cols[None], (groups,) + qkv_cols.shape),
        lambda rows, parts, down_both: (
            in_order(permute_copies(rows, DP), DP),
            in_order(sent_parts(parts, DP), DP),
            down_both,
        ),
        (first_normed, up_parts),
        (down_both,),
    )
    first_seq = first_seq.reshape(full_len, width)
    qkv_own = qkv_own.reshape(width, 3 * head_width)
    qkv_pair = (qkv_own, other_core(qkv_own))
    exp_up_pair, exp_down_pair = [(kept, other_core(sent)) for kept, sent in expert_weights]
    first_qkv = low(product(first_seq, by_layer(qkv_pair)[0]))
    up_both = lax.all_gather(up_rows.reshape(-1, hidden_here), HOMES, axis=0, tiled=True)
    up_both = up_both.reshape(sections, width, hidden_here)
    down_both = down_both.reshape(sections, hidden_here, width)

    segments = lax.dynamic_index_in_dim(segment_ids[:, 0], section_id, 0, keepdims=False)
    places = jnp.arange(full_len, dtype=jnp.int32)
    earlier = (places[None, :] < places[:, None]) & (
        places[None, :] // seq_rows == places[:, None] // seq_rows
    )

    def slot_table(route_now):
        rank = jnp.sum(
            ((route_now[:, None] == route_now[None, :]) & earlier).astype(jnp.int32), axis=1
        )
        home = route_now % sections * groups + route_now // sections
        target = home * slots + places // seq_rows * capacity + rank
        slot_ids = jnp.arange(sections * groups * slots, dtype=jnp.int32)
        table = low(slot_ids[:, None] == target[None, :])
        hot = route_now[:, None] == jnp.arange(experts_total, dtype=jnp.int32)[None, :]
        return table, hot.astype(jnp.float32)

    def packed_rows(token_rows, table):
        return low(product(table, token_rows)).reshape(sections * groups, slots, width)

    def coefficients(mid_seq, small_weights, hot):
        small_logits = product_nt(mid_seq, small_weights)
        gate_probs = jax.nn.softmax(small_logits[:, :experts_total], axis=-1)
        gate = jnp.sum(gate_probs * hot, axis=-1, keepdims=True)
        coef = jax.nn.softmax(small_logits[:, experts_total:], axis=-1)
        return gate_probs, gate, coef

    own_expert = expert_id * sections + section_id

    def dense_in(mid_seq, up_mat):
        hidden = product(mid_seq, up_mat)
        return hidden, low(gelu_tanh(hidden))

    def attended(qkv):
        return attention(segments, qkv).reshape(dp_size, seq_rows, head_width)

    def forward_zero():
        params = first_params
        table, hot = slot_table(routes_all[0].reshape(full_len))
        mixed, residual, mid, attn_squares = project(
            0, over_dp(attended(first_qkv)), proj_both, own_input, params[1:2], params[3:4]
        )
        mid_seq = gather_rows(mid)
        small_weights = params_all[0, 4:]

        expert_blocks = packed_rows(mid_seq, table)
        expert_rows, ((gate_probs, gate, coef), own_grad_seq) = beside(
            over_homes,
            expert_blocks,
            lambda blocks, mid_seq, small_weights, grad: (
                coefficients(mid_seq, small_weights, hot),
                in_order(permute_copies(started(grad, blocks), DP), DP).reshape(full_len, width),
            ),
            (expert_blocks, mid_seq, small_weights, own_grad),
        )
        expert_rows = expert_rows.reshape(-1, width)
        scale, exp_hidden, exp_hidden_low, exp_out = expert_forward(
            0, section_id, own_expert, expert_rows, small_weights, exp_up_pair, exp_down_pair
        )

        def return_work(mid_seq, up_mat, down_mat):
            hidden, hidden_low = dense_in(mid_seq, up_mat)
            return hidden, hidden_low, product(hidden_low, down_mat)

        returned, (hidden, hidden_low, dense_part) = beside(
            over_homes,
            exp_out.reshape(-1, slots, width),
            return_work,
            (mid_seq,),
            (up_both[0], down_both[0]),
        )
        expert_part = product_tn(table, returned.reshape(-1, width))
        branch_part = coef[:, 0:1] * dense_part + coef[:, 1:2] * gate * expert_part
        branch, settled = beside(
            over_dp,
            row_blocks(branch_part),
            lambda qkv_pair, down_both: (by_layer(qkv_pair), (down_both[0], down_both[1])),
            (qkv_pair, down_both),
        )
        next_params = params_all[1].astype(jnp.float32)
        out_low, next_normed, squares = layer_end(
            branch, residual, next_params[0:1], next_params[2:3]
        )
        record = SimpleNamespace(
            params=params,
            small_weights=small_weights,
            table=table,
            hot=hot,
            layer_in=own_input,
            normed_seq=first_seq,
            qkv=first_qkv,
            mixed=mixed,
            residual=residual,
            mid_seq=mid_seq,
            expert_rows=expert_rows,
            scale=scale,
            gate_probs=gate_probs,
            gate=gate,
            coef=coef,
            hidden=hidden,
            hidden_low=hidden_low,
            dense_part=dense_part,
            exp_hidden=exp_hidden,
            exp_hidden_low=exp_hidden_low,
            expert_part=expert_part,
        )
        squares = jnp.concatenate([attn_squares, squares], axis=0)
        return out_low, next_normed, squares, record, (*settled, own_grad_seq)

    def forward_one(layer_in, normed, own_grad_seq):
        params = params_all[1].astype(jnp.float32)
        table, hot = slot_table(routes_all[1].reshape(full_len))
        normed_seq = gather_rows(normed)
        qkv = low(product(normed_seq, qkv_both[1]))
        mixed, up_apart = beside(
            over_dp, attended(qkv), lambda mats: (mats[0], mats[1]), (up_both,)
        )
        mixed, residual, mid, attn_squares = project(
            1, mixed, proj_both, layer_in, params[1:2], params[3:4]
        )
        grad_rows, mid_seq = beside(
            over_homes, packed_rows(own_grad_seq, table), gather_rows, (mid,)
        )
        small_weights = params_all[1, 4:]

        def dispatch_work(mid_seq, small_weights, up_mat):
            return coefficients(mid_seq, small_weights, hot), dense_in(mid_seq, up_mat)

        expert_rows, ((gate_probs, gate, coef), (hidden, hidden_low)) = beside(
            over_homes,
            packed_rows(mid_seq, table),
            dispatch_work,
            (mid_seq, small_weights, up_apart[1]),
        )
        expert_rows = expert_rows.reshape(-1, width)
        scale, exp_hidden, exp_hidden_low, exp_out = expert_forward(
            1, section_id, own_expert, expert_rows, small_weights, exp_up_pair, exp_down_pair
        )
        returned, dense_part = beside(
            over_homes, exp_out.reshape(-1, slots, width), product, (hidden_low, down_apart[1])
        )
        expert_part = product_tn(table, returned.reshape(-1, width))
        branch_part = coef[:, 0:1] * dense_part + coef[:, 1:2] * gate * expert_part
        branch = low(branch_part)
        record = SimpleNamespace(
            params=params,
            small_weights=small_weights,
            table=table,
            hot=hot,
            layer_in=layer_in,
            normed_seq=normed_seq,
            qkv=qkv,
            mixed=mixed,
            residual=residual,
            mid_seq=mid_seq,
            expert_rows=expert_rows,
            scale=scale,
            gate_probs=gate_probs,
            gate=gate,
            coef=coef,
            hidden=hidden,
            hidden_low=hidden_low,
            dense_part=dense_part,
            exp_hidden=exp_hidden,
            exp_hidden_low=exp_hidden_low,
            expert_part=expert_part,
        )
        return branch, attn_squares, record, grad_rows, up_apart

    def over_expert(grad_mat):
        return lax.psum_scatter(grad_mat, EX, scatter_dimension=0, tiled=True)

    def by_rows(grad_mat, count):
        return low(grad_mat).reshape(count, -1, grad_mat.shape[-1])

    def dp_blocks(*grad_mats):
        blocks = [by_rows(grad_mat, dp_size) for grad_mat in grad_mats]
        return own_parts(jnp.concatenate(blocks, axis=2), DP)

    half_hidden, half_width = hidden_here // 2, width // 2

    def backward_layer(layer, grad_low, grad_seq, record, sums_one=(), operands_one=None, settle=(), grad_rows=None):
        params = record.params
        coef, gate, table = record.coef, record.gate, record.table
        def dense_back(grad_seq, coef, down_mat, up_mat, *sums_one):
            grad_seq = grad_seq.astype(jnp.float32)
            early = dp_blocks(*sums_one) if sums_one else ()
            d_dense = low(coef[:, 0:1] * grad_seq)
            dense_dot = jnp.sum(grad_seq * record.dense_part, axis=-1, keepdims=True)
            expert_dot = jnp.sum(grad_seq * record.expert_part, axis=-1, keepdims=True)
            d_coef = jnp.concatenate([dense_dot, gate * expert_dot], axis=1)
            d_mix = coef * (d_coef - jnp.sum(coef * d_coef, axis=-1, keepdims=True))
            d_logits = record.gate_probs * (record.hot - gate) * (coef[:, 1:2] * expert_dot)
            d_small = low(jnp.concatenate([d_logits, d_mix], axis=1))
            d_up = low(gelu_grad(record.hidden, product_nt(d_dense, down_mat)))
            d_mid_part = product_nt(d_up, up_mat) + product(d_small, record.small_weights)
            return d_dense, d_small, d_up, d_mid_part, early

        dense_operands = (grad_seq, coef, down_apart[layer], up_apart[layer])
        if layer == 0:
            grad_rows, dense_grad = beside(
                over_homes,
                packed_rows(grad_seq, table),
                dense_back,
                dense_operands,
                tuple(sums_one),
            )
        expert_grad_rows, d_exp_hidden, expert_back = expert_backward(
            layer,
            section_id,
            grad_rows.reshape(-1, width),
            record.scale,
            record.exp_hidden,
            exp_up_pair,
            exp_down_pair,
        )
        expert_operands = (
            record.expert_rows,
            d_exp_hidden,
            record.exp_hidden_low,
            expert_grad_rows,
        )

        swapped = tuple(other_core(operand) for operand in expert_operands)

        def owner_mats(index):
            return (
                expert_operands[index],
                swapped[index],
                operands_one[0][index],
                operands_one[1][index],
            )

        def dense_grads(hidden_low, d_dense, mid_seq, d_up, d_small):
            g_dense = pair_grads(section_id, (mid_seq, d_up), (hidden_low, d_dense))
            return g_dense, product_tn(d_small, mid_seq)

        expert_back = expert_back.reshape(-1, slots, width)
        parts_one, g_exp_down = (), None
        if layer == 0:
            d_dense, d_small, d_up, d_mid_part, early = dense_grad
            returned, (parts_one, (g_dense, g_small)) = beside(
                over_homes,
                expert_back,
                lambda early, *operands: (sent_parts(early, DP), dense_grads(*operands)),
                (early, record.hidden_low, d_dense, record.mid_seq, d_up, d_small),
            )
            d_mid_part = d_mid_part + product_tn(table, returned.reshape(-1, width))
            d_mid, (g_exp_down, settle) = beside(
                over_dp,
                row_blocks(d_mid_part),
                lambda left, right, settle: (owner_grads(section_id, left, right), settle),
                (owner_mats(2), owner_mats(3)),
                (settle,),
            )
        else:
            returned, dense_grad = beside(
                over_homes,
                expert_back,
                lambda blocks, *operands: dense_back(*started(operands, blocks)),
                (expert_back, *dense_operands),
            )
            d_dense, d_small, d_up, d_mid_part, _ = dense_grad
            d_mid_part = d_mid_part + product_tn(table, returned.reshape(-1, width))
            d_mid, (g_dense, g_small) = beside(
                over_dp,
                row_blocks(d_mid_part),
                dense_grads,
                (record.hidden_low, d_dense, record.mid_seq, d_up, d_small),
            )
        dense_sum = over_expert(g_dense)
        d_resid, d_attn, d_mixed, d_gain_one, d_shift_one = mid_back(
            layer, d_mid, record.residual, params[1:2], grad_low, proj_both, dp_size
        )
        d_mixed = over_dp(d_mixed)

        def attention_grads(d_mixed):
            d_qkv = attention_back(segments, record.qkv, d_mixed.reshape(full_len, head_width))
            return d_qkv, row_blocks(product_nt(d_qkv, qkv_both[layer]))

        d_qkv, in_blocks = attention_grads(d_mixed)
        in_blocks, normed_seq, d_qkv = lax.optimization_barrier(
            (in_blocks, record.normed_seq, d_qkv)
        )
        g_attn = pair_grads(section_id, (record.mixed, d_attn), (normed_seq, d_qkv))
        attn_sum = over_expert(g_attn)
        beside_it = g_attn
        d_normed, beside_it = lax.optimization_barrier((over_dp(in_blocks), beside_it))
        d_input, d_input_low, d_gain_zero, d_shift_zero = input_back(
            d_normed, record.layer_in, params[0:1], d_resid
        )
        small_grads = (d_gain_zero, d_gain_one, d_shift_zero, d_shift_one, g_small)
        if layer == 0:
            extra = (parts_one, owner_mats, g_exp_down, settle)
        else:
            extra = (expert_operands, swapped)
        return d_input, d_input_low, (dense_sum, attn_sum), small_grads, extra

    own_grad = lax.dynamic_index_in_dim(cotangent[:, 0], section_id, 0, keepdims=False)
    out_zero, next_normed, squares_zero, record_zero, settled = forward_zero()
    qkv_both, down_apart, own_grad_seq = settled
    branch_one, attn_squares_one, record_one, grad_rows, up_apart = forward_one(
        out_zero, next_normed, own_grad_seq
    )
    grad_one, grad_one_low, sums_one, small_one, operands_one = backward_layer(
        1, own_grad, own_grad_seq, record_one, grad_rows=grad_rows
    )
    dense_one, attn_one = sums_one
    branch_one = lax.psum_scatter(
        after(branch_one, grad_one_low), DP, scatter_dimension=0, tiled=True
    )
    grad_zero, _, (dense_zero, attn_zero), small_zero, extra = backward_layer(
        0,
        grad_one_low,
        gather_rows(grad_one_low),
        record_zero,
        (dense_one[:, :half_hidden], attn_one),
        operands_one,
        branch_one,
    )
    parts_one, owner_mats, grad_exp_down, branch_one = extra
    branch_one = branch_one.astype(jnp.float32)
    out_one = record_one.residual + branch_one
    squares_one = jnp.concatenate(
        [attn_squares_one, column_sums(branch_one * branch_one), column_sums(out_one * out_one)]
    )
    out_one = low(out_one)

    moved_one = in_order(after(parts_one, grad_zero), DP)
    small_message = pack_small(
        (small_zero, small_one), (squares_zero, squares_one), weight_rows
    )
    small_moved, grad_exp_up = beside(
        lambda blocks: exchange(blocks, EVERY),
        small_message,
        lambda *mats: owner_grads(section_id, *mats),
        (owner_mats(0), owner_mats(1)),
    )
    up_zero = over_dp(by_rows(after(dense_zero[:, :half_hidden], small_moved), dp_size))

    def of_both(of_zero, of_one):
        return of_zero, other_core(of_zero), of_one, other_core(of_one)

    def last_rows(small_moved, *rows):
        return jnp.sum(small_moved, axis=0), finish_rows(section_id, *rows)

    attn_zero, (small_sum, (activations, input_grads)) = beside(
        over_dp,
        by_rows(after(attn_zero, up_zero), dp_size),
        last_rows,
        (small_moved, of_both(out_zero, out_one), of_both(grad_zero, grad_one)),
    )
    up_one, attn_one = moved_one[..., :half_hidden], moved_one[..., half_hidden:]
    down_zero, down_one = dense_zero[:, half_hidden:], dense_one[:, half_hidden:]

    grad_qkv, grad_proj, grad_up, grad_down = finish_weights(
        section_id,
        of_both(up_zero, up_one),
        of_both(attn_zero, attn_one),
        of_both(down_zero, down_one),
        hidden_rows,
    )
    place = expert_id * dp_size + lax.axis_index(DP)
    sums = lax.dynamic_slice_in_dim(
        small_sum[:small_count], place * weight_rows % LANES, weight_rows, axis=1
    )
    totals = small_sum[small_count, :3]
    element_count = micro_count * seq_rows * width * groups * dp_size
    branch_rms = jnp.sqrt(totals / element_count)[None]
    return (
        activations[None, :, None],
        input_grads[None, :, None],
        sums[None, 0:2],
        sums[None, 2:4],
        grad_qkv[None],
        grad_proj[None],
        grad_up[None],
        grad_down[None],
        sums[4 : 4 + experts_total].T[None],
        sums[4 + experts_total :].T[None],
        grad_exp_up[None],
        grad_exp_down[None],
        branch_rms,
    )


def solution(mesh):
    placed = (
        P(None, EX, DP, None),
        P(None, EX, DP, None),
        P(None, EX, None),
        P(SEC, None, EX, DP, None),
        P(SEC, None, (EX, DP)),
        P(SEC, None, (EX, DP)),
        P(SEC, (EX, DP), None),
        P(SEC, (EX, DP), None),
        P(SEC, (EX, DP), None),
        P(SEC, (EX, DP), None),
        P(SEC, (EX, DP), None),
        P(SEC, (EX, DP), None),
        P(SEC, EX, None, DP),
        P(SEC, EX, DP, None),
    )
    return jax.shard_map(
        shards,
        mesh=mesh,
        in_specs=placed,
        out_specs=(
            P(SEC, None, EX, DP, None),
            P(SEC, None, EX, DP, None),
            P(SEC, None, (EX, DP)),
            P(SEC, None, (EX, DP)),
            P(SEC, (EX, DP), None),
            P(SEC, (EX, DP), None),
            P(SEC, (EX, DP), None),
            P(SEC, (EX, DP), None),
            P(SEC, (EX, DP), None),
            P(SEC, (EX, DP), None),
            P(SEC, EX, None, DP),
            P(SEC, EX, DP, None),
            P(SEC, None),
        ),
        check_vma=False,
    )
```

```python
from types import SimpleNamespace

import jax
import jax.numpy as jnp
from jax import lax
from jax.experimental import pallas as pl
from jax.experimental.pallas import tpu as pltpu
from jax.sharding import PartitionSpec as P

HEADS = 16
HEAD_DIM = 64
SEC, EX, DP = "section", "expert", "dp"
EVERY = (SEC, EX, DP)
HOMES = (SEC, EX)
LANES = 128


def layer_norm(value_rows, gain_vec, shift_vec):
    centre = jnp.mean(value_rows, axis=-1, keepdims=True)
    centred = value_rows - centre
    variance = jnp.mean(centred * centred, axis=-1, keepdims=True)
    return centred * lax.rsqrt(variance + 1e-05) * gain_vec + shift_vec


def gelu_tanh(value_rows):
    return jax.nn.gelu(value_rows, approximate=True)


def gelu_grad(value_rows, grad_in):
    return jax.vjp(gelu_tanh, value_rows)[1](grad_in)[0]


def product(left_mat, right_mat):
    return jnp.dot(left_mat, right_mat, preferred_element_type=jnp.float32)


def product_tn(left_mat, right_mat):
    return lax.dot_general(
        left_mat, right_mat, (((0,), (0,)), ((), ())), preferred_element_type=jnp.float32
    )


def product_nt(left_mat, right_mat):
    return lax.dot_general(
        left_mat, right_mat, (((1,), (1,)), ((), ())), preferred_element_type=jnp.float32
    )


def low(values):
    return values.astype(jnp.bfloat16)


def exchange(blocks, axes):
    return lax.all_to_all(blocks, axes, split_axis=0, concat_axis=0, tiled=True)


def spread(block, axes):
    count = lax.axis_size(axes)
    return exchange(jnp.broadcast_to(block[None], (count,) + block.shape), axes)


def gather_rows(block):
    return lax.all_gather(block, DP, axis=0, tiled=True)


def sum_blocks(blocks):
    return jnp.sum(blocks.astype(jnp.float32), axis=0)


def row_blocks(partial_rows):
    return low(partial_rows).reshape(lax.axis_size(DP), -1, partial_rows.shape[-1])


def beside(move, blocks, work, operands, late=()):
    blocks, operands = lax.optimization_barrier((blocks, operands))
    return lax.optimization_barrier((move(blocks), work(*operands, *late)))


def started(operands, blocks):
    tile = blocks[0, :16, :128]
    return after(operands, other_core(tile))


def over_dp(blocks):
    return exchange(blocks, DP)


def over_homes(blocks):
    return exchange(blocks, HOMES)


def after(values, event):
    return lax.optimization_barrier((values, event))[0]


def permute_copies(block, axis):
    count = lax.axis_size(axis)
    blocks = [block]
    for step in range(1, count):
        route = [((i - step) % count, i) for i in range(count)]
        blocks.append(lax.ppermute(block, axis, route))
    return blocks


def own_parts(blocks, axis):
    count = lax.axis_size(axis)
    place = lax.axis_index(axis)
    return [
        lax.dynamic_index_in_dim(blocks, (place + step) % count, 0, keepdims=False)
        for step in range(count)
    ]


def sent_parts(parts, axis):
    count = len(parts)
    return [parts[0]] + [
        lax.ppermute(parts[step], axis, [((i - step) % count, i) for i in range(count)])
        for step in range(1, count)
    ]


def permute_parts(blocks, axis):
    return sent_parts(own_parts(blocks, axis), axis)


SCALAR = pl.BlockSpec(memory_space=pltpu.SMEM)
WHOLE = pl.BlockSpec(memory_space=pltpu.VMEM)


def in_order(blocks, axis):
    count = lax.axis_size(axis)

    def kernel(place, *refs):
        for step in range(count):
            refs[-1][(place[0] + count - step) % count] = refs[step][...]

    return pl.pallas_call(
        kernel,
        out_shape=jax.ShapeDtypeStruct((count,) + blocks[0].shape, blocks[0].dtype),
        in_specs=[SCALAR] + [WHOLE] * count,
        compiler_params=pltpu.CompilerParams(vmem_limit_bytes=32 << 20),
        name="in_order",
    )(lax.axis_index(axis).reshape(1), *blocks)


def finish_weights(section_id, ups, attns, down_sums, hidden_rows):
    dp_size, rows, half_hidden = ups[0].shape
    down_rows, half_width = down_sums[0].shape
    width = 2 * half_width
    head_width = width // dp_size
    qkv_half = 3 * head_width // 2

    def kernel(place, *refs):
        qkv_ref, proj_ref, up_ref, down_ref = refs[12:]

        def write(up_halves, attn_halves, down_halves):
            for half in range(2):
                up, attn = up_halves[half], attn_halves[half]
                here = slice(half * half_width, (half + 1) * half_width)
                proj_sum = attn[0, :, :half_width].astype(jnp.float32)
                for z in range(1, dp_size):
                    proj_sum = proj_sum + attn[z, :, :half_width].astype(jnp.float32)
                proj_ref[:, here] = proj_sum
                down_ref[:, here] = down_halves[half][...].astype(jnp.float32)
                for z in range(dp_size):
                    for piece in range(half_hidden // hidden_rows):
                        group = half * (half_hidden // hidden_rows) + piece
                        start = (group * dp_size + z) * hidden_rows
                        up_ref[:, start : start + hidden_rows] = up[
                            z, :, piece * hidden_rows : (piece + 1) * hidden_rows
                        ].astype(jnp.float32)
                    at = 0
                    while at < qkv_half:
                        column = half * qkv_half + at
                        part, inner = column // head_width, column % head_width
                        size = min(head_width - inner, qkv_half - at)
                        first = half_width + at
                        start = part * width + z * head_width + inner
                        qkv_ref[:, start : start + size] = attn[
                            z, :, first : first + size
                        ].astype(jnp.float32)
                        at = at + size

        @pl.when(place[0] == 0)
        def _():
            write(refs[0:2], refs[4:6], refs[8:10])

        @pl.when(place[0] != 0)
        def _():
            write(refs[3:1:-1], refs[7:5:-1], refs[11:9:-1])

    shapes = ((rows, 3 * width), (rows, width), (rows, 2 * half_hidden * dp_size), (down_rows, width))
    return pl.pallas_call(
        kernel,
        out_shape=[jax.ShapeDtypeStruct(shape, jnp.float32) for shape in shapes],
        in_specs=[SCALAR] + [WHOLE] * 12,
        compiler_params=pltpu.CompilerParams(vmem_limit_bytes=32 << 20),
        name="finish_weights",
    )(section_id.reshape(1), *ups, *attns, *down_sums)


def finish_rows(section_id, *arrays):
    count = len(arrays)

    def kernel(place, *refs):
        outs = refs[4 * count :]
        for index in range(count):
            own_zero, other_zero, own_one, other_one = refs[4 * index : 4 * index + 4]

            @pl.when(place[0] == 0)
            def _():
                outs[index][0] = own_zero[...]
                outs[index][1] = other_zero[...]

            @pl.when(place[0] != 0)
            def _():
                outs[index][0] = other_one[...]
                outs[index][1] = own_one[...]

    return pl.pallas_call(
        kernel,
        out_shape=[
            jax.ShapeDtypeStruct((2,) + array[0].shape, array[0].dtype) for array in arrays
        ],
        in_specs=[SCALAR] + [WHOLE] * (4 * count),
        compiler_params=pltpu.CompilerParams(vmem_limit_bytes=32 << 20),
        name="finish_rows",
    )(section_id.reshape(1), *[rows for array in arrays for rows in array])


def sum_parts(parts):
    return sum(part.astype(jnp.float32) for part in parts)


def softmax_rows(queries, keys, allowed):
    scores = product_nt(queries, keys) * 0.125
    scores = jnp.where(allowed, scores, -jnp.inf)
    exp_scores = jnp.exp(scores - jnp.max(scores, axis=-1, keepdims=True))
    return exp_scores / jnp.sum(exp_scores, axis=-1, keepdims=True)


def allowed_keys(seg_column, seg_row):
    rows, columns = seg_column.shape[0], seg_row.shape[1]
    query_at = lax.broadcasted_iota(jnp.int32, (rows, columns), 0)
    key_at = lax.broadcasted_iota(jnp.int32, (rows, columns), 1)
    return (seg_column == seg_row) & (key_at <= query_at)


def head_slices(packed, head, head_width):
    start = head * HEAD_DIM
    return [
        packed[:, part * head_width + start : part * head_width + start + HEAD_DIM]
        for part in range(3)
    ]


def attention_kernel(seg_column, seg_row, qkv_ref, mixed_ref):
    head_width = mixed_ref.shape[1]
    allowed = allowed_keys(seg_column[...], seg_row[...])
    packed = qkv_ref[...]
    mixed = []
    for head in range(head_width // HEAD_DIM):
        queries, keys, values = head_slices(packed, head, head_width)
        probs = softmax_rows(queries, keys, allowed)
        mixed.append(low(product(low(probs), values)))
    mixed_ref[...] = jnp.concatenate(mixed, axis=1)


def attention_back_kernel(seg_column, seg_row, qkv_ref, d_mixed_ref, d_qkv_ref):
    head_width = d_mixed_ref.shape[1]
    allowed = allowed_keys(seg_column[...], seg_row[...])
    packed = qkv_ref[...]
    d_mixed_all = d_mixed_ref[...]
    grads = [[], [], []]
    for head in range(head_width // HEAD_DIM):
        queries, keys, values = head_slices(packed, head, head_width)
        d_mixed = d_mixed_all[:, head * HEAD_DIM : (head + 1) * HEAD_DIM]
        probs = softmax_rows(queries, keys, allowed)
        d_probs = product_nt(d_mixed, values)
        d_scores = low(probs * (d_probs - jnp.sum(probs * d_probs, axis=-1, keepdims=True)))
        grads[0].append(low(product(d_scores, keys) * 0.125))
        grads[1].append(low(product_tn(d_scores, queries) * 0.125))
        grads[2].append(low(product_tn(low(probs), d_mixed)))
    d_qkv_ref[...] = jnp.concatenate(grads[0] + grads[1] + grads[2], axis=1)


def attention(segments, qkv):
    head_width = qkv.shape[1] // 3
    return pl.pallas_call(
        attention_kernel,
        out_shape=jax.ShapeDtypeStruct((qkv.shape[0], head_width), jnp.bfloat16),
        compiler_params=pltpu.CompilerParams(vmem_limit_bytes=32 << 20),
        name="attention",
    )(segments[:, None], segments[None, :], qkv)


def attention_back(segments, qkv, d_mixed):
    return pl.pallas_call(
        attention_back_kernel,
        out_shape=jax.ShapeDtypeStruct(qkv.shape, jnp.bfloat16),
        compiler_params=pltpu.CompilerParams(vmem_limit_bytes=32 << 20),
        name="attention_back",
    )(segments[:, None], segments[None, :], qkv, d_mixed)


IN_HBM = pl.BlockSpec(memory_space=pltpu.HBM)


def in_hbm(mat):
    return pltpu.with_memory_space_constraint(mat, pltpu.HBM)


def expert_call(kernel, name, outs, section_id, operands, up_pair, down_pair, extra=()):
    width, hidden = up_pair[0].shape
    half = hidden // 2
    return pl.pallas_call(
        kernel,
        out_shape=[pltpu.HBM(shape, dtype) for shape, dtype in outs],
        out_specs=[WHOLE for _ in outs],
        in_specs=[SCALAR] + [WHOLE] * len(operands) + [IN_HBM] * (4 + len(extra)),
        scratch_shapes=[
            pltpu.VMEM((2, width, half), jnp.bfloat16),
            pltpu.VMEM((2, half, width), jnp.bfloat16),
            pltpu.SemaphoreType.DMA((2, 2)),
        ]
        + [pltpu.VMEM((2, mat.shape[0], half), mat.dtype) for mat in extra]
        + [pltpu.SemaphoreType.DMA((2,)) for _ in extra],
        compiler_params=pltpu.CompilerParams(vmem_limit_bytes=40 << 20),
        name=name,
    )(section_id.reshape(1), *operands, *[in_hbm(mat) for mat in (*up_pair, *down_pair, *extra)])


def expert_weights_in(layer, place, sources, up_here, down_here, arrived):
    half = up_here.shape[2]

    def copies(which, part):
        columns = pl.ds(part * half, half)
        return (
            pltpu.make_async_copy(
                sources[which].at[:, columns], up_here.at[part], arrived.at[0, part]
            ),
            pltpu.make_async_copy(
                sources[2 + which].at[columns], down_here.at[part], arrived.at[1, part]
            ),
        )

    for which in range(2):

        @pl.when((place[0] == layer) if which == 0 else (place[0] != layer))
        def _():
            for part in range(2):
                for copy in copies(which, part):
                    copy.start()

    return [copies(0, part) for part in range(2)]


def combine(table, returned, base, weight=None):
    def kernel(table_ref, returned_ref, base_ref, *refs):
        expert_part = product_tn(table_ref[...], returned_ref[...])
        if weight is None:
            refs[-1][...] = low(base_ref[...] + expert_part)
        else:
            refs[-2][...] = expert_part
            weights = refs[0][...]
            refs[-1][...] = low(weights[:, 0:1] * base_ref[...] + weights[:, 1:2] * expert_part)

    shape = (table.shape[1], returned.shape[1])
    outs = [jax.ShapeDtypeStruct(shape, jnp.bfloat16)]
    if weight is not None:
        outs = [jax.ShapeDtypeStruct(shape, jnp.float32)] + outs
    return pl.pallas_call(
        kernel,
        out_shape=outs,
        compiler_params=pltpu.CompilerParams(vmem_limit_bytes=32 << 20),
        name="combine",
    )(table, returned, base, *(() if weight is None else (weight,)))


def row_scales(logits, expert):
    lane = lax.broadcasted_iota(jnp.int32, logits.shape, 1)
    experts = logits.shape[1] - 2

    def share(among, one):
        chosen = jnp.where(among, logits, -jnp.inf)
        weights = jnp.exp(chosen - jnp.max(chosen, axis=1, keepdims=True))
        part = jnp.sum(jnp.where(one, weights, 0.0), axis=1, keepdims=True)
        return part / jnp.sum(weights, axis=1, keepdims=True)

    return share(lane >= experts, lane == experts + 1) * share(lane < experts, lane == expert)


def expert_forward(layer, section_id, expert, rows, small_weights, up_pair, down_pair):
    def kernel(place, expert_ref, rows_ref, small_ref, *refs):
        scale_ref, hidden_ref, low_ref, part_ref, up_here, down_here, arrived = refs[4:]
        waits = expert_weights_in(layer, place, refs[:4], up_here, down_here, arrived)
        scale_ref[...] = row_scales(product_nt(rows_ref[...], small_ref[...]), expert_ref[0, 0])
        half = up_here.shape[2]
        total = None
        for part in range(2):
            here = slice(part * half, (part + 1) * half)
            waits[part][0].wait()
            hidden = product(rows_ref[...], up_here[part])
            hidden_ref[:, here] = hidden
            hidden_low = low(gelu_tanh(hidden))
            low_ref[:, here] = hidden_low
            waits[part][1].wait()
            added = product(hidden_low, down_here[part])
            total = added if total is None else total + added
        part_ref[...] = low(total)

    count, width = rows.shape
    hidden = up_pair[0].shape[1]
    outs = [((count, 1), jnp.float32), ((count, hidden), jnp.float32)]
    outs += [((count, hidden), jnp.bfloat16), ((count, width), jnp.bfloat16)]
    return expert_call(
        kernel,
        "expert_forward",
        outs,
        section_id,
        (expert.reshape(1, 1), rows, small_weights),
        up_pair,
        down_pair,
    )


def expert_backward(layer, section_id, grad_rows, scale, hidden, up_pair, down_pair):
    def kernel(place, rows_ref, scale_ref, *refs):
        scaled_ref, d_hidden_ref, back_ref, up_here, down_here, arrived = refs[5:11]
        hidden_here, hidden_arrived = refs[11:]
        waits = expert_weights_in(layer, place, refs[:4], up_here, down_here, arrived)
        half = up_here.shape[2]
        fetches = [
            pltpu.make_async_copy(
                refs[4].at[:, pl.ds(part * half, half)], hidden_here.at[part], hidden_arrived.at[part]
            )
            for part in range(2)
        ]
        for fetch in fetches:
            fetch.start()
        scaled = low(scale_ref[...] * rows_ref[...].astype(jnp.float32))
        scaled_ref[...] = scaled
        total = None
        for part in range(2):
            here = slice(part * half, (part + 1) * half)
            waits[part][1].wait()
            d_low = product_nt(scaled, down_here[part])
            fetches[part].wait()
            d_hidden = low(gelu_grad(hidden_here[part], d_low))
            d_hidden_ref[:, here] = d_hidden
            waits[part][0].wait()
            added = product_nt(d_hidden, up_here[part])
            total = added if total is None else total + added
        back_ref[...] = low(total)

    shape = ((grad_rows.shape), jnp.bfloat16)
    outs = [shape, (hidden.shape, jnp.bfloat16), shape]
    return expert_call(
        kernel,
        "expert_backward",
        outs,
        section_id,
        (grad_rows, scale),
        up_pair,
        down_pair,
        (hidden,),
    )


def pair_grads(section_id, *pairs):
    mats = [side for left, right in pairs for side in (left, other_core(left), right, other_core(right))]
    left_width = pairs[0][0].shape[1]
    halves = [right.shape[1] // 2 for _, right in pairs]

    def kernel(place, *refs):
        start = 0
        for index, half in enumerate(halves):
            left_own, left_other, right_own, right_other = refs[4 * index : 4 * index + 4]
            here = pl.ds(pl.multiple_of(place[0] * half, LANES), half)
            total = product_tn(left_own[...], right_own[:, here])
            total = total + product_tn(left_other[...], right_other[:, here])
            refs[-1][:, start : start + half] = low(total)
            start = start + half

    return pl.pallas_call(
        kernel,
        out_shape=jax.ShapeDtypeStruct((left_width, sum(halves)), jnp.bfloat16),
        in_specs=[SCALAR] + [WHOLE] * len(mats),
        compiler_params=pltpu.CompilerParams(vmem_limit_bytes=40 << 20),
        name="pair_grads",
    )(section_id.reshape(1), *mats)


OWNER_TILE = 512


def owner_grads(section_id, left_mats, right_mats):
    rows, left_width = left_mats[0].shape
    right_width = right_mats[0].shape[1]
    tiles = left_width // OWNER_TILE

    def kernel(place, *refs):
        out_ref, left_here, right_here, arrived = refs[8:]
        expert, tile = pl.program_id(0), pl.program_id(1)

        def copies(source, slot):
            return (
                pltpu.make_async_copy(refs[source], left_here.at[slot], arrived.at[0, slot]),
                pltpu.make_async_copy(refs[4 + source], right_here.at[slot], arrived.at[1, slot]),
            )

        for first, sources in ((True, (0, 1)), (False, (3, 2))):
            here = (place[0] == 0) if first else (place[0] != 0)

            @pl.when(here & (expert == 0) & (tile == 0))
            def _():
                for slot, source in enumerate(sources):
                    for copy in copies(source, slot):
                        copy.start()

        @pl.when(tile == 0)
        def _():
            for copy in copies(0, expert):
                copy.wait()

        left = left_here[expert, :, pl.ds(tile * OWNER_TILE, OWNER_TILE)]
        out_ref[0] = product_tn(left, right_here[expert])

    return pl.pallas_call(
        kernel,
        out_shape=jax.ShapeDtypeStruct((2, left_width, right_width), jnp.float32),
        grid=(2, tiles),
        in_specs=[SCALAR] + [IN_HBM, WHOLE] * 4,
        out_specs=pl.BlockSpec((1, OWNER_TILE, right_width), lambda expert, tile: (expert, tile, 0)),
        scratch_shapes=[
            pltpu.VMEM((2, rows, left_width), jnp.bfloat16),
            pltpu.VMEM((2, rows, right_width), jnp.bfloat16),
            pltpu.SemaphoreType.DMA((2, 2)),
        ],
        compiler_params=pltpu.CompilerParams(vmem_limit_bytes=40 << 20),
        name="owner_grads",
    )(
        section_id.reshape(1),
        *[
            mat if index % 2 else in_hbm(mat)
            for index, mat in enumerate((*left_mats, *right_mats))
        ],
    )


def statistics(value_rows):
    centre = jnp.mean(value_rows, axis=-1, keepdims=True)
    centred = value_rows - centre
    variance = jnp.mean(centred * centred, axis=-1, keepdims=True)
    spread_inverse = lax.rsqrt(variance + 1e-05)
    return centred * spread_inverse, spread_inverse


def column_sums(value_rows):
    return jnp.sum(value_rows, axis=0, keepdims=True)


def block_sum(blocks_ref):
    total = blocks_ref[0].astype(jnp.float32)
    for place in range(1, blocks_ref.shape[0]):
        total = total + blocks_ref[place].astype(jnp.float32)
    return total


def call(kernel, name, outs, *operands):
    specs = [
        pl.BlockSpec(memory_space=pltpu.HBM)
        if operand.shape[1:] == (operand.shape[-1],) * 2
        else WHOLE
        for operand in operands
    ]
    operands = [
        operand if spec is WHOLE else pltpu.with_memory_space_constraint(operand, pltpu.HBM)
        for operand, spec in zip(operands, specs)
    ]
    mats = [operand.shape[1:] for operand, spec in zip(operands, specs) if spec is not WHOLE]
    scratch = [pltpu.VMEM(shape, jnp.bfloat16) for shape in mats]
    scratch += [pltpu.SemaphoreType.DMA for _ in mats]
    return pl.pallas_call(
        kernel,
        in_specs=specs,
        out_shape=[jax.ShapeDtypeStruct(shape, dtype) for shape, dtype in outs],
        scratch_shapes=scratch,
        compiler_params=pltpu.CompilerParams(vmem_limit_bytes=32 << 20),
        name=name,
    )(*operands)


def project(layer, mixed_blocks, proj_mat, layer_in, gain, shift):
    def kernel(mixed_ref, proj_ref, in_ref, gain_ref, shift_ref, *outs):
        rows_ref, res_ref, mid_ref, sq_ref, proj_here, arrived = outs
        fetch = pltpu.make_async_copy(proj_ref.at[layer], proj_here, arrived)
        fetch.start()
        places = mixed_ref.shape[0]
        mixed = jnp.concatenate([mixed_ref[place] for place in range(places)], axis=1)
        rows_ref[...] = mixed
        fetch.wait()
        branch = product(mixed, proj_here[...])
        residual = in_ref[...].astype(jnp.float32) + branch
        res_ref[...] = residual
        mid_ref[...] = low(statistics(residual)[0] * gain_ref[...] + shift_ref[...])
        sq_ref[...] = column_sums(branch * branch)

    rows, width = layer_in.shape
    outs = [((rows, width), jnp.bfloat16), ((rows, width), jnp.float32)]
    outs += [((rows, width), jnp.bfloat16), ((1, width), jnp.float32)]
    return call(kernel, "project", outs, mixed_blocks, proj_mat, layer_in, gain, shift)


def layer_end(branch_blocks, residual, gain, shift):
    def kernel(blocks_ref, res_ref, gain_ref, shift_ref, out_ref, normed_ref, sq_ref):
        branch = block_sum(blocks_ref)
        layer_out = res_ref[...] + branch
        rounded = low(layer_out)
        out_ref[...] = rounded
        normed = statistics(rounded.astype(jnp.float32))[0]
        normed_ref[...] = low(normed * gain_ref[...] + shift_ref[...])
        sq_ref[0:1] = column_sums(branch * branch)
        sq_ref[1:2] = column_sums(layer_out * layer_out)

    shape = residual.shape
    outs = [(shape, jnp.bfloat16), (shape, jnp.bfloat16), ((2, shape[1]), jnp.float32)]
    return call(kernel, "layer_end", outs, branch_blocks, residual, gain, shift)


def norm_back(blocks_ref, value_ref, gain_ref, grad_ref, gain_grad_ref, shift_grad_ref):
    d_normed = block_sum(blocks_ref)
    normed, spread_inverse = statistics(value_ref[...].astype(jnp.float32))
    gain_grad_ref[...] = column_sums(d_normed * normed)
    shift_grad_ref[...] = column_sums(d_normed)
    d_centred = d_normed * gain_ref[...]
    along = jnp.mean(d_centred * normed, axis=-1, keepdims=True)
    d_value = d_centred - jnp.mean(d_centred, axis=-1, keepdims=True) - normed * along
    return grad_ref[...].astype(jnp.float32) + d_value * spread_inverse


def mid_back(layer, mid_blocks, residual, gain, grad_out, proj_mat, dp_size):
    def kernel(blocks_ref, res_ref, gain_ref, grad_ref, proj_ref, *outs):
        sum_ref, low_ref, mixed_ref, gain_grad_ref, shift_grad_ref, proj_here, arrived = outs
        fetch = pltpu.make_async_copy(proj_ref.at[layer], proj_here, arrived)
        fetch.start()
        grad = norm_back(blocks_ref, res_ref, gain_ref, grad_ref, gain_grad_ref, shift_grad_ref)
        sum_ref[...] = grad
        low_ref[...] = low(grad)
        fetch.wait()
        d_mixed = low(product_nt(low(grad), proj_here[...]))
        part = d_mixed.shape[1] // dp_size
        for place in range(dp_size):
            mixed_ref[place] = d_mixed[:, place * part : (place + 1) * part]

    rows, width = residual.shape
    row = ((1, width), jnp.float32)
    outs = [((rows, width), jnp.float32), ((rows, width), jnp.bfloat16)]
    outs += [((dp_size, rows, width // dp_size), jnp.bfloat16), row, row]
    return call(kernel, "mid_back", outs, mid_blocks, residual, gain, grad_out, proj_mat)


def input_back(in_blocks, layer_in, gain, grad_resid):
    def kernel(blocks_ref, in_ref, gain_ref, grad_ref, sum_ref, low_ref, gain_grad_ref, shift_grad_ref):
        grad = norm_back(blocks_ref, in_ref, gain_ref, grad_ref, gain_grad_ref, shift_grad_ref)
        sum_ref[...] = grad
        low_ref[...] = low(grad)

    shape = layer_in.shape
    row = ((1, shape[1]), jnp.float32)
    outs = [(shape, jnp.float32), (shape, jnp.bfloat16), row, row]
    return call(kernel, "input_back", outs, in_blocks, layer_in, gain, grad_resid)


def pack_small(parts_of_layers, squares_of_layers, weight_rows):
    layers = len(parts_of_layers)
    flat = [part for parts in parts_of_layers for part in parts] + list(squares_of_layers)
    width = flat[0].shape[1]
    used = sum(part.shape[0] for part in parts_of_layers[0])
    height = -(-(used + 1) // 8) * 8
    places = width // weight_rows

    def kernel(*refs):
        out_ref, rows_ref = refs[-2], refs[-1]
        per_layer = len(parts_of_layers[0])
        for layer in range(layers):
            rows_ref[...] = jnp.zeros(rows_ref.shape, jnp.float32)
            start = 0
            for part in refs[layer * per_layer : (layer + 1) * per_layer]:
                rows_ref[start : start + part.shape[0]] = part[...]
                start = start + part.shape[0]
            lane = lax.broadcasted_iota(jnp.int32, (1, width), 1) % LANES
            marked = jnp.zeros((1, width), jnp.float32)
            sums = jnp.sum(refs[layers * per_layer + layer][...], axis=1, keepdims=True)
            for kind in range(3):
                marked = jnp.where(lane == kind, sums[kind : kind + 1], marked)
            rows_ref[start : start + 1] = marked
            for place in range(places):
                column = place * weight_rows // LANES * LANES
                out_ref[layer * places + place] = rows_ref[:, column : column + LANES]

    return pl.pallas_call(
        kernel,
        out_shape=jax.ShapeDtypeStruct((layers * places, height, LANES), jnp.float32),
        scratch_shapes=[pltpu.VMEM((height, width), jnp.float32)],
        name="pack_small",
    )(*flat)


def other_core(block):
    return lax.ppermute(block, SEC, [(0, 1), (1, 0)])


def shards(
    inputs,
    cotangent,
    segment_ids,
    routes,
    norm_gains,
    norm_shifts,
    attn_qkv,
    attn_proj,
    dense_up,
    dense_down,
    router,
    mixer,
    expert_up,
    expert_down,
):
    sections = lax.axis_size(SEC)
    groups = lax.axis_size(EX)
    dp_size = lax.axis_size(DP)
    section_id = lax.axis_index(SEC)
    expert_id = lax.axis_index(EX)
    micro_count = inputs.shape[0]
    seq_rows = inputs.shape[2]
    width = inputs.shape[3]
    full_len = segment_ids.shape[2]
    experts_total = router.shape[2]
    hidden_rows = dense_down.shape[1]
    weight_rows = attn_qkv.shape[1]
    heads_here = HEADS // dp_size
    head_width = heads_here * HEAD_DIM
    capacity = max(2, 5 * seq_rows // (4 * experts_total))
    slots = dp_size * capacity
    devices = sections * groups * dp_size

    small_parts = jnp.concatenate([norm_gains[0], norm_shifts[0], router[0].T, mixer[0].T], axis=0)
    small_count = small_parts.shape[0]
    route_row = low(routes[0, :, 0, :, 0])
    message = jnp.concatenate([small_parts.reshape(-1), route_row.reshape(-1)])
    filled = message.shape[0]
    padded = -(-filled // 1024) * 1024
    message = jnp.pad(message, (0, padded - filled)).reshape(padded // 128, 128)

    def expert_parts(*own_layers):
        return [
            (
                lax.dynamic_index_in_dim(own_layer, section_id, 0, keepdims=False),
                lax.dynamic_index_in_dim(own_layer, 1 - section_id, 0, keepdims=False),
            )
            for own_layer in own_layers
        ]

    hidden_here = groups * hidden_rows
    small_all, (proj_rows, up_parts) = beside(
        lambda blocks: exchange(blocks, EVERY),
        jnp.broadcast_to(message[None], (devices,) + message.shape),
        lambda proj_shard, up_cols: (
            in_order(permute_copies(proj_shard, DP), DP),
            own_parts(
                up_cols.reshape(weight_rows, groups, dp_size, hidden_rows)
                .transpose(2, 0, 1, 3)
                .reshape(dp_size, weight_rows, hidden_here),
                DP,
            ),
        ),
        (attn_proj[0], dense_up[0]),
    )
    small_all = small_all.reshape(sections, groups, dp_size, padded)

    def params_of(small_all):
        params_all = small_all[..., : small_count * weight_rows].reshape(
            sections, groups * dp_size, small_count, weight_rows
        )
        return params_all.transpose(0, 2, 1, 3).reshape(sections, small_count, width)

    def routes_of(small_all):
        routes_all = lax.dynamic_index_in_dim(
            small_all[..., small_count * weight_rows : filled], expert_id, 1, keepdims=False
        ).reshape(sections, dp_size, micro_count, seq_rows)
        routes_all = lax.dynamic_index_in_dim(routes_all, section_id, 2, keepdims=False)
        return routes_all.astype(jnp.int32)

    on_first = section_id == 0

    def by_layer(pair):
        of_own_layer, of_other_layer = pair
        return (
            jnp.where(on_first, of_own_layer, of_other_layer),
            jnp.where(on_first, of_other_layer, of_own_layer),
        )

    proj_both = lax.all_gather(proj_rows.reshape(-1, width), HOMES, axis=0, tiled=True)
    proj_both = proj_both.reshape(sections, width, width)
    qkv_cols = attn_qkv[0].reshape(weight_rows, 3, dp_size, head_width).transpose(2, 0, 1, 3)
    qkv_cols, small_all = lax.optimization_barrier(
        (qkv_cols.reshape(dp_size, weight_rows, 3 * head_width), small_all)
    )
    qkv_cols, expert_weights = beside(
        over_dp, qkv_cols, expert_parts, (expert_up[0], expert_down[0])
    )
    params_all = params_of(small_all)
    routes_all = routes_of(small_all)
    own_input = lax.dynamic_index_in_dim(inputs[:, 0], section_id, 0, keepdims=False)
    first_params = params_all[0].astype(jnp.float32)
    first_normed = low(
        layer_norm(own_input.astype(jnp.float32), first_params[0:1], first_params[2:3])
    )
    down_both = lax.all_gather(dense_down[0], HOMES, axis=0, tiled=True)
    qkv_own, (first_seq, up_rows, down_both) = beside(
        lambda blocks: exchange(blocks, EX),
        jnp.broadcast_to(qkv_cols[None], (groups,) + qkv_cols.shape),
        lambda rows, parts, down_both: (
            in_order(permute_copies(rows, DP), DP),
            in_order(sent_parts(parts, DP), DP),
            down_both,
        ),
        (first_normed, up_parts),
        (down_both,),
    )
    first_seq = first_seq.reshape(full_len, width)
    qkv_own = qkv_own.reshape(width, 3 * head_width)
    qkv_pair = (qkv_own, other_core(qkv_own))
    exp_up_pair, exp_down_pair = [(kept, other_core(sent)) for kept, sent in expert_weights]
    first_qkv = low(product(first_seq, by_layer(qkv_pair)[0]))
    up_both = lax.all_gather(up_rows.reshape(-1, hidden_here), HOMES, axis=0, tiled=True)
    up_both = up_both.reshape(sections, width, hidden_here)
    down_both = down_both.reshape(sections, hidden_here, width)

    segments = lax.dynamic_index_in_dim(segment_ids[:, 0], section_id, 0, keepdims=False)
    places = jnp.arange(full_len, dtype=jnp.int32)
    earlier = (places[None, :] < places[:, None]) & (
        places[None, :] // seq_rows == places[:, None] // seq_rows
    )

    def slot_table(route_now):
        rank = jnp.sum(
            ((route_now[:, None] == route_now[None, :]) & earlier).astype(jnp.int32), axis=1
        )
        home = route_now % sections * groups + route_now // sections
        target = home * slots + places // seq_rows * capacity + rank
        slot_ids = jnp.arange(sections * groups * slots, dtype=jnp.int32)
        table = low(slot_ids[:, None] == target[None, :])
        hot = route_now[:, None] == jnp.arange(experts_total, dtype=jnp.int32)[None, :]
        return table, hot.astype(jnp.float32)

    def packed_rows(token_rows, table):
        return low(product(table, token_rows)).reshape(sections * groups, slots, width)

    def coefficients(mid_seq, small_weights, hot):
        small_logits = product_nt(mid_seq, small_weights)
        gate_probs = jax.nn.softmax(small_logits[:, :experts_total], axis=-1)
        gate = jnp.sum(gate_probs * hot, axis=-1, keepdims=True)
        coef = jax.nn.softmax(small_logits[:, experts_total:], axis=-1)
        return gate_probs, gate, coef

    own_expert = expert_id * sections + section_id

    def dense_in(mid_seq, up_mat):
        hidden = product(mid_seq, up_mat)
        return hidden, low(gelu_tanh(hidden))

    def attended(qkv):
        return attention(segments, qkv).reshape(dp_size, seq_rows, head_width)

    def forward_zero():
        params = first_params
        table, hot = slot_table(routes_all[0].reshape(full_len))
        mixed, residual, mid, attn_squares = project(
            0, over_dp(attended(first_qkv)), proj_both, own_input, params[1:2], params[3:4]
        )
        mid_seq = gather_rows(mid)
        small_weights = params_all[0, 4:]

        expert_blocks = packed_rows(mid_seq, table)
        expert_rows, ((gate_probs, gate, coef), own_grad_seq) = beside(
            over_homes,
            expert_blocks,
            lambda blocks, mid_seq, small_weights, grad: (
                coefficients(mid_seq, small_weights, hot),
                in_order(permute_copies(started(grad, blocks), DP), DP).reshape(full_len, width),
            ),
            (expert_blocks, mid_seq, small_weights, own_grad),
        )
        expert_rows = expert_rows.reshape(-1, width)
        scale, exp_hidden, exp_hidden_low, exp_out = expert_forward(
            0, section_id, own_expert, expert_rows, small_weights, exp_up_pair, exp_down_pair
        )

        def return_work(mid_seq, up_mat, down_mat):
            hidden, hidden_low = dense_in(mid_seq, up_mat)
            return hidden, hidden_low, product(hidden_low, down_mat)

        returned, (hidden, hidden_low, dense_part) = beside(
            over_homes,
            exp_out.reshape(-1, slots, width),
            return_work,
            (mid_seq,),
            (up_both[0], down_both[0]),
        )
        expert_part = product_tn(table, returned.reshape(-1, width))
        branch_part = coef[:, 0:1] * dense_part + coef[:, 1:2] * gate * expert_part
        branch, settled = beside(
            over_dp,
            row_blocks(branch_part),
            lambda qkv_pair, down_both: (by_layer(qkv_pair), (down_both[0], down_both[1])),
            (qkv_pair, down_both),
        )
        next_params = params_all[1].astype(jnp.float32)
        out_low, next_normed, squares = layer_end(
            branch, residual, next_params[0:1], next_params[2:3]
        )
        record = SimpleNamespace(
            params=params,
            small_weights=small_weights,
            table=table,
            hot=hot,
            layer_in=own_input,
            normed_seq=first_seq,
            qkv=first_qkv,
            mixed=mixed,
            residual=residual,
            mid_seq=mid_seq,
            expert_rows=expert_rows,
            scale=scale,
            gate_probs=gate_probs,
            gate=gate,
            coef=coef,
            hidden=hidden,
            hidden_low=hidden_low,
            dense_part=dense_part,
            exp_hidden=exp_hidden,
            exp_hidden_low=exp_hidden_low,
            expert_part=expert_part,
        )
        squares = jnp.concatenate([attn_squares, squares], axis=0)
        return out_low, next_normed, squares, record, (*settled, own_grad_seq)

    def forward_one(layer_in, normed, own_grad_seq):
        params = params_all[1].astype(jnp.float32)
        table, hot = slot_table(routes_all[1].reshape(full_len))
        normed_seq = gather_rows(normed)
        qkv = low(product(normed_seq, qkv_both[1]))
        mixed, up_apart = beside(
            over_dp, attended(qkv), lambda mats: (mats[0], mats[1]), (up_both,)
        )
        mixed, residual, mid, attn_squares = project(
            1, mixed, proj_both, layer_in, params[1:2], params[3:4]
        )
        grad_rows, mid_seq = beside(
            over_homes, packed_rows(own_grad_seq, table), gather_rows, (mid,)
        )
        small_weights = params_all[1, 4:]

        def dispatch_work(mid_seq, small_weights, up_mat):
            return coefficients(mid_seq, small_weights, hot), dense_in(mid_seq, up_mat)

        expert_rows, ((gate_probs, gate, coef), (hidden, hidden_low)) = beside(
            over_homes,
            packed_rows(mid_seq, table),
            dispatch_work,
            (mid_seq, small_weights, up_apart[1]),
        )
        expert_rows = expert_rows.reshape(-1, width)
        scale, exp_hidden, exp_hidden_low, exp_out = expert_forward(
            1, section_id, own_expert, expert_rows, small_weights, exp_up_pair, exp_down_pair
        )
        returned, dense_part = beside(
            over_homes, exp_out.reshape(-1, slots, width), product, (hidden_low, down_apart[1])
        )
        expert_part = product_tn(table, returned.reshape(-1, width))
        branch_part = coef[:, 0:1] * dense_part + coef[:, 1:2] * gate * expert_part
        branch = low(branch_part)
        record = SimpleNamespace(
            params=params,
            small_weights=small_weights,
            table=table,
            hot=hot,
            layer_in=layer_in,
            normed_seq=normed_seq,
            qkv=qkv,
            mixed=mixed,
            residual=residual,
            mid_seq=mid_seq,
            expert_rows=expert_rows,
            scale=scale,
            gate_probs=gate_probs,
            gate=gate,
            coef=coef,
            hidden=hidden,
            hidden_low=hidden_low,
            dense_part=dense_part,
            exp_hidden=exp_hidden,
            exp_hidden_low=exp_hidden_low,
            expert_part=expert_part,
        )
        return branch, attn_squares, record, grad_rows, up_apart

    def over_expert(grad_mat):
        return lax.psum_scatter(grad_mat, EX, scatter_dimension=0, tiled=True)

    def by_rows(grad_mat, count):
        return low(grad_mat).reshape(count, -1, grad_mat.shape[-1])

    def dp_blocks(*grad_mats):
        blocks = [by_rows(grad_mat, dp_size) for grad_mat in grad_mats]
        return own_parts(jnp.concatenate(blocks, axis=2), DP)

    half_hidden, half_width = hidden_here // 2, width // 2

    def backward_layer(layer, grad_low, grad_seq, record, sums_one=(), operands_one=None, settle=(), grad_rows=None):
        params = record.params
        coef, gate, table = record.coef, record.gate, record.table
        def dense_back(grad_seq, coef, down_mat, up_mat, *sums_one):
            grad_seq = grad_seq.astype(jnp.float32)
            early = dp_blocks(*sums_one) if sums_one else ()
            d_dense = low(coef[:, 0:1] * grad_seq)
            dense_dot = jnp.sum(grad_seq * record.dense_part, axis=-1, keepdims=True)
            expert_dot = jnp.sum(grad_seq * record.expert_part, axis=-1, keepdims=True)
            d_coef = jnp.concatenate([dense_dot, gate * expert_dot], axis=1)
            d_mix = coef * (d_coef - jnp.sum(coef * d_coef, axis=-1, keepdims=True))
            d_logits = record.gate_probs * (record.hot - gate) * (coef[:, 1:2] * expert_dot)
            d_small = low(jnp.concatenate([d_logits, d_mix], axis=1))
            d_up = low(gelu_grad(record.hidden, product_nt(d_dense, down_mat)))
            d_mid_part = product_nt(d_up, up_mat) + product(d_small, record.small_weights)
            return d_dense, d_small, d_up, d_mid_part, early

        dense_operands = (grad_seq, coef, down_apart[layer], up_apart[layer])
        if layer == 0:
            grad_rows, dense_grad = beside(
                over_homes,
                packed_rows(grad_seq, table),
                dense_back,
                dense_operands,
                tuple(sums_one),
            )
        expert_grad_rows, d_exp_hidden, expert_back = expert_backward(
            layer,
            section_id,
            grad_rows.reshape(-1, width),
            record.scale,
            record.exp_hidden,
            exp_up_pair,
            exp_down_pair,
        )
        expert_operands = (
            record.expert_rows,
            d_exp_hidden,
            record.exp_hidden_low,
            expert_grad_rows,
        )

        swapped = tuple(other_core(operand) for operand in expert_operands)

        def owner_mats(index):
            return (
                expert_operands[index],
                swapped[index],
                operands_one[0][index],
                operands_one[1][index],
            )

        def dense_grads(hidden_low, d_dense, mid_seq, d_up, d_small):
            g_dense = pair_grads(section_id, (mid_seq, d_up), (hidden_low, d_dense))
            return g_dense, product_tn(d_small, mid_seq)

        expert_back = expert_back.reshape(-1, slots, width)
        parts_one, g_exp_down = (), None
        if layer == 0:
            d_dense, d_small, d_up, d_mid_part, early = dense_grad
            returned, (parts_one, (g_dense, g_small)) = beside(
                over_homes,
                expert_back,
                lambda early, *operands: (sent_parts(early, DP), dense_grads(*operands)),
                (early, record.hidden_low, d_dense, record.mid_seq, d_up, d_small),
            )
            (d_mid_part,) = combine(table, returned.reshape(-1, width), d_mid_part)
            d_mid, (g_exp_down, settle) = beside(
                over_dp,
                row_blocks(d_mid_part),
                lambda left, right, settle: (owner_grads(section_id, left, right), settle),
                (),
                (owner_mats(2), owner_mats(3), settle),
            )
        else:
            returned, dense_grad = beside(
                over_homes,
                expert_back,
                lambda blocks, *operands: dense_back(*started(operands, blocks)),
                (expert_back, *dense_operands),
            )
            d_dense, d_small, d_up, d_mid_part, _ = dense_grad
            d_mid_part = d_mid_part + product_tn(table, returned.reshape(-1, width))
            d_mid, (g_dense, g_small) = beside(
                over_dp,
                row_blocks(d_mid_part),
                dense_grads,
                (record.hidden_low, d_dense, record.mid_seq, d_up, d_small),
            )
        dense_sum = over_expert(g_dense)
        d_resid, d_attn, d_mixed, d_gain_one, d_shift_one = mid_back(
            layer, d_mid, record.residual, params[1:2], grad_low, proj_both, dp_size
        )
        d_mixed = over_dp(d_mixed)

        def attention_grads(d_mixed):
            d_qkv = attention_back(segments, record.qkv, d_mixed.reshape(full_len, head_width))
            return d_qkv, row_blocks(product_nt(d_qkv, qkv_both[layer]))

        d_qkv, in_blocks = attention_grads(d_mixed)
        in_blocks, normed_seq, d_qkv = lax.optimization_barrier(
            (in_blocks, record.normed_seq, d_qkv)
        )
        g_attn = pair_grads(section_id, (record.mixed, d_attn), (normed_seq, d_qkv))
        if layer == 1:
            attn_sum = over_expert(g_attn)
        d_normed, g_attn = lax.optimization_barrier((over_dp(in_blocks), g_attn))
        if layer == 0:
            attn_sum = over_expert(g_attn)
        d_input, d_input_low, d_gain_zero, d_shift_zero = input_back(
            d_normed, record.layer_in, params[0:1], d_resid
        )
        small_grads = (d_gain_zero, d_gain_one, d_shift_zero, d_shift_one, g_small)
        if layer == 0:
            extra = (parts_one, owner_mats, g_exp_down, settle)
        else:
            extra = (expert_operands, swapped)
        return d_input, d_input_low, (dense_sum, attn_sum), small_grads, extra

    own_grad = lax.dynamic_index_in_dim(cotangent[:, 0], section_id, 0, keepdims=False)
    out_zero, next_normed, squares_zero, record_zero, settled = forward_zero()
    qkv_both, down_apart, own_grad_seq = settled
    branch_one, attn_squares_one, record_one, grad_rows, up_apart = forward_one(
        out_zero, next_normed, own_grad_seq
    )
    grad_one, grad_one_low, sums_one, small_one, operands_one = backward_layer(
        1, own_grad, own_grad_seq, record_one, grad_rows=grad_rows
    )
    dense_one, attn_one = sums_one
    branch_one = lax.psum_scatter(
        after(branch_one, grad_one_low), DP, scatter_dimension=0, tiled=True
    )
    grad_zero, _, (dense_zero, attn_zero), small_zero, extra = backward_layer(
        0,
        grad_one_low,
        gather_rows(grad_one_low),
        record_zero,
        (dense_one[:, :half_hidden], attn_one),
        operands_one,
        branch_one,
    )
    parts_one, owner_mats, grad_exp_down, branch_one = extra
    branch_one = branch_one.astype(jnp.float32)
    out_one = record_one.residual + branch_one
    squares_one = jnp.concatenate(
        [attn_squares_one, column_sums(branch_one * branch_one), column_sums(out_one * out_one)]
    )
    out_one = low(out_one)

    moved_one = in_order(after(parts_one, grad_zero), DP)
    small_message = pack_small(
        (small_zero, small_one), (squares_zero, squares_one), weight_rows
    )
    small_moved, grad_exp_up = beside(
        lambda blocks: exchange(blocks, EVERY),
        small_message,
        lambda *mats: owner_grads(section_id, *mats),
        (owner_mats(0), owner_mats(1)),
    )
    up_zero = over_dp(by_rows(after(dense_zero[:, :half_hidden], small_moved), dp_size))

    def of_both(of_zero, of_one):
        return of_zero, other_core(of_zero), of_one, other_core(of_one)

    def last_rows(small_moved, *rows):
        return jnp.sum(small_moved, axis=0), finish_rows(section_id, *rows)

    attn_zero, (small_sum, (activations, input_grads)) = beside(
        over_dp,
        by_rows(after(attn_zero, up_zero), dp_size),
        last_rows,
        (small_moved, of_both(out_zero, out_one), of_both(grad_zero, grad_one)),
    )
    up_one, attn_one = moved_one[..., :half_hidden], moved_one[..., half_hidden:]
    down_zero, down_one = dense_zero[:, half_hidden:], dense_one[:, half_hidden:]

    grad_qkv, grad_proj, grad_up, grad_down = finish_weights(
        section_id,
        of_both(up_zero, up_one),
        of_both(attn_zero, attn_one),
        of_both(down_zero, down_one),
        hidden_rows,
    )
    place = expert_id * dp_size + lax.axis_index(DP)
    sums = lax.dynamic_slice_in_dim(
        small_sum[:small_count], place * weight_rows % LANES, weight_rows, axis=1
    )
    totals = small_sum[small_count, :3]
    element_count = micro_count * seq_rows * width * groups * dp_size
    branch_rms = jnp.sqrt(totals / element_count)[None]
    return (
        activations[None, :, None],
        input_grads[None, :, None],
        sums[None, 0:2],
        sums[None, 2:4],
        grad_qkv[None],
        grad_proj[None],
        grad_up[None],
        grad_down[None],
        sums[4 : 4 + experts_total].T[None],
        sums[4 + experts_total :].T[None],
        grad_exp_up[None],
        grad_exp_down[None],
        branch_rms,
    )


def solution(mesh):
    placed = (
        P(None, EX, DP, None),
        P(None, EX, DP, None),
        P(None, EX, None),
        P(SEC, None, EX, DP, None),
        P(SEC, None, (EX, DP)),
        P(SEC, None, (EX, DP)),
        P(SEC, (EX, DP), None),
        P(SEC, (EX, DP), None),
        P(SEC, (EX, DP), None),
        P(SEC, (EX, DP), None),
        P(SEC, (EX, DP), None),
        P(SEC, (EX, DP), None),
        P(SEC, EX, None, DP),
        P(SEC, EX, DP, None),
    )
    return jax.shard_map(
        shards,
        mesh=mesh,
        in_specs=placed,
        out_specs=(
            P(SEC, None, EX, DP, None),
            P(SEC, None, EX, DP, None),
            P(SEC, None, (EX, DP)),
            P(SEC, None, (EX, DP)),
            P(SEC, (EX, DP), None),
            P(SEC, (EX, DP), None),
            P(SEC, (EX, DP), None),
            P(SEC, (EX, DP), None),
            P(SEC, (EX, DP), None),
            P(SEC, (EX, DP), None),
            P(SEC, EX, None, DP),
            P(SEC, EX, DP, None),
            P(SEC, None),
        ),
        check_vma=False,
    )
```

```python
from types import SimpleNamespace

import jax
import jax.numpy as jnp
from jax import lax
from jax.experimental import pallas as pl
from jax.experimental.pallas import tpu as pltpu
from jax.sharding import PartitionSpec as P

HEADS = 16
HEAD_DIM = 64
SEC, EX, DP = "section", "expert", "dp"
EVERY = (SEC, EX, DP)
HOMES = (SEC, EX)
LANES = 128


def layer_norm(value_rows, gain_vec, shift_vec):
    centre = jnp.mean(value_rows, axis=-1, keepdims=True)
    centred = value_rows - centre
    variance = jnp.mean(centred * centred, axis=-1, keepdims=True)
    return centred * lax.rsqrt(variance + 1e-05) * gain_vec + shift_vec


def gelu_tanh(value_rows):
    return jax.nn.gelu(value_rows, approximate=True)


def gelu_grad(value_rows, grad_in):
    return jax.vjp(gelu_tanh, value_rows)[1](grad_in)[0]


def product(left_mat, right_mat):
    return jnp.dot(left_mat, right_mat, preferred_element_type=jnp.float32)


def product_tn(left_mat, right_mat):
    return lax.dot_general(
        left_mat, right_mat, (((0,), (0,)), ((), ())), preferred_element_type=jnp.float32
    )


def product_nt(left_mat, right_mat):
    return lax.dot_general(
        left_mat, right_mat, (((1,), (1,)), ((), ())), preferred_element_type=jnp.float32
    )


def low(values):
    return values.astype(jnp.bfloat16)


def exchange(blocks, axes):
    return lax.all_to_all(blocks, axes, split_axis=0, concat_axis=0, tiled=True)


def spread(block, axes):
    count = lax.axis_size(axes)
    return exchange(jnp.broadcast_to(block[None], (count,) + block.shape), axes)


def gather_rows(block):
    return lax.all_gather(block, DP, axis=0, tiled=True)


def sum_blocks(blocks):
    return jnp.sum(blocks.astype(jnp.float32), axis=0)


def row_blocks(partial_rows):
    return low(partial_rows).reshape(lax.axis_size(DP), -1, partial_rows.shape[-1])


def beside(move, blocks, work, operands, late=()):
    blocks, operands = lax.optimization_barrier((blocks, operands))
    return lax.optimization_barrier((move(blocks), work(*operands, *late)))


def over_dp(blocks):
    return exchange(blocks, DP)


def over_homes(blocks):
    return exchange(blocks, HOMES)


def after(values, event):
    return lax.optimization_barrier((values, event))[0]


def permute_copies(block, axis):
    count = lax.axis_size(axis)
    blocks = [block]
    for step in range(1, count):
        route = [((i - step) % count, i) for i in range(count)]
        blocks.append(lax.ppermute(block, axis, route))
    return blocks


def own_parts(blocks, axis):
    count = lax.axis_size(axis)
    place = lax.axis_index(axis)
    return [
        lax.dynamic_index_in_dim(blocks, (place + step) % count, 0, keepdims=False)
        for step in range(count)
    ]


def sent_parts(parts, axis):
    count = len(parts)
    return [parts[0]] + [
        lax.ppermute(parts[step], axis, [((i - step) % count, i) for i in range(count)])
        for step in range(1, count)
    ]


def permute_parts(blocks, axis):
    return sent_parts(own_parts(blocks, axis), axis)


SCALAR = pl.BlockSpec(memory_space=pltpu.SMEM)
WHOLE = pl.BlockSpec(memory_space=pltpu.VMEM)


def in_order(blocks, axis):
    count = lax.axis_size(axis)

    def kernel(place, *refs):
        for step in range(count):
            refs[-1][(place[0] + count - step) % count] = refs[step][...]

    return pl.pallas_call(
        kernel,
        out_shape=jax.ShapeDtypeStruct((count,) + blocks[0].shape, blocks[0].dtype),
        in_specs=[SCALAR] + [WHOLE] * count,
        compiler_params=pltpu.CompilerParams(vmem_limit_bytes=32 << 20),
        name="in_order",
    )(lax.axis_index(axis).reshape(1), *blocks)


def finish_weights(section_id, ups, attns, down_sums, hidden_rows):
    dp_size, rows, half_hidden = ups[0].shape
    down_rows, half_width = down_sums[0].shape
    width = 2 * half_width
    head_width = width // dp_size
    qkv_half = 3 * head_width // 2

    def kernel(place, *refs):
        qkv_ref, proj_ref, up_ref, down_ref = refs[12:]

        def write(up_halves, attn_halves, down_halves):
            for half in range(2):
                up, attn = up_halves[half], attn_halves[half]
                here = slice(half * half_width, (half + 1) * half_width)
                proj_sum = attn[0, :, :half_width].astype(jnp.float32)
                for z in range(1, dp_size):
                    proj_sum = proj_sum + attn[z, :, :half_width].astype(jnp.float32)
                proj_ref[:, here] = proj_sum
                down_ref[:, here] = down_halves[half][...].astype(jnp.float32)
                for z in range(dp_size):
                    for piece in range(half_hidden // hidden_rows):
                        group = half * (half_hidden // hidden_rows) + piece
                        start = (group * dp_size + z) * hidden_rows
                        up_ref[:, start : start + hidden_rows] = up[
                            z, :, piece * hidden_rows : (piece + 1) * hidden_rows
                        ].astype(jnp.float32)
                    at = 0
                    while at < qkv_half:
                        column = half * qkv_half + at
                        part, inner = column // head_width, column % head_width
                        size = min(head_width - inner, qkv_half - at)
                        first = half_width + at
                        start = part * width + z * head_width + inner
                        qkv_ref[:, start : start + size] = attn[
                            z, :, first : first + size
                        ].astype(jnp.float32)
                        at = at + size

        @pl.when(place[0] == 0)
        def _():
            write(refs[0:2], refs[4:6], refs[8:10])

        @pl.when(place[0] != 0)
        def _():
            write(refs[3:1:-1], refs[7:5:-1], refs[11:9:-1])

    shapes = ((rows, 3 * width), (rows, width), (rows, 2 * half_hidden * dp_size), (down_rows, width))
    return pl.pallas_call(
        kernel,
        out_shape=[jax.ShapeDtypeStruct(shape, jnp.float32) for shape in shapes],
        in_specs=[SCALAR] + [WHOLE] * 12,
        compiler_params=pltpu.CompilerParams(vmem_limit_bytes=32 << 20),
        name="finish_weights",
    )(section_id.reshape(1), *ups, *attns, *down_sums)


def finish_rows(section_id, *arrays):
    count = len(arrays)

    def kernel(place, *refs):
        outs = refs[4 * count :]
        for index in range(count):
            own_zero, other_zero, own_one, other_one = refs[4 * index : 4 * index + 4]

            @pl.when(place[0] == 0)
            def _():
                outs[index][0] = own_zero[...]
                outs[index][1] = other_zero[...]

            @pl.when(place[0] != 0)
            def _():
                outs[index][0] = other_one[...]
                outs[index][1] = own_one[...]

    return pl.pallas_call(
        kernel,
        out_shape=[
            jax.ShapeDtypeStruct((2,) + array[0].shape, array[0].dtype) for array in arrays
        ],
        in_specs=[SCALAR] + [WHOLE] * (4 * count),
        compiler_params=pltpu.CompilerParams(vmem_limit_bytes=32 << 20),
        name="finish_rows",
    )(section_id.reshape(1), *[rows for array in arrays for rows in array])


def sum_parts(parts):
    return sum(part.astype(jnp.float32) for part in parts)


def softmax_rows(queries, keys, allowed):
    scores = product_nt(queries, keys) * 0.125
    scores = jnp.where(allowed, scores, -jnp.inf)
    exp_scores = jnp.exp(scores - jnp.max(scores, axis=-1, keepdims=True))
    return exp_scores / jnp.sum(exp_scores, axis=-1, keepdims=True)


def allowed_keys(seg_column, seg_row):
    rows, columns = seg_column.shape[0], seg_row.shape[1]
    query_at = lax.broadcasted_iota(jnp.int32, (rows, columns), 0)
    key_at = lax.broadcasted_iota(jnp.int32, (rows, columns), 1)
    return (seg_column == seg_row) & (key_at <= query_at)


def head_slices(packed, head, head_width):
    start = head * HEAD_DIM
    return [
        packed[:, part * head_width + start : part * head_width + start + HEAD_DIM]
        for part in range(3)
    ]


def attention_kernel(seg_column, seg_row, qkv_ref, mixed_ref):
    head_width = mixed_ref.shape[1]
    allowed = allowed_keys(seg_column[...], seg_row[...])
    packed = qkv_ref[...]
    mixed = []
    for head in range(head_width // HEAD_DIM):
        queries, keys, values = head_slices(packed, head, head_width)
        probs = softmax_rows(queries, keys, allowed)
        mixed.append(low(product(low(probs), values)))
    mixed_ref[...] = jnp.concatenate(mixed, axis=1)


def attention_back_kernel(seg_column, seg_row, qkv_ref, d_mixed_ref, d_qkv_ref):
    head_width = d_mixed_ref.shape[1]
    allowed = allowed_keys(seg_column[...], seg_row[...])
    packed = qkv_ref[...]
    d_mixed_all = d_mixed_ref[...]
    grads = [[], [], []]
    for head in range(head_width // HEAD_DIM):
        queries, keys, values = head_slices(packed, head, head_width)
        d_mixed = d_mixed_all[:, head * HEAD_DIM : (head + 1) * HEAD_DIM]
        probs = softmax_rows(queries, keys, allowed)
        d_probs = product_nt(d_mixed, values)
        d_scores = low(probs * (d_probs - jnp.sum(probs * d_probs, axis=-1, keepdims=True)))
        grads[0].append(low(product(d_scores, keys) * 0.125))
        grads[1].append(low(product_tn(d_scores, queries) * 0.125))
        grads[2].append(low(product_tn(low(probs), d_mixed)))
    d_qkv_ref[...] = jnp.concatenate(grads[0] + grads[1] + grads[2], axis=1)


def attention(segments, qkv):
    head_width = qkv.shape[1] // 3
    return pl.pallas_call(
        attention_kernel,
        out_shape=jax.ShapeDtypeStruct((qkv.shape[0], head_width), jnp.bfloat16),
        compiler_params=pltpu.CompilerParams(vmem_limit_bytes=32 << 20),
        name="attention",
    )(segments[:, None], segments[None, :], qkv)


def attention_back(segments, qkv, d_mixed):
    return pl.pallas_call(
        attention_back_kernel,
        out_shape=jax.ShapeDtypeStruct(qkv.shape, jnp.bfloat16),
        compiler_params=pltpu.CompilerParams(vmem_limit_bytes=32 << 20),
        name="attention_back",
    )(segments[:, None], segments[None, :], qkv, d_mixed)


IN_HBM = pl.BlockSpec(memory_space=pltpu.HBM)


def in_hbm(mat):
    return pltpu.with_memory_space_constraint(mat, pltpu.HBM)


def expert_call(kernel, name, outs, section_id, operands, up_pair, down_pair, extra=()):
    width, hidden = up_pair[0].shape
    half = hidden // 2
    return pl.pallas_call(
        kernel,
        out_shape=[pltpu.HBM(shape, dtype) for shape, dtype in outs],
        out_specs=[WHOLE for _ in outs],
        in_specs=[SCALAR] + [WHOLE] * len(operands) + [IN_HBM] * (4 + len(extra)),
        scratch_shapes=[
            pltpu.VMEM((2, width, half), jnp.bfloat16),
            pltpu.VMEM((2, half, width), jnp.bfloat16),
            pltpu.SemaphoreType.DMA((2, 2)),
        ]
        + [pltpu.VMEM((2, mat.shape[0], half), mat.dtype) for mat in extra]
        + [pltpu.SemaphoreType.DMA((2,)) for _ in extra],
        compiler_params=pltpu.CompilerParams(vmem_limit_bytes=40 << 20),
        name=name,
    )(section_id.reshape(1), *operands, *[in_hbm(mat) for mat in (*up_pair, *down_pair, *extra)])


def expert_weights_in(layer, place, sources, up_here, down_here, arrived):
    half = up_here.shape[2]

    def copies(which, part):
        columns = pl.ds(part * half, half)
        return (
            pltpu.make_async_copy(
                sources[which].at[:, columns], up_here.at[part], arrived.at[0, part]
            ),
            pltpu.make_async_copy(
                sources[2 + which].at[columns], down_here.at[part], arrived.at[1, part]
            ),
        )

    for which in range(2):

        @pl.when((place[0] == layer) if which == 0 else (place[0] != layer))
        def _():
            for part in range(2):
                for copy in copies(which, part):
                    copy.start()

    return [copies(0, part) for part in range(2)]


def combine(table, returned, base, weight=None):
    def kernel(table_ref, returned_ref, base_ref, *refs):
        expert_part = product_tn(table_ref[...], returned_ref[...])
        if weight is None:
            refs[-1][...] = low(base_ref[...] + expert_part)
        else:
            refs[-2][...] = expert_part
            weights = refs[0][...]
            refs[-1][...] = low(weights[:, 0:1] * base_ref[...] + weights[:, 1:2] * expert_part)

    shape = (table.shape[1], returned.shape[1])
    outs = [jax.ShapeDtypeStruct(shape, jnp.bfloat16)]
    if weight is not None:
        outs = [jax.ShapeDtypeStruct(shape, jnp.float32)] + outs
    return pl.pallas_call(
        kernel,
        out_shape=outs,
        compiler_params=pltpu.CompilerParams(vmem_limit_bytes=32 << 20),
        name="combine",
    )(table, returned, base, *(() if weight is None else (weight,)))


def row_scales(logits, expert):
    lane = lax.broadcasted_iota(jnp.int32, logits.shape, 1)
    experts = logits.shape[1] - 2

    def share(among, one):
        chosen = jnp.where(among, logits, -jnp.inf)
        weights = jnp.exp(chosen - jnp.max(chosen, axis=1, keepdims=True))
        part = jnp.sum(jnp.where(one, weights, 0.0), axis=1, keepdims=True)
        return part / jnp.sum(weights, axis=1, keepdims=True)

    return share(lane >= experts, lane == experts + 1) * share(lane < experts, lane == expert)


def expert_forward(layer, section_id, expert, rows, small_weights, up_pair, down_pair):
    def kernel(place, expert_ref, rows_ref, small_ref, *refs):
        scale_ref, hidden_ref, low_ref, part_ref, up_here, down_here, arrived = refs[4:]
        waits = expert_weights_in(layer, place, refs[:4], up_here, down_here, arrived)
        scale_ref[...] = row_scales(product_nt(rows_ref[...], small_ref[...]), expert_ref[0, 0])
        half = up_here.shape[2]
        total = None
        for part in range(2):
            here = slice(part * half, (part + 1) * half)
            waits[part][0].wait()
            hidden = product(rows_ref[...], up_here[part])
            hidden_ref[:, here] = hidden
            hidden_low = low(gelu_tanh(hidden))
            low_ref[:, here] = hidden_low
            waits[part][1].wait()
            added = product(hidden_low, down_here[part])
            total = added if total is None else total + added
        part_ref[...] = low(total)

    count, width = rows.shape
    hidden = up_pair[0].shape[1]
    outs = [((count, 1), jnp.float32), ((count, hidden), jnp.float32)]
    outs += [((count, hidden), jnp.bfloat16), ((count, width), jnp.bfloat16)]
    return expert_call(
        kernel,
        "expert_forward",
        outs,
        section_id,
        (expert.reshape(1, 1), rows, small_weights),
        up_pair,
        down_pair,
    )


def expert_backward(layer, section_id, grad_rows, scale, hidden, up_pair, down_pair):
    def kernel(place, rows_ref, scale_ref, *refs):
        scaled_ref, d_hidden_ref, back_ref, up_here, down_here, arrived = refs[5:11]
        hidden_here, hidden_arrived = refs[11:]
        waits = expert_weights_in(layer, place, refs[:4], up_here, down_here, arrived)
        half = up_here.shape[2]
        fetches = [
            pltpu.make_async_copy(
                refs[4].at[:, pl.ds(part * half, half)], hidden_here.at[part], hidden_arrived.at[part]
            )
            for part in range(2)
        ]
        for fetch in fetches:
            fetch.start()
        scaled = low(scale_ref[...] * rows_ref[...].astype(jnp.float32))
        scaled_ref[...] = scaled
        total = None
        for part in range(2):
            here = slice(part * half, (part + 1) * half)
            waits[part][1].wait()
            d_low = product_nt(scaled, down_here[part])
            fetches[part].wait()
            d_hidden = low(gelu_grad(hidden_here[part], d_low))
            d_hidden_ref[:, here] = d_hidden
            waits[part][0].wait()
            added = product_nt(d_hidden, up_here[part])
            total = added if total is None else total + added
        back_ref[...] = low(total)

    shape = ((grad_rows.shape), jnp.bfloat16)
    outs = [shape, (hidden.shape, jnp.bfloat16), shape]
    return expert_call(
        kernel,
        "expert_backward",
        outs,
        section_id,
        (grad_rows, scale),
        up_pair,
        down_pair,
        (hidden,),
    )


def pair_grads(section_id, *pairs):
    mats = [side for left, right in pairs for side in (left, other_core(left), right, other_core(right))]
    left_width = pairs[0][0].shape[1]
    halves = [right.shape[1] // 2 for _, right in pairs]

    def kernel(place, *refs):
        start = 0
        for index, half in enumerate(halves):
            left_own, left_other, right_own, right_other = refs[4 * index : 4 * index + 4]
            here = pl.ds(pl.multiple_of(place[0] * half, LANES), half)
            total = product_tn(left_own[...], right_own[:, here])
            total = total + product_tn(left_other[...], right_other[:, here])
            refs[-1][:, start : start + half] = low(total)
            start = start + half

    return pl.pallas_call(
        kernel,
        out_shape=jax.ShapeDtypeStruct((left_width, sum(halves)), jnp.bfloat16),
        in_specs=[SCALAR] + [WHOLE] * len(mats),
        compiler_params=pltpu.CompilerParams(vmem_limit_bytes=40 << 20),
        name="pair_grads",
    )(section_id.reshape(1), *mats)


OWNER_TILE = 512


def owner_grads(section_id, left_mats, right_mats):
    rows, left_width = left_mats[0].shape
    right_width = right_mats[0].shape[1]
    tiles = left_width // OWNER_TILE

    def kernel(place, *refs):
        out_ref, left_here, right_here, arrived = refs[8:]
        expert, tile = pl.program_id(0), pl.program_id(1)

        def copies(source, slot):
            return (
                pltpu.make_async_copy(refs[source], left_here.at[slot], arrived.at[0, slot]),
                pltpu.make_async_copy(refs[4 + source], right_here.at[slot], arrived.at[1, slot]),
            )

        for first, sources in ((True, (0, 1)), (False, (3, 2))):
            here = (place[0] == 0) if first else (place[0] != 0)

            @pl.when(here & (expert == 0) & (tile == 0))
            def _():
                for slot, source in enumerate(sources):
                    for copy in copies(source, slot):
                        copy.start()

        @pl.when(tile == 0)
        def _():
            for copy in copies(0, expert):
                copy.wait()

        left = left_here[expert, :, pl.ds(tile * OWNER_TILE, OWNER_TILE)]
        out_ref[0] = product_tn(left, right_here[expert])

    return pl.pallas_call(
        kernel,
        out_shape=jax.ShapeDtypeStruct((2, left_width, right_width), jnp.float32),
        grid=(2, tiles),
        in_specs=[SCALAR] + [IN_HBM, WHOLE] * 4,
        out_specs=pl.BlockSpec((1, OWNER_TILE, right_width), lambda expert, tile: (expert, tile, 0)),
        scratch_shapes=[
            pltpu.VMEM((2, rows, left_width), jnp.bfloat16),
            pltpu.VMEM((2, rows, right_width), jnp.bfloat16),
            pltpu.SemaphoreType.DMA((2, 2)),
        ],
        compiler_params=pltpu.CompilerParams(vmem_limit_bytes=40 << 20),
        name="owner_grads",
    )(
        section_id.reshape(1),
        *[
            mat if index % 2 else in_hbm(mat)
            for index, mat in enumerate((*left_mats, *right_mats))
        ],
    )


def statistics(value_rows):
    centre = jnp.mean(value_rows, axis=-1, keepdims=True)
    centred = value_rows - centre
    variance = jnp.mean(centred * centred, axis=-1, keepdims=True)
    spread_inverse = lax.rsqrt(variance + 1e-05)
    return centred * spread_inverse, spread_inverse


def column_sums(value_rows):
    return jnp.sum(value_rows, axis=0, keepdims=True)


def block_sum(blocks_ref):
    total = blocks_ref[0].astype(jnp.float32)
    for place in range(1, blocks_ref.shape[0]):
        total = total + blocks_ref[place].astype(jnp.float32)
    return total


def call(kernel, name, outs, *operands):
    specs = [
        pl.BlockSpec(memory_space=pltpu.HBM)
        if operand.shape[1:] == (operand.shape[-1],) * 2
        else WHOLE
        for operand in operands
    ]
    operands = [
        operand if spec is WHOLE else pltpu.with_memory_space_constraint(operand, pltpu.HBM)
        for operand, spec in zip(operands, specs)
    ]
    mats = [operand.shape[1:] for operand, spec in zip(operands, specs) if spec is not WHOLE]
    scratch = [pltpu.VMEM(shape, jnp.bfloat16) for shape in mats]
    scratch += [pltpu.SemaphoreType.DMA for _ in mats]
    return pl.pallas_call(
        kernel,
        in_specs=specs,
        out_shape=[jax.ShapeDtypeStruct(shape, dtype) for shape, dtype in outs],
        scratch_shapes=scratch,
        compiler_params=pltpu.CompilerParams(vmem_limit_bytes=32 << 20),
        name=name,
    )(*operands)


def project(layer, mixed_blocks, proj_mat, layer_in, gain, shift):
    def kernel(mixed_ref, proj_ref, in_ref, gain_ref, shift_ref, *outs):
        rows_ref, res_ref, mid_ref, sq_ref, proj_here, arrived = outs
        fetch = pltpu.make_async_copy(proj_ref.at[layer], proj_here, arrived)
        fetch.start()
        places = mixed_ref.shape[0]
        mixed = jnp.concatenate([mixed_ref[place] for place in range(places)], axis=1)
        rows_ref[...] = mixed
        fetch.wait()
        branch = product(mixed, proj_here[...])
        residual = in_ref[...].astype(jnp.float32) + branch
        res_ref[...] = residual
        mid_ref[...] = low(statistics(residual)[0] * gain_ref[...] + shift_ref[...])
        sq_ref[...] = column_sums(branch * branch)

    rows, width = layer_in.shape
    outs = [((rows, width), jnp.bfloat16), ((rows, width), jnp.float32)]
    outs += [((rows, width), jnp.bfloat16), ((1, width), jnp.float32)]
    return call(kernel, "project", outs, mixed_blocks, proj_mat, layer_in, gain, shift)


def layer_end(branch_blocks, residual, gain, shift):
    def kernel(blocks_ref, res_ref, gain_ref, shift_ref, out_ref, normed_ref, sq_ref):
        branch = block_sum(blocks_ref)
        layer_out = res_ref[...] + branch
        rounded = low(layer_out)
        out_ref[...] = rounded
        normed = statistics(rounded.astype(jnp.float32))[0]
        normed_ref[...] = low(normed * gain_ref[...] + shift_ref[...])
        sq_ref[0:1] = column_sums(branch * branch)
        sq_ref[1:2] = column_sums(layer_out * layer_out)

    shape = residual.shape
    outs = [(shape, jnp.bfloat16), (shape, jnp.bfloat16), ((2, shape[1]), jnp.float32)]
    return call(kernel, "layer_end", outs, branch_blocks, residual, gain, shift)


def norm_back(blocks_ref, value_ref, gain_ref, grad_ref, gain_grad_ref, shift_grad_ref):
    d_normed = block_sum(blocks_ref)
    normed, spread_inverse = statistics(value_ref[...].astype(jnp.float32))
    gain_grad_ref[...] = column_sums(d_normed * normed)
    shift_grad_ref[...] = column_sums(d_normed)
    d_centred = d_normed * gain_ref[...]
    along = jnp.mean(d_centred * normed, axis=-1, keepdims=True)
    d_value = d_centred - jnp.mean(d_centred, axis=-1, keepdims=True) - normed * along
    return grad_ref[...].astype(jnp.float32) + d_value * spread_inverse


def mid_back(layer, mid_blocks, residual, gain, grad_out, proj_mat, dp_size):
    def kernel(blocks_ref, res_ref, gain_ref, grad_ref, proj_ref, *outs):
        sum_ref, low_ref, mixed_ref, gain_grad_ref, shift_grad_ref, proj_here, arrived = outs
        fetch = pltpu.make_async_copy(proj_ref.at[layer], proj_here, arrived)
        fetch.start()
        grad = norm_back(blocks_ref, res_ref, gain_ref, grad_ref, gain_grad_ref, shift_grad_ref)
        sum_ref[...] = grad
        low_ref[...] = low(grad)
        fetch.wait()
        d_mixed = low(product_nt(low(grad), proj_here[...]))
        part = d_mixed.shape[1] // dp_size
        for place in range(dp_size):
            mixed_ref[place] = d_mixed[:, place * part : (place + 1) * part]

    rows, width = residual.shape
    row = ((1, width), jnp.float32)
    outs = [((rows, width), jnp.float32), ((rows, width), jnp.bfloat16)]
    outs += [((dp_size, rows, width // dp_size), jnp.bfloat16), row, row]
    return call(kernel, "mid_back", outs, mid_blocks, residual, gain, grad_out, proj_mat)


def input_back(in_blocks, layer_in, gain, grad_resid):
    def kernel(blocks_ref, in_ref, gain_ref, grad_ref, sum_ref, low_ref, gain_grad_ref, shift_grad_ref):
        grad = norm_back(blocks_ref, in_ref, gain_ref, grad_ref, gain_grad_ref, shift_grad_ref)
        sum_ref[...] = grad
        low_ref[...] = low(grad)

    shape = layer_in.shape
    row = ((1, shape[1]), jnp.float32)
    outs = [(shape, jnp.float32), (shape, jnp.bfloat16), row, row]
    return call(kernel, "input_back", outs, in_blocks, layer_in, gain, grad_resid)


def pack_small(parts_of_layers, squares_of_layers, weight_rows):
    layers = len(parts_of_layers)
    flat = [part for parts in parts_of_layers for part in parts] + list(squares_of_layers)
    width = flat[0].shape[1]
    used = sum(part.shape[0] for part in parts_of_layers[0])
    height = -(-(used + 1) // 8) * 8
    places = width // weight_rows

    def kernel(*refs):
        out_ref, rows_ref = refs[-2], refs[-1]
        per_layer = len(parts_of_layers[0])
        for layer in range(layers):
            rows_ref[...] = jnp.zeros(rows_ref.shape, jnp.float32)
            start = 0
            for part in refs[layer * per_layer : (layer + 1) * per_layer]:
                rows_ref[start : start + part.shape[0]] = part[...]
                start = start + part.shape[0]
            lane = lax.broadcasted_iota(jnp.int32, (1, width), 1) % LANES
            marked = jnp.zeros((1, width), jnp.float32)
            sums = jnp.sum(refs[layers * per_layer + layer][...], axis=1, keepdims=True)
            for kind in range(3):
                marked = jnp.where(lane == kind, sums[kind : kind + 1], marked)
            rows_ref[start : start + 1] = marked
            for place in range(places):
                column = place * weight_rows // LANES * LANES
                out_ref[layer * places + place] = rows_ref[:, column : column + LANES]

    return pl.pallas_call(
        kernel,
        out_shape=jax.ShapeDtypeStruct((layers * places, height, LANES), jnp.float32),
        scratch_shapes=[pltpu.VMEM((height, width), jnp.float32)],
        name="pack_small",
    )(*flat)


def other_core(block):
    return lax.ppermute(block, SEC, [(0, 1), (1, 0)])


def shards(
    inputs,
    cotangent,
    segment_ids,
    routes,
    norm_gains,
    norm_shifts,
    attn_qkv,
    attn_proj,
    dense_up,
    dense_down,
    router,
    mixer,
    expert_up,
    expert_down,
):
    sections = lax.axis_size(SEC)
    groups = lax.axis_size(EX)
    dp_size = lax.axis_size(DP)
    section_id = lax.axis_index(SEC)
    expert_id = lax.axis_index(EX)
    micro_count = inputs.shape[0]
    seq_rows = inputs.shape[2]
    width = inputs.shape[3]
    full_len = segment_ids.shape[2]
    experts_total = router.shape[2]
    hidden_rows = dense_down.shape[1]
    weight_rows = attn_qkv.shape[1]
    heads_here = HEADS // dp_size
    head_width = heads_here * HEAD_DIM
    capacity = max(2, 5 * seq_rows // (4 * experts_total))
    slots = dp_size * capacity
    devices = sections * groups * dp_size

    small_parts = jnp.concatenate([norm_gains[0], norm_shifts[0], router[0].T, mixer[0].T], axis=0)
    small_count = small_parts.shape[0]
    route_row = low(routes[0, :, 0, :, 0])
    message = jnp.concatenate([small_parts.reshape(-1), route_row.reshape(-1)])
    filled = message.shape[0]
    padded = -(-filled // 1024) * 1024
    message = jnp.pad(message, (0, padded - filled)).reshape(padded // 128, 128)

    def expert_parts(*own_layers):
        return [
            (
                lax.dynamic_index_in_dim(own_layer, section_id, 0, keepdims=False),
                lax.dynamic_index_in_dim(own_layer, 1 - section_id, 0, keepdims=False),
            )
            for own_layer in own_layers
        ]

    hidden_here = groups * hidden_rows
    small_all, (proj_rows, up_parts) = beside(
        lambda blocks: exchange(blocks, EVERY),
        jnp.broadcast_to(message[None], (devices,) + message.shape),
        lambda proj_shard, up_cols: (
            in_order(permute_copies(proj_shard, DP), DP),
            own_parts(
                up_cols.reshape(weight_rows, groups, dp_size, hidden_rows)
                .transpose(2, 0, 1, 3)
                .reshape(dp_size, weight_rows, hidden_here),
                DP,
            ),
        ),
        (attn_proj[0], dense_up[0]),
    )
    small_all = small_all.reshape(sections, groups, dp_size, padded)

    def params_of(small_all):
        params_all = small_all[..., : small_count * weight_rows].reshape(
            sections, groups * dp_size, small_count, weight_rows
        )
        return params_all.transpose(0, 2, 1, 3).reshape(sections, small_count, width)

    def routes_of(small_all):
        routes_all = lax.dynamic_index_in_dim(
            small_all[..., small_count * weight_rows : filled], expert_id, 1, keepdims=False
        ).reshape(sections, dp_size, micro_count, seq_rows)
        routes_all = lax.dynamic_index_in_dim(routes_all, section_id, 2, keepdims=False)
        return routes_all.astype(jnp.int32)

    on_first = section_id == 0

    def by_layer(pair):
        of_own_layer, of_other_layer = pair
        return (
            jnp.where(on_first, of_own_layer, of_other_layer),
            jnp.where(on_first, of_other_layer, of_own_layer),
        )

    proj_both = lax.all_gather(proj_rows.reshape(-1, width), HOMES, axis=0, tiled=True)
    proj_both = proj_both.reshape(sections, width, width)
    qkv_cols = attn_qkv[0].reshape(weight_rows, 3, dp_size, head_width).transpose(2, 0, 1, 3)
    qkv_cols, small_all = lax.optimization_barrier(
        (qkv_cols.reshape(dp_size, weight_rows, 3 * head_width), small_all)
    )
    qkv_cols, expert_weights = beside(
        over_dp, qkv_cols, expert_parts, (expert_up[0], expert_down[0])
    )
    params_all = params_of(small_all)
    routes_all = routes_of(small_all)
    own_input = lax.dynamic_index_in_dim(inputs[:, 0], section_id, 0, keepdims=False)
    first_params = params_all[0].astype(jnp.float32)
    first_normed = low(
        layer_norm(own_input.astype(jnp.float32), first_params[0:1], first_params[2:3])
    )
    down_both = lax.all_gather(dense_down[0], HOMES, axis=0, tiled=True)
    qkv_own, (first_seq, up_rows, down_both) = beside(
        lambda blocks: exchange(blocks, EX),
        jnp.broadcast_to(qkv_cols[None], (groups,) + qkv_cols.shape),
        lambda rows, parts, down_both: (
            in_order(permute_copies(rows, DP), DP),
            in_order(sent_parts(parts, DP), DP),
            down_both,
        ),
        (first_normed, up_parts),
        (down_both,),
    )
    first_seq = first_seq.reshape(full_len, width)
    qkv_own = qkv_own.reshape(width, 3 * head_width)
    qkv_pair = (qkv_own, other_core(qkv_own))
    exp_up_pair, exp_down_pair = [(kept, other_core(sent)) for kept, sent in expert_weights]
    first_qkv = low(product(first_seq, by_layer(qkv_pair)[0]))
    up_both = lax.all_gather(up_rows.reshape(-1, hidden_here), HOMES, axis=0, tiled=True)
    up_both = up_both.reshape(sections, width, hidden_here)
    down_both = down_both.reshape(sections, hidden_here, width)

    segments = lax.dynamic_index_in_dim(segment_ids[:, 0], section_id, 0, keepdims=False)
    places = jnp.arange(full_len, dtype=jnp.int32)
    earlier = (places[None, :] < places[:, None]) & (
        places[None, :] // seq_rows == places[:, None] // seq_rows
    )

    def slot_table(route_now):
        rank = jnp.sum(
            ((route_now[:, None] == route_now[None, :]) & earlier).astype(jnp.int32), axis=1
        )
        home = route_now % sections * groups + route_now // sections
        target = home * slots + places // seq_rows * capacity + rank
        slot_ids = jnp.arange(sections * groups * slots, dtype=jnp.int32)
        table = low(slot_ids[:, None] == target[None, :])
        hot = route_now[:, None] == jnp.arange(experts_total, dtype=jnp.int32)[None, :]
        return table, hot.astype(jnp.float32)

    def packed_rows(token_rows, table):
        return low(product(table, token_rows)).reshape(sections * groups, slots, width)

    def coefficients(mid_seq, small_weights, hot):
        small_logits = product_nt(mid_seq, small_weights)
        gate_probs = jax.nn.softmax(small_logits[:, :experts_total], axis=-1)
        gate = jnp.sum(gate_probs * hot, axis=-1, keepdims=True)
        coef = jax.nn.softmax(small_logits[:, experts_total:], axis=-1)
        return gate_probs, gate, coef

    own_expert = expert_id * sections + section_id

    def dense_in(mid_seq, up_mat):
        hidden = product(mid_seq, up_mat)
        return hidden, low(gelu_tanh(hidden))

    def attended(qkv):
        return attention(segments, qkv).reshape(dp_size, seq_rows, head_width)

    def forward_zero():
        params = first_params
        table, hot = slot_table(routes_all[0].reshape(full_len))
        mixed, residual, mid, attn_squares = project(
            0, over_dp(attended(first_qkv)), proj_both, own_input, params[1:2], params[3:4]
        )
        mid_seq = gather_rows(mid)
        small_weights = params_all[0, 4:]

        expert_blocks = packed_rows(mid_seq, table)
        expert_rows, ((gate_probs, gate, coef), own_grad_seq) = beside(
            over_homes,
            expert_blocks,
            lambda mid_seq, small_weights, grad: (
                coefficients(mid_seq, small_weights, hot),
                in_order(permute_copies(grad, DP), DP).reshape(full_len, width),
            ),
            (mid_seq, small_weights, own_grad),
        )
        expert_rows = expert_rows.reshape(-1, width)
        scale, exp_hidden, exp_hidden_low, exp_out = expert_forward(
            0, section_id, own_expert, expert_rows, small_weights, exp_up_pair, exp_down_pair
        )

        def return_work(mid_seq, up_mat, down_mat):
            hidden, hidden_low = dense_in(mid_seq, up_mat)
            return hidden, hidden_low, product(hidden_low, down_mat)

        returned, (hidden, hidden_low, dense_part) = beside(
            over_homes,
            exp_out.reshape(-1, slots, width),
            return_work,
            (mid_seq,),
            (up_both[0], down_both[0]),
        )
        expert_part = product_tn(table, returned.reshape(-1, width))
        branch_part = coef[:, 0:1] * dense_part + coef[:, 1:2] * gate * expert_part
        branch, settled = beside(
            over_dp,
            row_blocks(branch_part),
            lambda qkv_pair, down_both: (by_layer(qkv_pair), (down_both[0], down_both[1])),
            (qkv_pair, down_both),
        )
        next_params = params_all[1].astype(jnp.float32)
        out_low, next_normed, squares = layer_end(
            branch, residual, next_params[0:1], next_params[2:3]
        )
        record = SimpleNamespace(
            params=params,
            small_weights=small_weights,
            table=table,
            hot=hot,
            layer_in=own_input,
            normed_seq=first_seq,
            qkv=first_qkv,
            mixed=mixed,
            residual=residual,
            mid_seq=mid_seq,
            expert_rows=expert_rows,
            scale=scale,
            gate_probs=gate_probs,
            gate=gate,
            coef=coef,
            hidden=hidden,
            hidden_low=hidden_low,
            dense_part=dense_part,
            exp_hidden=exp_hidden,
            exp_hidden_low=exp_hidden_low,
            expert_part=expert_part,
        )
        squares = jnp.concatenate([attn_squares, squares], axis=0)
        return out_low, next_normed, squares, record, (*settled, own_grad_seq)

    def forward_one(layer_in, normed, own_grad_seq):
        params = params_all[1].astype(jnp.float32)
        table, hot = slot_table(routes_all[1].reshape(full_len))
        normed_seq = gather_rows(normed)
        qkv = low(product(normed_seq, qkv_both[1]))
        mixed, up_apart = beside(
            over_dp, attended(qkv), lambda mats: (mats[0], mats[1]), (up_both,)
        )
        mixed, residual, mid, attn_squares = project(
            1, mixed, proj_both, layer_in, params[1:2], params[3:4]
        )
        grad_rows, mid_seq = beside(
            over_homes, packed_rows(own_grad_seq, table), gather_rows, (mid,)
        )
        small_weights = params_all[1, 4:]

        def dispatch_work(mid_seq, small_weights, up_mat):
            return coefficients(mid_seq, small_weights, hot), dense_in(mid_seq, up_mat)

        expert_rows, ((gate_probs, gate, coef), (hidden, hidden_low)) = beside(
            over_homes,
            packed_rows(mid_seq, table),
            dispatch_work,
            (mid_seq, small_weights, up_apart[1]),
        )
        expert_rows = expert_rows.reshape(-1, width)
        scale, exp_hidden, exp_hidden_low, exp_out = expert_forward(
            1, section_id, own_expert, expert_rows, small_weights, exp_up_pair, exp_down_pair
        )
        returned, dense_part = beside(
            over_homes, exp_out.reshape(-1, slots, width), product, (hidden_low, down_apart[1])
        )
        expert_part = product_tn(table, returned.reshape(-1, width))
        branch_part = coef[:, 0:1] * dense_part + coef[:, 1:2] * gate * expert_part
        branch = low(branch_part)
        record = SimpleNamespace(
            params=params,
            small_weights=small_weights,
            table=table,
            hot=hot,
            layer_in=layer_in,
            normed_seq=normed_seq,
            qkv=qkv,
            mixed=mixed,
            residual=residual,
            mid_seq=mid_seq,
            expert_rows=expert_rows,
            scale=scale,
            gate_probs=gate_probs,
            gate=gate,
            coef=coef,
            hidden=hidden,
            hidden_low=hidden_low,
            dense_part=dense_part,
            exp_hidden=exp_hidden,
            exp_hidden_low=exp_hidden_low,
            expert_part=expert_part,
        )
        return branch, attn_squares, record, grad_rows, up_apart

    def over_expert(grad_mat):
        return lax.psum_scatter(grad_mat, EX, scatter_dimension=0, tiled=True)

    def by_rows(grad_mat, count):
        return low(grad_mat).reshape(count, -1, grad_mat.shape[-1])

    def dp_blocks(*grad_mats):
        blocks = [by_rows(grad_mat, dp_size) for grad_mat in grad_mats]
        return own_parts(jnp.concatenate(blocks, axis=2), DP)

    half_hidden, half_width = hidden_here // 2, width // 2

    def backward_layer(layer, grad_low, grad_seq, record, sums_one=(), operands_one=None, settle=(), grad_rows=None):
        params = record.params
        coef, gate, table = record.coef, record.gate, record.table
        def dense_back(grad_seq, coef, down_mat, up_mat, *sums_one):
            grad_seq = grad_seq.astype(jnp.float32)
            early = dp_blocks(*sums_one) if sums_one else ()
            d_dense = low(coef[:, 0:1] * grad_seq)
            dense_dot = jnp.sum(grad_seq * record.dense_part, axis=-1, keepdims=True)
            expert_dot = jnp.sum(grad_seq * record.expert_part, axis=-1, keepdims=True)
            d_coef = jnp.concatenate([dense_dot, gate * expert_dot], axis=1)
            d_mix = coef * (d_coef - jnp.sum(coef * d_coef, axis=-1, keepdims=True))
            d_logits = record.gate_probs * (record.hot - gate) * (coef[:, 1:2] * expert_dot)
            d_small = low(jnp.concatenate([d_logits, d_mix], axis=1))
            d_up = low(gelu_grad(record.hidden, product_nt(d_dense, down_mat)))
            d_mid_part = product_nt(d_up, up_mat) + product(d_small, record.small_weights)
            return d_dense, d_small, d_up, d_mid_part, early

        dense_operands = (grad_seq, coef, down_apart[layer], up_apart[layer])
        if layer == 0:
            grad_rows, dense_grad = beside(
                over_homes,
                packed_rows(grad_seq, table),
                dense_back,
                dense_operands,
                tuple(sums_one),
            )
        expert_grad_rows, d_exp_hidden, expert_back = expert_backward(
            layer,
            section_id,
            grad_rows.reshape(-1, width),
            record.scale,
            record.exp_hidden,
            exp_up_pair,
            exp_down_pair,
        )
        expert_operands = (
            record.expert_rows,
            d_exp_hidden,
            record.exp_hidden_low,
            expert_grad_rows,
        )

        swapped = tuple(other_core(operand) for operand in expert_operands)

        def owner_mats(index):
            return (
                expert_operands[index],
                swapped[index],
                operands_one[0][index],
                operands_one[1][index],
            )

        def dense_grads(hidden_low, d_dense, mid_seq, d_up, d_small):
            g_dense = pair_grads(section_id, (mid_seq, d_up), (hidden_low, d_dense))
            return g_dense, product_tn(d_small, mid_seq)

        expert_back = expert_back.reshape(-1, slots, width)
        parts_one, g_exp_down = (), None
        if layer == 0:
            d_dense, d_small, d_up, d_mid_part, early = dense_grad
            returned, (parts_one, (g_dense, g_small)) = beside(
                over_homes,
                expert_back,
                lambda early, *operands: (sent_parts(early, DP), dense_grads(*operands)),
                (early, record.hidden_low, d_dense, record.mid_seq, d_up, d_small),
            )
            (d_mid_part,) = combine(table, returned.reshape(-1, width), d_mid_part)
            d_mid, (g_exp_down, settle) = beside(
                over_dp,
                row_blocks(d_mid_part),
                lambda left, right, settle: (owner_grads(section_id, left, right), settle),
                (),
                (owner_mats(2), owner_mats(3), settle),
            )
        else:
            returned, dense_grad = beside(
                over_homes,
                expert_back,
                dense_back,
                dense_operands,
            )
            d_dense, d_small, d_up, d_mid_part, _ = dense_grad
            d_mid_part = d_mid_part + product_tn(table, returned.reshape(-1, width))
            d_mid, (g_dense, g_small) = beside(
                over_dp,
                row_blocks(d_mid_part),
                dense_grads,
                (record.hidden_low, d_dense, record.mid_seq, d_up, d_small),
            )
        dense_sum = over_expert(g_dense)
        d_resid, d_attn, d_mixed, d_gain_one, d_shift_one = mid_back(
            layer, d_mid, record.residual, params[1:2], grad_low, proj_both, dp_size
        )
        d_mixed = over_dp(d_mixed)

        def attention_grads(d_mixed):
            d_qkv = attention_back(segments, record.qkv, d_mixed.reshape(full_len, head_width))
            return d_qkv, row_blocks(product_nt(d_qkv, qkv_both[layer]))

        d_qkv, in_blocks = attention_grads(d_mixed)
        in_blocks, normed_seq, d_qkv = lax.optimization_barrier(
            (in_blocks, record.normed_seq, d_qkv)
        )
        g_attn = pair_grads(section_id, (record.mixed, d_attn), (normed_seq, d_qkv))
        if layer == 1:
            attn_sum = over_expert(g_attn)
        d_normed, g_attn = lax.optimization_barrier((over_dp(in_blocks), g_attn))
        if layer == 0:
            attn_sum = over_expert(g_attn)
        d_input, d_input_low, d_gain_zero, d_shift_zero = input_back(
            d_normed, record.layer_in, params[0:1], d_resid
        )
        small_grads = (d_gain_zero, d_gain_one, d_shift_zero, d_shift_one, g_small)
        if layer == 0:
            extra = (parts_one, owner_mats, g_exp_down, settle)
        else:
            extra = (expert_operands, swapped)
        return d_input, d_input_low, (dense_sum, attn_sum), small_grads, extra

    own_grad = lax.dynamic_index_in_dim(cotangent[:, 0], section_id, 0, keepdims=False)
    out_zero, next_normed, squares_zero, record_zero, settled = forward_zero()
    qkv_both, down_apart, own_grad_seq = settled
    branch_one, attn_squares_one, record_one, grad_rows, up_apart = forward_one(
        out_zero, next_normed, own_grad_seq
    )
    grad_one, grad_one_low, sums_one, small_one, operands_one = backward_layer(
        1, own_grad, own_grad_seq, record_one, grad_rows=grad_rows
    )
    dense_one, attn_one = sums_one
    branch_one = lax.psum_scatter(
        after(branch_one, grad_one_low), DP, scatter_dimension=0, tiled=True
    )
    grad_zero, _, (dense_zero, attn_zero), small_zero, extra = backward_layer(
        0,
        grad_one_low,
        gather_rows(grad_one_low),
        record_zero,
        (dense_one[:, :half_hidden], attn_one),
        operands_one,
        branch_one,
    )
    parts_one, owner_mats, grad_exp_down, branch_one = extra
    branch_one = branch_one.astype(jnp.float32)
    out_one = record_one.residual + branch_one
    squares_one = jnp.concatenate(
        [attn_squares_one, column_sums(branch_one * branch_one), column_sums(out_one * out_one)]
    )
    out_one = low(out_one)

    moved_one = in_order(after(parts_one, grad_zero), DP)
    small_message = pack_small(
        (small_zero, small_one), (squares_zero, squares_one), weight_rows
    )
    small_moved, grad_exp_up = beside(
        lambda blocks: exchange(blocks, EVERY),
        small_message,
        lambda *mats: owner_grads(section_id, *mats),
        (owner_mats(0), owner_mats(1)),
    )
    up_zero = over_dp(by_rows(after(dense_zero[:, :half_hidden], small_moved), dp_size))

    def of_both(of_zero, of_one):
        return of_zero, other_core(of_zero), of_one, other_core(of_one)

    def last_rows(small_moved, *rows):
        return jnp.sum(small_moved, axis=0), finish_rows(section_id, *rows)

    attn_zero, (small_sum, (activations, input_grads)) = beside(
        over_dp,
        by_rows(after(attn_zero, up_zero), dp_size),
        last_rows,
        (small_moved, of_both(out_zero, out_one), of_both(grad_zero, grad_one)),
    )
    up_one, attn_one = moved_one[..., :half_hidden], moved_one[..., half_hidden:]
    down_zero, down_one = dense_zero[:, half_hidden:], dense_one[:, half_hidden:]

    grad_qkv, grad_proj, grad_up, grad_down = finish_weights(
        section_id,
        of_both(up_zero, up_one),
        of_both(attn_zero, attn_one),
        of_both(down_zero, down_one),
        hidden_rows,
    )
    place = expert_id * dp_size + lax.axis_index(DP)
    sums = lax.dynamic_slice_in_dim(
        small_sum[:small_count], place * weight_rows % LANES, weight_rows, axis=1
    )
    totals = small_sum[small_count, :3]
    element_count = micro_count * seq_rows * width * groups * dp_size
    branch_rms = jnp.sqrt(totals / element_count)[None]
    return (
        activations[None, :, None],
        input_grads[None, :, None],
        sums[None, 0:2],
        sums[None, 2:4],
        grad_qkv[None],
        grad_proj[None],
        grad_up[None],
        grad_down[None],
        sums[4 : 4 + experts_total].T[None],
        sums[4 + experts_total :].T[None],
        grad_exp_up[None],
        grad_exp_down[None],
        branch_rms,
    )


def solution(mesh):
    placed = (
        P(None, EX, DP, None),
        P(None, EX, DP, None),
        P(None, EX, None),
        P(SEC, None, EX, DP, None),
        P(SEC, None, (EX, DP)),
        P(SEC, None, (EX, DP)),
        P(SEC, (EX, DP), None),
        P(SEC, (EX, DP), None),
        P(SEC, (EX, DP), None),
        P(SEC, (EX, DP), None),
        P(SEC, (EX, DP), None),
        P(SEC, (EX, DP), None),
        P(SEC, EX, None, DP),
        P(SEC, EX, DP, None),
    )
    return jax.shard_map(
        shards,
        mesh=mesh,
        in_specs=placed,
        out_specs=(
            P(SEC, None, EX, DP, None),
            P(SEC, None, EX, DP, None),
            P(SEC, None, (EX, DP)),
            P(SEC, None, (EX, DP)),
            P(SEC, (EX, DP), None),
            P(SEC, (EX, DP), None),
            P(SEC, (EX, DP), None),
            P(SEC, (EX, DP), None),
            P(SEC, (EX, DP), None),
            P(SEC, (EX, DP), None),
            P(SEC, EX, None, DP),
            P(SEC, EX, DP, None),
            P(SEC, None),
        ),
        check_vma=False,
    )
```
